128 devices in a mesh: rep: 1, dp: 128 (over x, y, z, core).
Axes of the slice: x: 4, y: 4, z: 4, core: 2. Of those that a mesh axis runs over, the one named last changes fastest.
Arguments:
- x: bfloat16 [128, 1024, 1024], P(('rep', 'dp'))
- dy: bfloat16 [128, 1024, 1024], P(('rep', 'dp'))
- wq: bfloat16 [1, 1024, 1024], replicated
- wk: bfloat16 [1, 1024, 1024], replicated
- wv: bfloat16 [1, 1024, 1024], replicated
- wo: bfloat16 [1, 1024, 1024], replicated
- w_gate: bfloat16 [1, 1024, 4096], replicated
- w_up: bfloat16 [1, 1024, 4096], replicated
- w_down: bfloat16 [1, 4096, 1024], replicated
- m_wq: float32 [1, 1024, 1024], replicated
- m_wk: float32 [1, 1024, 1024], replicated
- m_wv: float32 [1, 1024, 1024], replicated
- m_wo: float32 [1, 1024, 1024], replicated
- m_w_gate: float32 [1, 1024, 4096], replicated
- m_w_up: float32 [1, 1024, 4096], replicated
- m_w_down: float32 [1, 4096, 1024], replicated
- v_wq: float32 [1, 1024, 1024], replicated
- v_wk: float32 [1, 1024, 1024], replicated
- v_wv: float32 [1, 1024, 1024], replicated
- v_wo: float32 [1, 1024, 1024], replicated
- v_w_gate: float32 [1, 1024, 4096], replicated
- v_w_up: float32 [1, 1024, 4096], replicated
- v_w_down: float32 [1, 4096, 1024], replicated
Outputs:
- output 1: bfloat16 [1, 1024, 1024], P('rep')
- output 2: bfloat16 [1, 1024, 1024], P('rep')
- output 3: bfloat16 [1, 1024, 1024], P('rep')
- output 4: bfloat16 [1, 1024, 1024], P('rep')
- output 5: bfloat16 [1, 1024, 4096], P('rep')
- output 6: bfloat16 [1, 1024, 4096], P('rep')
- output 7: bfloat16 [1, 4096, 1024], P('rep')
- output 8: float32 [1, 1024, 1024], P('rep')
- output 9: float32 [1, 1024, 1024], P('rep')
- output 10: float32 [1, 1024, 1024], P('rep')
- output 11: float32 [1, 1024, 1024], P('rep')
- output 12: float32 [1, 1024, 4096], P('rep')
- output 13: float32 [1, 1024, 4096], P('rep')
- output 14: float32 [1, 4096, 1024], P('rep')
- output 15: float32 [1, 1024, 1024], P('rep')
- output 16: float32 [1, 1024, 1024], P('rep')
- output 17: float32 [1, 1024, 1024], P('rep')
- output 18: float32 [1, 1024, 1024], P('rep')
- output 19: float32 [1, 1024, 4096], P('rep')
- output 20: float32 [1, 1024, 4096], P('rep')
- output 21: float32 [1, 4096, 1024], P('rep')
All inputs are finite; a program needn't handle non-finite values.
Results may differ from the reference program's by a relative error of at most 0.024.
Values are sent between devices in bfloat16 or wider.
A program may use at most 1.5 GiB of HBM per device.

```python
import jax
import jax.numpy as jnp
from jax import lax

SEQUENCES = 128
TOKENS = 1024
D = 1024
HEADS = 8
KV_HEADS = 8
HEAD = 128
FF = 4096
LAYERS = 1
THETA = 10000
NAMES = ("wq", "wk", "wv", "wo", "w_gate", "w_up", "w_down")
SHAPES = {
    "wq": (LAYERS, D, HEADS * HEAD),
    "wk": (LAYERS, D, KV_HEADS * HEAD),
    "wv": (LAYERS, D, KV_HEADS * HEAD),
    "wo": (LAYERS, HEADS * HEAD, D),
    "w_gate": (LAYERS, D, FF),
    "w_up": (LAYERS, D, FF),
    "w_down": (LAYERS, FF, D),
}


def bump(key, n, height):
    away = (jnp.arange(n, dtype=jnp.int32) - jax.random.randint(key, (), 0, n, jnp.int32)) % n
    return jnp.where(away < n // 8, height, 1.0)


def together(key, own, strength):
    shared = jax.random.normal(key, own.shape[1:], jnp.float32)
    return (own + strength * shared) * lax.rsqrt(1 + strength * strength)


def setup_inputs(seed: int = 0, part: int = 0) -> dict:
    kx, kdy, ka, kb, kz, kf, kh, kl, *keys = jax.random.split(jax.random.key(seed), 8 + 3 * len(NAMES))
    kx, kdy, ka, kb = (jax.random.fold_in(k, part) for k in (kx, kdy, ka, kb))
    kw, km, kv = (keys[i::3] for i in range(3))
    shape = (SEQUENCES, TOKENS, D)
    much_x, much_dy = jax.random.uniform(kz, (2,), jnp.float32, 0.0, 1.0)
    loud = 2.0 ** jax.random.uniform(jax.random.fold_in(kz, 1), (), jnp.float32, -1.0, 2.0)
    layers = 2.0 ** jax.random.uniform(kl, (LAYERS, 1, 1), jnp.float32, -1.0, 1.0)
    times = {"wq": 1.0, "wk": 1.0, "wv": 2.0, "wo": layers, "w_gate": 1.0, "w_up": bump(kh, FF, 4.0), "w_down": layers}
    x = together(ka, jax.random.normal(kx, shape, jnp.float32), much_x) * bump(kf, D, 4.0)
    dy = together(kb, jax.random.normal(kdy, shape, jnp.float32), much_dy)
    drawn = {"x": x.astype(jnp.bfloat16), "dy": (loud * dy * (SEQUENCES * TOKENS) ** -0.5).astype(jnp.bfloat16)}
    for key, name in zip(kw, NAMES, strict=True):
        drawn[name] = (jax.random.normal(key, SHAPES[name], jnp.float32) * SHAPES[name][1] ** -0.5 * times[name]).astype(jnp.bfloat16)
    for key, name in zip(km, NAMES, strict=True):
        drawn[f"m_{name}"] = 0.1 * jax.random.normal(key, SHAPES[name], jnp.float32)
    for key, name in zip(kv, NAMES, strict=True):
        drawn[f"v_{name}"] = loud * loud * jax.random.uniform(key, SHAPES[name], jnp.float32, 0.2, 0.6)
    return drawn


def matmul(a, w):
    return jnp.dot(a, w, preferred_element_type=jnp.float32).astype(jnp.bfloat16)


def normed(h):
    wide = h.astype(jnp.float32)
    scale = lax.rsqrt(jnp.mean(wide**2, -1, keepdims=True) + 1e-6)
    return (wide * scale).astype(jnp.bfloat16)


def turned(t, theta):
    half = t.shape[-1] // 2
    angle = jnp.arange(t.shape[0], dtype=jnp.float32)[:, None] * theta ** (-jnp.arange(half, dtype=jnp.float32) / half)
    cos, sin = jnp.cos(angle)[:, None], jnp.sin(angle)[:, None]
    a, b = t[..., :half].astype(jnp.float32), t[..., half:].astype(jnp.float32)
    return jnp.concatenate([a * cos - b * sin, b * cos + a * sin], -1).astype(jnp.bfloat16)


def seen_by(q, k, v):
    tokens, kv = q.shape[0], k.shape[1]
    q = q.reshape(tokens, kv, -1, q.shape[-1])
    scores = jnp.einsum("tgsd,ugd->gstu", q.astype(jnp.float32), k.astype(jnp.float32)) * q.shape[-1] ** -0.5
    place = jnp.arange(tokens)
    weights = jax.nn.softmax(jnp.where(place[:, None] >= place, scores, -jnp.inf), -1).astype(jnp.bfloat16)
    return jnp.einsum("gstu,ugd->tgsd", weights.astype(jnp.float32), v.astype(jnp.float32)).astype(jnp.bfloat16).reshape(tokens, -1)


def layer(h, w):
    a = normed(h)
    q, k = (turned(matmul(a, w[name]).reshape(h.shape[0], -1, HEAD), THETA) for name in ("wq", "wk"))
    h = h + matmul(seen_by(q, k, matmul(a, w["wv"]).reshape(h.shape[0], -1, HEAD)), w["wo"])
    b = normed(h)
    gate = jnp.dot(b, w["w_gate"], preferred_element_type=jnp.float32)
    up = jnp.dot(b, w["w_up"], preferred_element_type=jnp.float32)
    return h + matmul((jax.nn.silu(gate) * up).astype(jnp.bfloat16), w["w_down"])


def adamw(w, m, v, g):
    m = 0.9 * m + 0.1 * g
    v = 0.95 * v + 0.05 * g * g
    step = m * lax.rsqrt(v + 1e-8) + 0.1 * w
    return (w - 0.02 * step).astype(jnp.bfloat16), m, v


def stack(weights, h):
    return lax.scan(lambda h, w: (layer(h, w), None), h, weights)[0]


def reference(x, dy, wq, wk, wv, wo, w_gate, w_up, w_down, m_wq, m_wk, m_wv, m_wo, m_w_gate, m_w_up, m_w_down, v_wq, v_wk, v_wv, v_wo, v_w_gate, v_w_up, v_w_down):
    weights = dict(zip(NAMES, (wq, wk, wv, wo, w_gate, w_up, w_down), strict=True))

    def take(so_far, sequence):
        h, by_y = sequence
        _, back = jax.vjp(stack, weights, h)
        by_weights, by_h = back(by_y)
        return jax.tree.map(lambda total, term: total + term.astype(jnp.float32), so_far, by_weights), by_h

    none_yet = {name: jnp.zeros(w.shape, jnp.float32) for name, w in weights.items()}
    by_weights, by_x = lax.scan(take, none_yet, (x, dy))
    gradients = [by_weights[name].astype(jnp.bfloat16).astype(jnp.float32) for name in NAMES]
    first = (m_wq, m_wk, m_wv, m_wo, m_w_gate, m_w_up, m_w_down)
    second = (v_wq, v_wk, v_wv, v_wo, v_w_gate, v_w_up, v_w_down)
    new = [adamw(weights[name].astype(jnp.float32), m, v, g) for name, m, v, g in zip(NAMES, first, second, gradients, strict=True)]
    return tuple(one[which] for which in range(3) for one in new)
```

```python
import functools

import jax
import jax.numpy as jnp
import numpy as np
from jax import lax
from jax.experimental import pallas as pl
from jax.experimental.pallas import tpu as pltpu
from jax.sharding import PartitionSpec as P

HEAD = 128
THETA = 10000
NAMES = ("wq", "wk", "wv", "wo", "w_gate", "w_up", "w_down")
LOG2E = 1.4426950408889634
T = 256
F = 512
VMEM = 63 * 2**20
BF, F32 = jnp.bfloat16, jnp.float32


def _dot(a, b, ca, cb):
    return lax.dot_general(a, b, (((ca,), (cb,)), ((), ())), preferred_element_type=F32)


def _turns(tokens):
    half = HEAD // 2
    angle = np.arange(tokens, dtype=np.float32)[:, None] * np.float32(THETA) ** (-np.arange(half, dtype=np.float32) / np.float32(half))
    cos, sin = np.cos(angle).astype(np.float32), np.sin(angle).astype(np.float32)
    return np.concatenate([cos, cos], 1), np.concatenate([-sin, sin], 1)


def _normed(wide):
    return wide * lax.rsqrt(jnp.mean(wide * wide, -1, keepdims=True) + 1e-6)


def _turn(t, c, s):
    t = t.astype(BF).astype(F32)
    parts = [t[:, at : at + HEAD] for at in range(0, t.shape[1], HEAD)]
    return jnp.concatenate([x * c + pltpu.roll(x, HEAD // 2, 1) * s for x in parts], 1).astype(BF)


def _hidden(s):
    n = s.shape[0]
    low = s[n - T :]
    ok = lax.broadcasted_iota(jnp.int32, (T, T), 0) <= lax.broadcasted_iota(jnp.int32, (T, T), 1)
    low = jnp.where(ok, low, -1e30)
    return low if n == T else jnp.concatenate([s[: n - T], low], 0)


def _attention(x_ref, wq_ref, wk_ref, wv_ref, wo_ref, c_ref, s_ref, q_ref, k_ref, v_ref, o_ref, lse_ref, a_ref, h_ref, b_ref, acc):
    i, tokens = pl.program_id(0), x_ref.shape[0]
    rows = [slice(r, r + T) for r in range(0, tokens, T)]
    e = HEAD**-0.5 * LOG2E

    @pl.when(i == 0)
    def _():
        for r in rows:
            a_ref[r] = _normed(x_ref[r].astype(F32)).astype(BF)

    for r in rows:
        a = a_ref[r]
        q_ref[r] = _turn(_dot(a, wq_ref[...], 1, 0), c_ref[r], s_ref[r])
        k_ref[r] = _turn(_dot(a, wk_ref[...], 1, 0), c_ref[r], s_ref[r])
        v_ref[r] = _dot(a, wv_ref[...], 1, 0).astype(BF)
    for n in range(q_ref.shape[1] // HEAD):
        cols = slice(n * HEAD, (n + 1) * HEAD)
        for r in rows:
            keys = slice(0, r.stop)
            s = _hidden(_dot(k_ref[keys, cols], q_ref[r, cols], 1, 1))
            top = s.max(axis=0, keepdims=True)
            p = jnp.exp2((s - top) * e).astype(BF)
            values = jnp.concatenate([v_ref[keys, cols].T, jnp.ones((8, r.stop), BF)], 0)
            mix = _dot(values, p, 1, 0)
            total = mix[HEAD : HEAD + 1]
            o_ref[r, cols] = (mix[:HEAD] * (1 / total)).T.astype(BF)
            lse_ref[0, n : n + 1, r] = top * e + jnp.log(total) * LOG2E
    for r in rows:
        part = _dot(o_ref[r], wo_ref[...], 1, 0)

        @pl.when(i == 0)
        def _():
            acc[r] = part

        @pl.when(i > 0)
        def _():
            acc[r] += part

    @pl.when(i == pl.num_programs(0) - 1)
    def _():
        for r in rows:
            h = x_ref[r] + acc[r].astype(BF)
            h_ref[r] = h
            b_ref[r] = _normed(h.astype(F32)).astype(BF)


def _once(shape):
    return pl.BlockSpec(shape, lambda i: (0,) * len(shape), pipeline_mode=pl.Buffered(1))


def attention(x, wq, wk, wv, wo):
    tokens, d = x.shape
    wide = 2 * HEAD
    steps = wq.shape[1] // wide
    c, s = _turns(tokens)
    cols = pl.BlockSpec((tokens, wide), lambda i: (0, i))
    weights = pl.BlockSpec((d, wide), lambda i: (0, i))
    like = jax.ShapeDtypeStruct((tokens, d), BF)
    return pl.pallas_call(
        _attention,
        grid=(steps,),
        in_specs=[_once((tokens, d)), weights, weights, weights, pl.BlockSpec((wide, d), lambda i: (i, 0)), _once(c.shape), _once(s.shape)],
        out_specs=[cols] * 4 + [pl.BlockSpec((1, 8, tokens), lambda i: (i, 0, 0))] + [_once((tokens, d))] * 3,
        out_shape=[like] * 4 + [jax.ShapeDtypeStruct((steps, 8, tokens), F32)] + [like] * 3,
        scratch_shapes=[pltpu.VMEM((tokens, d), F32)],
        compiler_params=pltpu.CompilerParams(dimension_semantics=("arbitrary",), vmem_limit_bytes=VMEM),
        cost_estimate=pl.CostEstimate(flops=8 * tokens * d * d + 4 * tokens * tokens * d, transcendentals=tokens * tokens * 8, bytes_accessed=24 * 2**20),
        name="attention_forward",
    )(x, wq, wk, wv, wo, jnp.asarray(c), jnp.asarray(s))


def _feed(b_ref, dy_ref, h_ref, wg_ref, wu_ref, wd_ref, dwg_ref, dwu_ref, dwd_ref, dh_ref, bt, acc, act, dg, du):
    i, tokens = pl.program_id(0), b_ref.shape[0]
    rows = [slice(r, r + T) for r in range(0, tokens, T)]

    @pl.when(i == 0)
    def _():
        for r in rows:
            bt[:, r] = b_ref[r].T
        acc[...] = jnp.zeros_like(acc)

    for r in rows:
        b = b_ref[r]
        gate, up = _dot(b, wg_ref[...], 1, 0), _dot(b, wu_ref[...], 1, 0)
        da = _dot(dy_ref[r], wd_ref[...], 1, 1).astype(BF).astype(F32)
        sig = 1 / (1 + jnp.exp2(gate * -LOG2E))
        silu = gate * sig
        act[r] = (silu * up).astype(BF)
        du[r] = (da * silu).astype(BF)
        dg[r] = (da * up * (sig + silu * (1 - sig))).astype(BF)
    dwd_ref[...] = _dot(act[...], dy_ref[...], 0, 0).astype(BF)
    dwg_ref[...] = _dot(bt[...], dg[...], 1, 0).astype(BF)
    dwu_ref[...] = _dot(bt[...], du[...], 1, 0).astype(BF)
    for r in rows:
        acc[r] += _dot(dg[r], wg_ref[...], 1, 1) + _dot(du[r], wu_ref[...], 1, 1)

    @pl.when(i == pl.num_programs(0) - 1)
    def _():
        for r in rows:
            wide, ct = h_ref[r].astype(F32), acc[r].astype(BF).astype(F32)
            scale = lax.rsqrt(jnp.mean(wide * wide, -1, keepdims=True) + 1e-6)
            back = ct * scale - wide * (scale * scale * scale * jnp.mean(ct * wide, -1, keepdims=True))
            dh_ref[r] = dy_ref[r] + back.astype(BF)


def feed(b, dy, h, wg, wu, wd):
    tokens, d = b.shape
    ff = wg.shape[1]
    cols, down = pl.BlockSpec((d, F), lambda i: (0, i)), pl.BlockSpec((F, d), lambda i: (i, 0))
    like = lambda a: jax.ShapeDtypeStruct(a.shape, BF)
    return pl.pallas_call(
        _feed,
        grid=(ff // F,),
        in_specs=[_once((tokens, d))] * 3 + [cols, cols, down],
        out_specs=[cols, cols, down, _once((tokens, d))],
        out_shape=[like(wg), like(wu), like(wd), like(b)],
        scratch_shapes=[pltpu.VMEM((d, tokens), BF), pltpu.VMEM((tokens, d), F32)] + [pltpu.VMEM((tokens, F), BF)] * 3,
        compiler_params=pltpu.CompilerParams(dimension_semantics=("arbitrary",), vmem_limit_bytes=VMEM),
        cost_estimate=pl.CostEstimate(flops=16 * tokens * d * ff, transcendentals=tokens * ff * 2, bytes_accessed=60 * 2**20),
        name="feed_forward_backward",
    )(b, dy, h, wg, wu, wd)


def _attention_back(dh_ref, a_ref, wo_ref, q_ref, k_ref, v_ref, o_ref, lse_ref, c_ref, s_ref, dwq_ref, dwk_ref, dwv_ref, dwo_ref,
                    at, do, dq, dk, dv):
    i, tokens = pl.program_id(0), dh_ref.shape[0]
    rows = [slice(r, r + T) for r in range(0, tokens, T)]
    scale = HEAD**-0.5
    e = scale * LOG2E

    @pl.when(i == 0)
    def _():
        for r in rows:
            at[:, r] = a_ref[r].T

    for r in rows:
        do[r] = _dot(dh_ref[r], wo_ref[...], 1, 1).astype(BF)
    dwo_ref[...] = _dot(o_ref[...], dh_ref[...], 0, 0).astype(BF)
    for n in range(q_ref.shape[1] // HEAD):
        cols = slice(n * HEAD, (n + 1) * HEAD)
        dk[...] = jnp.zeros_like(dk)
        dv[...] = jnp.zeros_like(dv)
        for r in rows:
            keys = slice(0, r.stop)
            dor, qr = do[r, cols], q_ref[r, cols]
            delta = (dor.astype(F32) * o_ref[r, cols].astype(F32)).T.sum(axis=0, keepdims=True)
            s = _hidden(_dot(k_ref[keys, cols], qr, 1, 1) * e - lse_ref[0, n : n + 1, r])
            p = jnp.exp2(s)
            ds = (p * (_dot(v_ref[keys, cols], dor, 1, 1) - delta)).astype(BF)
            dv[keys] += _dot(p.astype(BF), dor, 1, 0)
            dk[keys] += _dot(ds, qr, 1, 0)
            dq[r, cols] = (_dot(k_ref[keys, cols], ds, 0, 0) * scale).T.astype(BF)
        do[:, cols] = dv[...].astype(BF)
        k_out = (dk[...] * scale).astype(BF).astype(F32)
        dq[:, 2 * HEAD + n * HEAD : 2 * HEAD + (n + 1) * HEAD] = (k_out * c_ref[...] - pltpu.roll(k_out, HEAD // 2, 1) * s_ref[...]).astype(BF)
        q_out = dq[:, cols].astype(F32)
        dq[:, cols] = (q_out * c_ref[...] - pltpu.roll(q_out, HEAD // 2, 1) * s_ref[...]).astype(BF)
    dwq_ref[...] = _dot(at[...], dq[:, : 2 * HEAD], 1, 0).astype(BF)
    dwk_ref[...] = _dot(at[...], dq[:, 2 * HEAD :], 1, 0).astype(BF)
    dwv_ref[...] = _dot(at[...], do[...], 1, 0).astype(BF)


def attention_back(dh, a, wo, q, k, v, o, lse):
    tokens, d = dh.shape
    wide = 2 * HEAD
    c, s = _turns(tokens)
    cols, out = pl.BlockSpec((tokens, wide), lambda i: (0, i)), pl.BlockSpec((d, wide), lambda i: (0, i))
    down = pl.BlockSpec((wide, d), lambda i: (i, 0))
    like = jax.ShapeDtypeStruct((d, d), BF)
    return pl.pallas_call(
        _attention_back,
        grid=(d // wide,),
        in_specs=[_once((tokens, d))] * 2 + [down] + [cols] * 4 + [pl.BlockSpec((1, 8, tokens), lambda i: (i, 0, 0)), _once(c.shape), _once(s.shape)],
        out_specs=[out, out, out, down],
        out_shape=[like] * 4,
        scratch_shapes=[pltpu.VMEM((d, tokens), BF), pltpu.VMEM((tokens, wide), BF), pltpu.VMEM((tokens, 2 * wide), BF)]
        + [pltpu.VMEM((tokens, HEAD), F32)] * 2,
        compiler_params=pltpu.CompilerParams(dimension_semantics=("arbitrary",), vmem_limit_bytes=VMEM),
        cost_estimate=pl.CostEstimate(flops=10 * tokens * d * d + 10 * tokens * tokens * d, transcendentals=tokens * tokens * 8, bytes_accessed=30 * 2**20),
        name="attention_backward",
    )(dh, a, wo, q, k, v, o, lse, jnp.asarray(c), jnp.asarray(s))


def adamw(w, m, v, g):
    m = 0.9 * m + 0.1 * g
    v = 0.95 * v + 0.05 * g * g
    step = m * lax.rsqrt(v + 1e-8) + 0.1 * w
    return (w - 0.02 * step).astype(jnp.bfloat16), m, v


def gradients(x, dy, w):
    q, k, v, o, lse, a, h, b = attention(x, w["wq"], w["wk"], w["wv"], w["wo"])
    dwg, dwu, dwd, dh = feed(b, dy, h, w["w_gate"], w["w_up"], w["w_down"])
    dwq, dwk, dwv, dwo = attention_back(dh, a, w["wo"], q, k, v, o, lse)
    return {"wq": dwq, "wk": dwk, "wv": dwv, "wo": dwo, "w_gate": dwg, "w_up": dwu, "w_down": dwd}


def solution(mesh):
    def step(x, dy, *arrays):
        weights, m, v = (dict(zip(NAMES, arrays[i : i + 7], strict=True)) for i in (0, 7, 14))
        mine = gradients(x[0], dy[0], {n: w[0] for n, w in weights.items()})
        new, feeds = {}, ("w_gate", "w_up", "w_down")
        summed = dict(zip(feeds, lax.psum([mine[n] for n in feeds], "dp"), strict=True))
        others = [n for n in NAMES if n not in feeds]
        tied = lax.optimization_barrier(([mine[n] for n in others], summed))
        summed = tied[1]
        summed.update(zip(others, lax.psum(tied[0], "dp"), strict=True))
        for name in NAMES:
            new[name] = adamw(weights[name].astype(F32), m[name], v[name], summed[name][None].astype(F32))
        return tuple(new[name][which] for which in range(3) for name in NAMES)

    states, all_of = P(("rep", "dp"), None, None), P(None, None, None)
    return jax.shard_map(
        step,
        mesh=mesh,
        in_specs=(states, states) + (all_of,) * 21,
        out_specs=(P("rep", None, None),) * 21,
        check_vma=False,
    )
```

```python
import functools

import jax
import jax.numpy as jnp
import numpy as np
from jax import lax
from jax.experimental import pallas as pl
from jax.experimental.pallas import tpu as pltpu
from jax.sharding import PartitionSpec as P

HEAD = 128
THETA = 10000
NAMES = ("wq", "wk", "wv", "wo", "w_gate", "w_up", "w_down")
LOG2E = 1.4426950408889634
T = 256
F = 512
VMEM = 63 * 2**20
BF, F32 = jnp.bfloat16, jnp.float32


def _dot(a, b, ca, cb):
    return lax.dot_general(a, b, (((ca,), (cb,)), ((), ())), preferred_element_type=F32)


def _turns(tokens):
    half = HEAD // 2
    angle = np.arange(tokens, dtype=np.float32)[:, None] * np.float32(THETA) ** (-np.arange(half, dtype=np.float32) / np.float32(half))
    cos, sin = np.cos(angle).astype(np.float32), np.sin(angle).astype(np.float32)
    return np.concatenate([cos, cos], 1), np.concatenate([-sin, sin], 1)


def _normed(wide):
    return wide * lax.rsqrt(jnp.mean(wide * wide, -1, keepdims=True) + 1e-6)


def _turn(t, c, s):
    t = t.astype(BF).astype(F32)
    parts = [t[:, at : at + HEAD] for at in range(0, t.shape[1], HEAD)]
    return jnp.concatenate([x * c + pltpu.roll(x, HEAD // 2, 1) * s for x in parts], 1).astype(BF)


def _hidden(s):
    n = s.shape[0]
    low = s[n - T :]
    ok = lax.broadcasted_iota(jnp.int32, (T, T), 0) <= lax.broadcasted_iota(jnp.int32, (T, T), 1)
    low = jnp.where(ok, low, -1e30)
    return low if n == T else jnp.concatenate([s[: n - T], low], 0)


def _attention(x_ref, wq_ref, wk_ref, wv_ref, wo_ref, c_ref, s_ref, q_ref, k_ref, v_ref, o_ref, lse_ref, a_ref, h_ref, b_ref, acc):
    i, tokens = pl.program_id(0), x_ref.shape[0]
    rows = [slice(r, r + T) for r in range(0, tokens, T)]
    e = HEAD**-0.5 * LOG2E

    @pl.when(i == 0)
    def _():
        for r in rows:
            a_ref[r] = _normed(x_ref[r].astype(F32)).astype(BF)

    for r in rows:
        a = a_ref[r]
        q_ref[r] = _turn(_dot(a, wq_ref[...], 1, 0), c_ref[r], s_ref[r])
        k_ref[r] = _turn(_dot(a, wk_ref[...], 1, 0), c_ref[r], s_ref[r])
        v_ref[r] = _dot(a, wv_ref[...], 1, 0).astype(BF)
    for n in range(q_ref.shape[1] // HEAD):
        cols = slice(n * HEAD, (n + 1) * HEAD)
        for r in rows:
            keys = slice(0, r.stop)
            s = _hidden(_dot(k_ref[keys, cols], q_ref[r, cols], 1, 1))
            top = s.max(axis=0, keepdims=True)
            p = jnp.exp2((s - top) * e).astype(BF)
            values = jnp.concatenate([v_ref[keys, cols].T, jnp.ones((8, r.stop), BF)], 0)
            mix = _dot(values, p, 1, 0)
            total = mix[HEAD : HEAD + 1]
            o_ref[r, cols] = (mix[:HEAD] * (1 / total)).T.astype(BF)
            lse_ref[0, n : n + 1, r] = top * e + jnp.log(total) * LOG2E
    for r in rows:
        part = _dot(o_ref[r], wo_ref[...], 1, 0)

        @pl.when(i == 0)
        def _():
            acc[r] = part

        @pl.when(i > 0)
        def _():
            acc[r] += part

    @pl.when(i == pl.num_programs(0) - 1)
    def _():
        for r in rows:
            h = x_ref[r] + acc[r].astype(BF)
            h_ref[r] = h
            b_ref[r] = _normed(h.astype(F32)).astype(BF)


def _once(shape):
    return pl.BlockSpec(shape, lambda i: (0,) * len(shape), pipeline_mode=pl.Buffered(1))


def attention(x, wq, wk, wv, wo):
    tokens, d = x.shape
    wide = 2 * HEAD
    steps = wq.shape[1] // wide
    c, s = _turns(tokens)
    cols = pl.BlockSpec((tokens, wide), lambda i: (0, i))
    weights = pl.BlockSpec((d, wide), lambda i: (0, i))
    like = jax.ShapeDtypeStruct((tokens, d), BF)
    return pl.pallas_call(
        _attention,
        grid=(steps,),
        in_specs=[_once((tokens, d)), weights, weights, weights, pl.BlockSpec((wide, d), lambda i: (i, 0)), _once(c.shape), _once(s.shape)],
        out_specs=[cols] * 4 + [pl.BlockSpec((1, 8, tokens), lambda i: (i, 0, 0))] + [_once((tokens, d))] * 3,
        out_shape=[like] * 4 + [jax.ShapeDtypeStruct((steps, 8, tokens), F32)] + [like] * 3,
        scratch_shapes=[pltpu.VMEM((tokens, d), F32)],
        compiler_params=pltpu.CompilerParams(dimension_semantics=("arbitrary",), vmem_limit_bytes=VMEM),
        cost_estimate=pl.CostEstimate(flops=8 * tokens * d * d + 4 * tokens * tokens * d, transcendentals=tokens * tokens * 8, bytes_accessed=24 * 2**20),
        name="attention_forward",
    )(x, wq, wk, wv, wo, jnp.asarray(c), jnp.asarray(s))


def _feed(b_ref, dy_ref, h_ref, wg_ref, wu_ref, wd_ref, dwg_ref, dwu_ref, dwd_ref, dh_ref, bt, acc, act, dg, du):
    i, tokens = pl.program_id(0), b_ref.shape[0]
    rows = [slice(r, r + T) for r in range(0, tokens, T)]

    @pl.when(i == 0)
    def _():
        for r in rows:
            bt[:, r] = b_ref[r].T
        acc[...] = jnp.zeros_like(acc)

    for r in rows:
        b = b_ref[r]
        gate, up = _dot(b, wg_ref[...], 1, 0), _dot(b, wu_ref[...], 1, 0)
        da = _dot(dy_ref[r], wd_ref[...], 1, 1).astype(BF).astype(F32)
        sig = 1 / (1 + jnp.exp2(gate * -LOG2E))
        silu = gate * sig
        act[r] = (silu * up).astype(BF)
        du[r] = (da * silu).astype(BF)
        dg[r] = (da * up * (sig + silu * (1 - sig))).astype(BF)
    dwd_ref[...] = _dot(act[...], dy_ref[...], 0, 0).astype(BF)
    dwg_ref[...] = _dot(bt[...], dg[...], 1, 0).astype(BF)
    dwu_ref[...] = _dot(bt[...], du[...], 1, 0).astype(BF)
    for r in rows:
        acc[r] += _dot(dg[r], wg_ref[...], 1, 1) + _dot(du[r], wu_ref[...], 1, 1)

    @pl.when(i == pl.num_programs(0) - 1)
    def _():
        for r in rows:
            wide, ct = h_ref[r].astype(F32), acc[r].astype(BF).astype(F32)
            scale = lax.rsqrt(jnp.mean(wide * wide, -1, keepdims=True) + 1e-6)
            back = ct * scale - wide * (scale * scale * scale * jnp.mean(ct * wide, -1, keepdims=True))
            dh_ref[r] = dy_ref[r] + back.astype(BF)


def feed(b, dy, h, wg, wu, wd):
    tokens, d = b.shape
    ff = wg.shape[1]
    cols, down = pl.BlockSpec((d, F), lambda i: (0, i)), pl.BlockSpec((F, d), lambda i: (i, 0))
    like = lambda a: jax.ShapeDtypeStruct(a.shape, BF)
    return pl.pallas_call(
        _feed,
        grid=(ff // F,),
        in_specs=[_once((tokens, d))] * 3 + [cols, cols, down],
        out_specs=[cols, cols, down, _once((tokens, d))],
        out_shape=[like(wg), like(wu), like(wd), like(b)],
        scratch_shapes=[pltpu.VMEM((d, tokens), BF), pltpu.VMEM((tokens, d), F32)] + [pltpu.VMEM((tokens, F), BF)] * 3,
        compiler_params=pltpu.CompilerParams(dimension_semantics=("arbitrary",), vmem_limit_bytes=VMEM),
        cost_estimate=pl.CostEstimate(flops=16 * tokens * d * ff, transcendentals=tokens * ff * 2, bytes_accessed=60 * 2**20),
        name="feed_forward_backward",
    )(b, dy, h, wg, wu, wd)


def _attention_back(dh_ref, a_ref, wo_ref, q_ref, k_ref, v_ref, o_ref, lse_ref, c_ref, s_ref, dwq_ref, dwk_ref, dwv_ref, dwo_ref,
                    at, do, dq, dk, dv):
    i, tokens = pl.program_id(0), dh_ref.shape[0]
    rows = [slice(r, r + T) for r in range(0, tokens, T)]
    scale = HEAD**-0.5
    e = scale * LOG2E

    @pl.when(i == 0)
    def _():
        for r in rows:
            at[:, r] = a_ref[r].T

    for r in rows:
        do[r] = _dot(dh_ref[r], wo_ref[...], 1, 1).astype(BF)
    dwo_ref[...] = _dot(o_ref[...], dh_ref[...], 0, 0).astype(BF)
    for n in range(q_ref.shape[1] // HEAD):
        cols = slice(n * HEAD, (n + 1) * HEAD)
        dk[...] = jnp.zeros_like(dk)
        dv[...] = jnp.zeros_like(dv)
        for r in rows:
            keys = slice(0, r.stop)
            dor, qr = do[r, cols], q_ref[r, cols]
            delta = (dor.astype(F32) * o_ref[r, cols].astype(F32)).T.sum(axis=0, keepdims=True)
            s = _hidden(_dot(k_ref[keys, cols], qr, 1, 1) * e - lse_ref[0, n : n + 1, r])
            p = jnp.exp2(s)
            ds = (p * (_dot(v_ref[keys, cols], dor, 1, 1) - delta)).astype(BF)
            dv[keys] += _dot(p.astype(BF), dor, 1, 0)
            dk[keys] += _dot(ds, qr, 1, 0)
            dq[r, cols] = (_dot(k_ref[keys, cols], ds, 0, 0) * scale).T.astype(BF)
        do[:, cols] = dv[...].astype(BF)
        k_out = (dk[...] * scale).astype(BF).astype(F32)
        dq[:, 2 * HEAD + n * HEAD : 2 * HEAD + (n + 1) * HEAD] = (k_out * c_ref[...] - pltpu.roll(k_out, HEAD // 2, 1) * s_ref[...]).astype(BF)
        q_out = dq[:, cols].astype(F32)
        dq[:, cols] = (q_out * c_ref[...] - pltpu.roll(q_out, HEAD // 2, 1) * s_ref[...]).astype(BF)
    dwq_ref[...] = _dot(at[...], dq[:, : 2 * HEAD], 1, 0).astype(BF)
    dwk_ref[...] = _dot(at[...], dq[:, 2 * HEAD :], 1, 0).astype(BF)
    dwv_ref[...] = _dot(at[...], do[...], 1, 0).astype(BF)


def attention_back(dh, a, wo, q, k, v, o, lse):
    tokens, d = dh.shape
    wide = 2 * HEAD
    c, s = _turns(tokens)
    cols, out = pl.BlockSpec((tokens, wide), lambda i: (0, i)), pl.BlockSpec((d, wide), lambda i: (0, i))
    down = pl.BlockSpec((wide, d), lambda i: (i, 0))
    like = jax.ShapeDtypeStruct((d, d), BF)
    return pl.pallas_call(
        _attention_back,
        grid=(d // wide,),
        in_specs=[_once((tokens, d))] * 2 + [down] + [cols] * 4 + [pl.BlockSpec((1, 8, tokens), lambda i: (i, 0, 0)), _once(c.shape), _once(s.shape)],
        out_specs=[out, out, out, down],
        out_shape=[like] * 4,
        scratch_shapes=[pltpu.VMEM((d, tokens), BF), pltpu.VMEM((tokens, wide), BF), pltpu.VMEM((tokens, 2 * wide), BF)]
        + [pltpu.VMEM((tokens, HEAD), F32)] * 2,
        compiler_params=pltpu.CompilerParams(dimension_semantics=("arbitrary",), vmem_limit_bytes=VMEM),
        cost_estimate=pl.CostEstimate(flops=10 * tokens * d * d + 10 * tokens * tokens * d, transcendentals=tokens * tokens * 8, bytes_accessed=30 * 2**20),
        name="attention_backward",
    )(dh, a, wo, q, k, v, o, lse, jnp.asarray(c), jnp.asarray(s))


def adamw(w, m, v, g):
    m = 0.9 * m + 0.1 * g
    v = 0.95 * v + 0.05 * g * g
    step = m * lax.rsqrt(v + 1e-8) + 0.1 * w
    return (w - 0.02 * step).astype(jnp.bfloat16), m, v


def gradients(x, dy, w):
    q, k, v, o, lse, a, h, b = attention(x, w["wq"], w["wk"], w["wv"], w["wo"])
    dwg, dwu, dwd, dh = feed(b, dy, h, w["w_gate"], w["w_up"], w["w_down"])
    dwq, dwk, dwv, dwo = attention_back(dh, a, w["wo"], q, k, v, o, lse)
    return {"wq": dwq, "wk": dwk, "wv": dwv, "wo": dwo, "w_gate": dwg, "w_up": dwu, "w_down": dwd}


RING = 4
STRIDE = {"x": 32, "y": 8, "z": 2}
COLOURS = (("x", "y", "z"), ("y", "z", "x"), ("z", "x", "y"))
TICKS = 4
AT = (0, 1, 3, 5, 7, 9, 11, 13, 15, 17, 20, 22, 24)
LAG = AT[-1] // TICKS + 1


class Sum:
    def __init__(self, colour, blk, local, out, refs, sems):
        self.c, (self.R, self.C) = colour, blk
        self.local, self.out = local, out
        self.rc, self.s, self.sa1, self.ra1, self.sa2, self.ra2, self.ra, self.sb1, self.rb1, self.sb2, self.rb2, self.rb, self.sc, self.rcc, self.sg = refs
        self.send, self.recv, self.gather = sems
        me = lax.axis_index("dp")
        self.me, self.core = me, lax.rem(me, 2)
        self.partner = me + 1 - 2 * self.core
        place = lambda axis: lax.rem(lax.div(me, STRIDE[axis]), RING)
        self.a, self.b, self.k = (place(axis) for axis in COLOURS[colour])

    def peer(self, n, by):
        axis, at = COLOURS[self.c][n], (self.a, self.b, self.k)[n]
        return self.me + (lax.rem(at + by + RING, RING) - at) * STRIDE[axis]

    def copy(self, src, dst, kind, device, slot=None, r=None):
        recv = self.recv.at[self.c, kind, slot] if r is None else self.gather.at[self.c, kind - 6, r]
        return pltpu.make_async_remote_copy(src, dst, self.send.at[self.c, kind], recv, device_id={"dp": device})

    def wait(self, ref, kind, slot=None, r=None, send=None):
        recv = self.recv.at[self.c, kind, slot] if r is None else self.gather.at[self.c, kind - 6, r]
        pltpu.make_async_copy(ref, ref, recv).wait()
        ref = ref if send is None else send
        pltpu.make_async_copy(ref, ref, self.send.at[self.c, kind]).wait()

    def rows(self, q, n):
        return pl.ds(pl.multiple_of(q * n, 16), n)

    def cols(self, q):
        return pl.ds(pl.multiple_of(q * (self.C // 4), 128), self.C // 4)

    def region(self, r, level):
        first = self.core * (self.R // 2)
        if level > 0:
            first = first + self.a * (self.R // 8)
        if level > 1:
            first = first + self.b * (self.R // 32)
        return first

    def stage(self, n, r):
        R, C = self.R, self.C
        slot = lax.rem(r, 2)
        n8, n32, half = R // 8, R // 32, C // 2
        left, right = pl.ds(0, half), pl.ds(half, half)
        f32 = lambda v: v.astype(F32)
        low = lambda v: v.astype(BF)
        if n == 0:
            self.copy(self.local.at[slot, self.rows(1 - self.core, R // 2)], self.rc.at[slot], 0, self.partner, slot).start()
        elif n == 1:
            self.wait(self.rc.at[slot], 0, slot)
            for at in range(0, R // 2, n8):
                self.s[pl.ds(at, n8)] = f32(self.local[slot, self.rows(self.core * (R // 2 // n8) + at // n8, n8)]) + f32(self.rc[slot, pl.ds(at, n8)])
            self.sa1[...] = low(self.s[self.rows(lax.rem(self.a + 2, RING), n8)])
            self.both(self.sa1, self.ra1, 1, 0, slot, left, right)
        elif n == 2:
            self.wait(self.ra1.at[slot], 1, slot)
            self.second(self.s, self.a, n8, self.ra1, self.sa2, slot, half)
            self.pair(self.sa2, self.ra2, 2, 0, slot)
        elif n == 3:
            self.wait(self.ra2.at[slot], 2, slot)
            self.ra[...] = self.s[self.rows(self.a, n8)] + f32(self.ra2[slot, 0]) + f32(self.ra2[slot, 1])
            self.sb1[...] = low(self.ra[self.rows(lax.rem(self.b + 2, RING), n32)])
            self.both(self.sb1, self.rb1, 3, 1, slot, left, right)
        elif n == 4:
            self.wait(self.rb1.at[slot], 3, slot)
            self.second(self.ra, self.b, n32, self.rb1, self.sb2, slot, half)
            self.pair(self.sb2, self.rb2, 4, 1, slot)
        elif n == 5:
            self.wait(self.rb2.at[slot], 4, slot)
            total = self.ra[self.rows(self.b, n32)] + f32(self.rb2[slot, 0]) + f32(self.rb2[slot, 1])
            self.rb[...] = total
            self.sc[...] = low(total)
            for by in (1, 2, 3):
                to = lax.rem(self.k + by, RING)
                self.copy(self.sc.at[:, self.cols(to)], self.rcc.at[slot, by - 1], 5, self.peer(2, by), slot).start()
        elif n == 6:
            self.wait(self.rcc.at[slot], 5, slot)
            total = self.rb[:, self.cols(self.k)]
            for by in range(3):
                total = total + f32(self.rcc[slot, by])
            self.sg[...] = low(total)
            mine = self.out(r, self.region(r, 2), n32).at[:, self.cols(self.k)]
            pltpu.make_async_copy(self.sg, mine, self.gather.at[self.c, 0, r]).start()
            for by in (1, 2, 3):
                self.copy(self.sg, mine, 6, self.peer(2, by), r=r).start()
        elif n == 7:
            mine = self.out(r, self.region(r, 2), n32)
            self.wait(mine, 6, r=r, send=self.rcc.at[slot])
            for by in (1, -1):
                self.copy(mine, mine, 7, self.peer(1, by), r=r).start()
        elif n == 8:
            self.wait(self.out(r, 0, 2 * n32), 7, r=r)
            self.onward(r, 8, 1, self.region(r, 1), self.b, n32, left, right)
        elif n == 9:
            self.wait(self.out(r, 0, n32), 8, r=r)
            mine = self.out(r, self.region(r, 1), n8)
            for by in (1, -1):
                self.copy(mine, mine, 9, self.peer(0, by), r=r).start()
        elif n == 10:
            self.wait(self.out(r, 0, 2 * n8), 9, r=r)
            self.onward(r, 10, 0, self.region(r, 0), self.a, n8, left, right)
        elif n == 11:
            self.wait(self.out(r, 0, n8), 10, r=r)
            mine = self.out(r, self.region(r, 0), R // 2)
            self.copy(mine, mine, 11, self.partner, r=r).start()
        else:
            self.wait(self.out(r, 0, R // 2), 11, r=r)

    def both(self, src, dst, kind, axis, slot, left, right):
        self.copy(src.at[:, left], dst.at[slot, :, left], kind, self.peer(axis, 1), slot).start()
        self.copy(src.at[:, right], dst.at[slot, :, right], kind, self.peer(axis, -1), slot).start()

    def second(self, total, at, n, came, out, slot, half):
        up, down = self.rows(lax.rem(at + 1, RING), n), self.rows(lax.rem(at + 3, RING), n)
        out[0, :, :half] = (total[up, :half] + came[slot, :, :half].astype(F32)).astype(BF)
        out[0, :, half:] = total[up, half:].astype(BF)
        out[1, :, :half] = total[down, :half].astype(BF)
        out[1, :, half:] = (total[down, half:] + came[slot, :, half:].astype(F32)).astype(BF)

    def pair(self, src, dst, kind, axis, slot):
        self.copy(src.at[0], dst.at[slot, 0], kind, self.peer(axis, 1), slot).start()
        self.copy(src.at[1], dst.at[slot, 1], kind, self.peer(axis, -1), slot).start()

    def onward(self, r, kind, axis, first, at, n, left, right):
        before = self.out(r, first + lax.rem(at + 3, RING) * n, n).at[:, left]
        after = self.out(r, first + lax.rem(at + 1, RING) * n, n).at[:, right]
        self.copy(before, before, kind, self.peer(axis, 1), r=r).start()
        self.copy(after, after, kind, self.peer(axis, -1), r=r).start()


def _sum_scratch(R, C):
    n2, n8, n32 = R // 2, R // 8, R // 32
    return [pltpu.VMEM(shape, kind) for shape, kind in (
        ((2, n2, C), BF), ((n2, C), F32), ((n8, C), BF), ((2, n8, C), BF), ((2, n8, C), BF), ((2, 2, n8, C), BF), ((n8, C), F32),
        ((n32, C), BF), ((2, n32, C), BF), ((2, n32, C), BF), ((2, 2, n32, C), BF), ((n32, C), F32), ((n32, C), BF), ((2, 3, n32, C // 4), BF),
        ((n32, C // 4), BF))]


def _meet():
    me = lax.axis_index("dp")
    sem = pltpu.get_barrier_semaphore()
    pl.semaphore_signal(sem, 1, device_id={"dp": me + 1 - 2 * lax.rem(me, 2)})
    for stride in STRIDE.values():
        at = lax.rem(lax.div(me, stride), RING)
        for by in (1, 2, 3):
            pl.semaphore_signal(sem, 1, device_id={"dp": me + (lax.rem(at + by, RING) - at) * stride})
    pl.semaphore_wait(sem, 1 + 3 * 3)


def _stages(step, sums, last, tick):
    for n in reversed(range(len(AT))):
        if AT[n] % TICKS == tick:
            r = step - 1 - AT[n] // TICKS
            for c, one in enumerate(sums):

                @pl.when((r >= 0) & (r <= last[c]))
                def _():
                    one.stage(n, r)


DOWN, UP = (512, 1024), (1024, 512)
LAST = (9, 10, 10)
BASE = 512 * (LAST[1] + 1)


def _group_sum(wq, wk, wv, wo, w_gate, w_up, w_down, rows_out, cols_out, *scratch, shapes, last):
    step = pl.program_id(0)
    n = 15
    parts, (local0, local1, local2, send, recv, gather, load) = [scratch[i * n : (i + 1) * n] for i in range(3)], scratch[3 * n :]
    locals_ = (local0, local1, local2)
    (R0, C0), (R1, C1) = shapes[0], shapes[1]
    outs = (
        lambda r, first, size: rows_out.at[pl.ds(pl.multiple_of(r * R0 + first, 16), size)],
        lambda r, first, size: cols_out.at[pl.ds(pl.multiple_of(first, 16), size), pl.ds(pl.multiple_of(r * C1, 128), C1)],
        lambda r, first, size: cols_out.at[pl.ds(pl.multiple_of(first, 16), size), pl.ds(pl.multiple_of((r + last[1] + 1) * C1, 128), C1)],
    )
    sums = [Sum(c, shapes[c], locals_[c], outs[c], parts[c], (send, recv, gather)) for c in range(3)]
    slot = lax.rem(step, 2)
    feed = lambda a: (lambda: a.at[:, pl.ds(pl.multiple_of(step * C1, 128), C1)])
    col = lambda a, at: (lambda: a.at[:, pl.ds(at * C1, C1)])
    row = lambda a, at: (lambda: a.at[pl.ds(pl.multiple_of(at * R0, 16), R0)])
    f = last[1] - 2
    sources = (
        ((lambda i: i < f, row(w_down, step)), (lambda i: (i >= f) & (i <= last[0]), row(wo, step - f))),
        ((lambda i: i < f, feed(w_gate)), (lambda i: i == f, col(wq, 0)), (lambda i: i == f + 1, col(wq, 1)), (lambda i: i == f + 2, col(wv, 0))),
        ((lambda i: i < f, feed(w_up)), (lambda i: i == f, col(wk, 0)), (lambda i: i == f + 1, col(wk, 1)), (lambda i: i == f + 2, col(wv, 1))),
    )

    @pl.when(step == 0)
    def _():
        _meet()

    for tick in range(TICKS):
        _stages(step, sums, last, tick)
        if 0 < tick < TICKS - 1:
            continue
        for c in range(3):
            for on, source in sources[c]:

                @pl.when(on(step) & (step <= last[c]))
                def _():
                    copy = pltpu.make_async_copy(source(), locals_[c].at[slot], load.at[c])
                    copy.start() if tick == 0 else copy.wait()


def group_sum(grads, shapes=(DOWN, UP, UP), last=LAST):
    rounds = max(last) + 1
    (R0, C0), (R1, C1) = shapes[:2]
    hbm = pl.BlockSpec(memory_space=pl.ANY)
    return pl.pallas_call(
        functools.partial(_group_sum, shapes=shapes, last=last),
        grid=(rounds + 1 + AT[-1] // TICKS,),
        in_specs=[hbm] * 7,
        out_specs=[hbm] * 2,
        out_shape=[jax.ShapeDtypeStruct((R0 * (last[0] + 1), C0), BF), jax.ShapeDtypeStruct((R1, 2 * rounds * C1), BF)],
        scratch_shapes=[s for shape in shapes for s in _sum_scratch(*shape)]
        + [pltpu.VMEM((2, *shape), BF) for shape in shapes]
        + [pltpu.SemaphoreType.DMA((3, 12)), pltpu.SemaphoreType.DMA((3, 6, 2)), pltpu.SemaphoreType.DMA((3, 6, rounds)), pltpu.SemaphoreType.DMA((3,))],
        compiler_params=pltpu.CompilerParams(dimension_semantics=("arbitrary",), vmem_limit_bytes=VMEM, collective_id=0, has_side_effects=True),
        cost_estimate=pl.CostEstimate(flops=10**9, transcendentals=0, bytes_accessed=2**28),
        name="group_sum",
    )(*[grads[n] for n in NAMES])


def solution(mesh):
    def step(x, dy, *arrays):
        weights, m, v = (dict(zip(NAMES, arrays[i : i + 7], strict=True)) for i in (0, 7, 14))
        rows, cols = group_sum(gradients(x[0], dy[0], {n: w[0] for n, w in weights.items()}))
        ff, half = 4096, 512
        summed = {
            "w_down": rows[:ff], "wo": rows[ff:], "w_gate": cols[:, :ff], "wq": cols[:, ff : ff + 2 * half],
            "w_up": cols[:, BASE : BASE + ff], "wk": cols[:, BASE + ff : BASE + ff + 2 * half],
            "wv": jnp.concatenate([cols[:, BASE - half : BASE], cols[:, 2 * BASE - half :]], 1),
        }
        new = {name: adamw(weights[name].astype(F32), m[name], v[name], summed[name][None].astype(F32)) for name in NAMES}
        return tuple(new[name][which] for which in range(3) for name in NAMES)

    states, all_of = P(("rep", "dp"), None, None), P(None, None, None)
    return jax.shard_map(
        step,
        mesh=mesh,
        in_specs=(states, states) + (all_of,) * 21,
        out_specs=(P("rep", None, None),) * 21,
        check_vma=False,
    )
```

```python
import functools

import jax
import jax.numpy as jnp
import numpy as np
from jax import lax
from jax.experimental import pallas as pl
from jax.experimental.pallas import tpu as pltpu
from jax.sharding import PartitionSpec as P

HEAD = 128
THETA = 10000
NAMES = ("wq", "wk", "wv", "wo", "w_gate", "w_up", "w_down")
LOG2E = 1.4426950408889634
T = 256
F = 512
VMEM = 63 * 2**20
BF, F32 = jnp.bfloat16, jnp.float32


def _dot(a, b, ca, cb):
    return lax.dot_general(a, b, (((ca,), (cb,)), ((), ())), preferred_element_type=F32)


def _turns(tokens):
    half = HEAD // 2
    angle = np.arange(tokens, dtype=np.float32)[:, None] * np.float32(THETA) ** (-np.arange(half, dtype=np.float32) / np.float32(half))
    cos, sin = np.cos(angle).astype(np.float32), np.sin(angle).astype(np.float32)
    return np.concatenate([cos, cos], 1), np.concatenate([-sin, sin], 1)


def _normed(wide):
    return wide * lax.rsqrt(jnp.mean(wide * wide, -1, keepdims=True) + 1e-6)


def _turn(t, c, s):
    t = t.astype(BF).astype(F32)
    parts = [t[:, at : at + HEAD] for at in range(0, t.shape[1], HEAD)]
    return jnp.concatenate([x * c + pltpu.roll(x, HEAD // 2, 1) * s for x in parts], 1).astype(BF)


def _hidden(s):
    n = s.shape[0]
    low = s[n - T :]
    ok = lax.broadcasted_iota(jnp.int32, (T, T), 0) <= lax.broadcasted_iota(jnp.int32, (T, T), 1)
    low = jnp.where(ok, low, -1e30)
    return low if n == T else jnp.concatenate([s[: n - T], low], 0)


def _attention(x_ref, wq_ref, wk_ref, wv_ref, wo_ref, c_ref, s_ref, q_ref, k_ref, v_ref, o_ref, lse_ref, at_ref, h_ref, b_ref, bt_ref, a_s, acc):
    i, tokens = pl.program_id(0), x_ref.shape[0]
    rows = [slice(r, r + T) for r in range(0, tokens, T)]
    e = HEAD**-0.5 * LOG2E

    @pl.when(i == 0)
    def _():
        for r in rows:
            a = _normed(x_ref[r].astype(F32)).astype(BF)
            a_s[r] = a
            at_ref[:, r] = a.T

    for r in rows:
        a = a_s[r]
        q_ref[r] = _turn(_dot(a, wq_ref[...], 1, 0), c_ref[r], s_ref[r])
        k_ref[r] = _turn(_dot(a, wk_ref[...], 1, 0), c_ref[r], s_ref[r])
        v_ref[r] = _dot(a, wv_ref[...], 1, 0).astype(BF)
    heads = [(n, slice(n * HEAD, (n + 1) * HEAD)) for n in range(q_ref.shape[1] // HEAD)]
    for r in rows:
        keys = slice(0, r.stop)
        scores = [_hidden(_dot(k_ref[keys, cols], q_ref[r, cols], 1, 1)) for _, cols in heads]
        tops = [s.max(axis=0, keepdims=True) for s in scores]
        weights = [jnp.exp2((s - top) * e).astype(BF) for s, top in zip(scores, tops)]
        for (n, cols), p, top in zip(heads, weights, tops):
            values = jnp.concatenate([v_ref[keys, cols].T, jnp.ones((8, r.stop), BF)], 0)
            mix = _dot(values, p, 1, 0)
            total = mix[HEAD : HEAD + 1]
            o_ref[r, cols] = (mix[:HEAD] * (1 / total)).T.astype(BF)
            lse_ref[0, n : n + 1, r] = top * e + jnp.log(total) * LOG2E
    for r in rows:
        part = _dot(o_ref[r], wo_ref[...], 1, 0)

        @pl.when(i == 0)
        def _():
            acc[r] = part

        @pl.when(i > 0)
        def _():
            acc[r] += part

    @pl.when(i == pl.num_programs(0) - 1)
    def _():
        for r in rows:
            h = x_ref[r] + acc[r].astype(BF)
            h_ref[r] = h
            b = _normed(h.astype(F32)).astype(BF)
            b_ref[r] = b
            bt_ref[:, r] = b.T


def _once(shape):
    return pl.BlockSpec(shape, lambda i: (0,) * len(shape), pipeline_mode=pl.Buffered(1))


def attention(x, wq, wk, wv, wo):
    tokens, d = x.shape
    wide = 2 * HEAD
    steps = wq.shape[1] // wide
    c, s = _turns(tokens)
    cols = pl.BlockSpec((tokens, wide), lambda i: (0, i))
    weights = pl.BlockSpec((d, wide), lambda i: (0, i))
    like = jax.ShapeDtypeStruct((tokens, d), BF)
    return pl.pallas_call(
        _attention,
        grid=(steps,),
        in_specs=[_once((tokens, d)), weights, weights, weights, pl.BlockSpec((wide, d), lambda i: (i, 0)), _once(c.shape), _once(s.shape)],
        out_specs=[cols] * 4 + [pl.BlockSpec((1, 8, tokens), lambda i: (i, 0, 0))] + [_once((tokens, d))] * 4,
        out_shape=[like] * 4 + [jax.ShapeDtypeStruct((steps, 8, tokens), F32)] + [like] * 4,
        scratch_shapes=[pltpu.VMEM((tokens, d), BF), pltpu.VMEM((tokens, d), F32)],
        compiler_params=pltpu.CompilerParams(dimension_semantics=("arbitrary",), vmem_limit_bytes=VMEM),
        cost_estimate=pl.CostEstimate(flops=8 * tokens * d * d + 4 * tokens * tokens * d, transcendentals=tokens * tokens * 8, bytes_accessed=24 * 2**20),
        name="attention_forward",
    )(x, wq, wk, wv, wo, jnp.asarray(c), jnp.asarray(s))


def adamw(w, m, v, g):
    m = 0.9 * m + 0.1 * g
    v = 0.95 * v + 0.05 * g * g
    step = m * lax.rsqrt(v + 1e-8) + 0.1 * w
    return (w - 0.02 * step).astype(jnp.bfloat16), m, v


RING = 4
STRIDE = {"x": 32, "y": 8, "z": 2}
COLOURS = (("x", "y", "z"), ("y", "z", "x"), ("z", "x", "y"))
TICKS = 4
AT = (0, 1, 3, 5, 7, 9, 11, 13, 15, 17, 20, 22, 24)
LAG = AT[-1] // TICKS + 1


class Sum:
    def __init__(self, colour, blk, local, out, refs, sems, slot):
        self.c, (self.R, self.C), self.slot = colour, blk, slot
        self.local, self.out = local, out
        self.rc, self.s, self.sa1, self.ra1, self.sa2, self.ra2, self.ra, self.sb1, self.rb1, self.sb2, self.rb2, self.rb, self.sc, self.rcc, self.sg = refs
        self.send, self.recv, self.gather = sems
        me = lax.axis_index("dp")
        self.me, self.core = me, lax.rem(me, 2)
        self.partner = me + 1 - 2 * self.core
        place = lambda axis: lax.rem(lax.div(me, STRIDE[axis]), RING)
        self.a, self.b, self.k = (place(axis) for axis in COLOURS[colour])

    def peer(self, n, by):
        axis, at = COLOURS[self.c][n], (self.a, self.b, self.k)[n]
        return self.me + (lax.rem(at + by + RING, RING) - at) * STRIDE[axis]

    def copy(self, src, dst, kind, device, slot=None, r=None):
        recv = self.recv.at[self.c, kind, slot] if r is None else self.gather.at[self.c, kind - 6, r]
        return pltpu.make_async_remote_copy(src, dst, self.send.at[self.c, kind], recv, device_id={"dp": device})

    def wait(self, ref, kind, slot=None, r=None, send=None):
        recv = self.recv.at[self.c, kind, slot] if r is None else self.gather.at[self.c, kind - 6, r]
        pltpu.make_async_copy(ref, ref, recv).wait()
        ref = ref if send is None else send
        pltpu.make_async_copy(ref, ref, self.send.at[self.c, kind]).wait()

    def rows(self, q, n):
        return pl.ds(pl.multiple_of(q * n, 16), n)

    def cols(self, q):
        return pl.ds(pl.multiple_of(q * (self.C // 4), 128), self.C // 4)

    def region(self, r, level):
        first = self.core * (self.R // 2)
        if level > 0:
            first = first + self.a * (self.R // 8)
        if level > 1:
            first = first + self.b * (self.R // 32)
        return first

    def stage(self, n, r):
        R, C = self.R, self.C
        slot = self.slot(r)
        n8, n32, half = R // 8, R // 32, C // 2
        left, right = pl.ds(0, half), pl.ds(half, half)
        f32 = lambda v: v.astype(F32)
        low = lambda v: v.astype(BF)
        if n == 0:
            self.copy(self.local.at[slot, self.rows(1 - self.core, R // 2)], self.rc.at[slot], 0, self.partner, slot).start()
        elif n == 1:
            self.wait(self.rc.at[slot], 0, slot)
            for at in range(0, R // 2, n8):
                self.s[pl.ds(at, n8)] = f32(self.local[slot, self.rows(self.core * (R // 2 // n8) + at // n8, n8)]) + f32(self.rc[slot, pl.ds(at, n8)])
            self.sa1[...] = low(self.s[self.rows(lax.rem(self.a + 2, RING), n8)])
            self.both(self.sa1, self.ra1, 1, 0, slot, left, right)
        elif n == 2:
            self.wait(self.ra1.at[slot], 1, slot)
            self.second(self.s, self.a, n8, self.ra1, self.sa2, slot, half)
            self.pair(self.sa2, self.ra2, 2, 0, slot)
        elif n == 3:
            self.wait(self.ra2.at[slot], 2, slot)
            self.ra[...] = self.s[self.rows(self.a, n8)] + f32(self.ra2[slot, 0]) + f32(self.ra2[slot, 1])
            self.sb1[...] = low(self.ra[self.rows(lax.rem(self.b + 2, RING), n32)])
            self.both(self.sb1, self.rb1, 3, 1, slot, left, right)
        elif n == 4:
            self.wait(self.rb1.at[slot], 3, slot)
            self.second(self.ra, self.b, n32, self.rb1, self.sb2, slot, half)
            self.pair(self.sb2, self.rb2, 4, 1, slot)
        elif n == 5:
            self.wait(self.rb2.at[slot], 4, slot)
            total = self.ra[self.rows(self.b, n32)] + f32(self.rb2[slot, 0]) + f32(self.rb2[slot, 1])
            self.rb[...] = total
            self.sc[...] = low(total)
            for by in (1, 2, 3):
                to = lax.rem(self.k + by, RING)
                self.copy(self.sc.at[:, self.cols(to)], self.rcc.at[slot, by - 1], 5, self.peer(2, by), slot).start()
        elif n == 6:
            self.wait(self.rcc.at[slot], 5, slot)
            total = self.rb[:, self.cols(self.k)]
            for by in range(3):
                total = total + f32(self.rcc[slot, by])
            self.sg[...] = low(total)
            mine = self.out(r, self.region(r, 2), n32).at[:, self.cols(self.k)]
            pltpu.make_async_copy(self.sg, mine, self.gather.at[self.c, 0, r]).start()
            for by in (1, 2, 3):
                self.copy(self.sg, mine, 6, self.peer(2, by), r=r).start()
        elif n == 7:
            mine = self.out(r, self.region(r, 2), n32)
            self.wait(mine, 6, r=r, send=self.rcc.at[slot])
            for by in (1, -1):
                self.copy(mine, mine, 7, self.peer(1, by), r=r).start()
        elif n == 8:
            self.wait(self.out(r, 0, 2 * n32), 7, r=r)
            self.onward(r, 8, 1, self.region(r, 1), self.b, n32, left, right)
        elif n == 9:
            self.wait(self.out(r, 0, n32), 8, r=r)
            mine = self.out(r, self.region(r, 1), n8)
            for by in (1, -1):
                self.copy(mine, mine, 9, self.peer(0, by), r=r).start()
        elif n == 10:
            self.wait(self.out(r, 0, 2 * n8), 9, r=r)
            self.onward(r, 10, 0, self.region(r, 0), self.a, n8, left, right)
        elif n == 11:
            self.wait(self.out(r, 0, n8), 10, r=r)
            mine = self.out(r, self.region(r, 0), R // 2)
            self.copy(mine, mine, 11, self.partner, r=r).start()
        else:
            self.wait(self.out(r, 0, R // 2), 11, r=r)

    def both(self, src, dst, kind, axis, slot, left, right):
        self.copy(src.at[:, left], dst.at[slot, :, left], kind, self.peer(axis, 1), slot).start()
        self.copy(src.at[:, right], dst.at[slot, :, right], kind, self.peer(axis, -1), slot).start()

    def second(self, total, at, n, came, out, slot, half):
        up, down = self.rows(lax.rem(at + 1, RING), n), self.rows(lax.rem(at + 3, RING), n)
        out[0, :, :half] = (total[up, :half] + came[slot, :, :half].astype(F32)).astype(BF)
        out[0, :, half:] = total[up, half:].astype(BF)
        out[1, :, :half] = total[down, :half].astype(BF)
        out[1, :, half:] = (total[down, half:] + came[slot, :, half:].astype(F32)).astype(BF)

    def pair(self, src, dst, kind, axis, slot):
        self.copy(src.at[0], dst.at[slot, 0], kind, self.peer(axis, 1), slot).start()
        self.copy(src.at[1], dst.at[slot, 1], kind, self.peer(axis, -1), slot).start()

    def onward(self, r, kind, axis, first, at, n, left, right):
        before = self.out(r, first + lax.rem(at + 3, RING) * n, n).at[:, left]
        after = self.out(r, first + lax.rem(at + 1, RING) * n, n).at[:, right]
        self.copy(before, before, kind, self.peer(axis, 1), r=r).start()
        self.copy(after, after, kind, self.peer(axis, -1), r=r).start()


def _sum_scratch(R, C):
    n2, n8, n32 = R // 2, R // 8, R // 32
    return [pltpu.VMEM(shape, kind) for shape, kind in (
        ((2, n2, C), BF), ((n2, C), F32), ((n8, C), BF), ((2, n8, C), BF), ((2, n8, C), BF), ((2, 2, n8, C), BF), ((n8, C), F32),
        ((n32, C), BF), ((2, n32, C), BF), ((2, n32, C), BF), ((2, 2, n32, C), BF), ((n32, C), F32), ((n32, C), BF), ((2, 3, n32, C // 4), BF),
        ((n32, C // 4), BF))]


def _meet():
    me = lax.axis_index("dp")
    sem = pltpu.get_barrier_semaphore()
    pl.semaphore_signal(sem, 1, device_id={"dp": me + 1 - 2 * lax.rem(me, 2)})
    for stride in STRIDE.values():
        at = lax.rem(lax.div(me, stride), RING)
        for by in (1, 2, 3):
            pl.semaphore_signal(sem, 1, device_id={"dp": me + (lax.rem(at + by, RING) - at) * stride})
    pl.semaphore_wait(sem, 1 + 3 * 3)


def _stages(step, sums, tick, on):
    for n in reversed(range(len(AT))):
        if AT[n] % TICKS == tick:
            r = step - 1 - AT[n] // TICKS
            for c, one in enumerate(sums):

                @pl.when((r >= 0) & on(c, r))
                def _():
                    one.stage(n, r)


DOWN, UP = (512, 1024), (1024, 512)
SHAPES = (DOWN, UP, UP)
FEEDS = 8
LAST = (FEEDS + 1, FEEDS + 3, FEEDS + 3)
ROUNDS = FEEDS + 4


def _slot(c, r):
    return lax.rem(r if c == 0 else r + lax.div(r, FEEDS + 1), 2)


def _backward(b_hbm, bt_hbm, dy_hbm, h_hbm, at_hbm, q_hbm, k_hbm, v_hbm, o_hbm, wo_hbm, lse_ref, c_ref, s_ref, wg_ref, wu_ref, wd_ref,
              rows_out, cols_out, *scratch):
    n = 15
    parts, rest = [scratch[i * n : (i + 1) * n] for i in range(3)], scratch[3 * n :]
    x1, x2, x3, x4, q, k, v, o, wo, dvs, act, dg, du, acc, l0, l1, l2, send, recv, gather, load = rest
    i = pl.program_id(0)
    tokens = x1.shape[0]
    rows = [slice(r, r + T) for r in range(0, tokens, T)]
    scale = HEAD**-0.5
    e = scale * LOG2E
    (R0, C0), (R1, C1), _ = SHAPES
    outs = (
        lambda r, first, size: rows_out.at[pl.ds(pl.multiple_of(r * R0 + first, 16), size)],
        lambda r, first, size: cols_out.at[pl.ds(pl.multiple_of(first, 16), size), pl.ds(pl.multiple_of(r * C1, 128), C1)],
        lambda r, first, size: cols_out.at[pl.ds(pl.multiple_of(first, 16), size), pl.ds(pl.multiple_of((r + ROUNDS) * C1, 128), C1)],
    )
    locals_ = (l0, l1, l2)
    sums = [Sum(c, SHAPES[c], locals_[c], outs[c], parts[c], (send, recv, gather), functools.partial(_slot, c)) for c in range(3)]
    s0, s1 = _slot(0, i), _slot(1, i)

    def fetch(n, src, dst):
        return pltpu.make_async_copy(src, dst, load.at[n])

    first = [(0, b_hbm, x1), (1, dy_hbm, x2), (2, bt_hbm, x3)]
    later = [(3, h_hbm, x4), (4, o_hbm, o), (5, wo_hbm, wo), (6, q_hbm, q), (7, k_hbm, k), (8, v_hbm, v)]

    @pl.when(i == 0)
    def _():
        for one in first:
            fetch(*one).start()
        _meet()
        acc[...] = jnp.zeros_like(acc)
        for one in first:
            fetch(*one).wait()
        for one in later:
            fetch(*one).start()

    def units(r):
        b = x1[r]
        gate, up = _dot(b, wg_ref[...], 1, 0), _dot(b, wu_ref[...], 1, 0)
        da = _dot(x2[r], wd_ref[...], 1, 1).astype(BF).astype(F32)
        sig = 1 / (1 + jnp.exp2(gate * -LOG2E))
        silu = gate * sig
        act[r] = (silu * up).astype(BF)
        du[r] = (da * silu).astype(BF)
        dg[r] = (da * up * (sig + silu * (1 - sig))).astype(BF)

    def inward(r):
        acc[r] += _dot(dg[r], wg_ref[...], 1, 1) + _dot(du[r], wu_ref[...], 1, 1)

    def norm_back():
        for r in rows:
            wide, ct = x4[r].astype(F32), acc[r].astype(BF).astype(F32)
            scale = lax.rsqrt(jnp.mean(wide * wide, -1, keepdims=True) + 1e-6)
            back = ct * scale - wide * (scale * scale * scale * jnp.mean(ct * wide, -1, keepdims=True))
            x2[r] = x2[r] + back.astype(BF)

    def head(n, place):
        cols = pl.ds(pl.multiple_of(n * HEAD, HEAD), HEAD)
        to = slice(place * HEAD, (place + 1) * HEAD)
        dk, dv = slice(0, HEAD), slice(HEAD, 2 * HEAD)
        for r in reversed(rows):
            keys = slice(0, r.stop)
            dor, qr = x1[r, cols], q[r, cols]
            delta = (dor.astype(F32) * o[r, cols].astype(F32)).T.sum(axis=0, keepdims=True)
            lse = lse_ref[lax.div(n, 2), pl.ds(lax.rem(n, 2), 1), r]
            s = _hidden(_dot(k[keys, cols], qr, 1, 1) * e - lse)
            p = jnp.exp2(s)
            ds = (p * (_dot(v[keys, cols], dor, 1, 1) - delta)).astype(BF)
            if r.stop == tokens:
                acc[keys, dv] = _dot(p.astype(BF), dor, 1, 0)
                acc[keys, dk] = _dot(ds, qr, 1, 0)
            else:
                acc[keys, dv] += _dot(p.astype(BF), dor, 1, 0)
                acc[keys, dk] += _dot(ds, qr, 1, 0)
            t = (_dot(k[keys, cols], ds, 0, 0) * scale).T.astype(BF).astype(F32)
            dg[r, to] = (t * c_ref[r] - pltpu.roll(t, HEAD // 2, 1) * s_ref[r]).astype(BF)
        dvs[:, cols] = acc[:, dv].astype(BF)
        t = (acc[:, dk] * scale).astype(BF).astype(F32)
        du[:, to] = (t * c_ref[...] - pltpu.roll(t, HEAD // 2, 1) * s_ref[...]).astype(BF)

    feeding = i < FEEDS
    attending = (i == FEEDS + 1) | (i == FEEDS + 2)
    for tick in range(TICKS):
        _stages(i, sums, tick, lambda c, r: (r <= LAST[c]) if c == 0 else (r <= LAST[c]) & (r != FEEDS))

        @pl.when(feeding)
        def _():
            if tick < 2:
                units(rows[2 * tick])
                units(rows[2 * tick + 1])
            elif tick == 2:
                l0[s0] = _dot(act[...], x2[...], 0, 0).astype(BF)
                l1[s1] = _dot(x3[...], dg[...], 1, 0).astype(BF)
                inward(rows[0])
            else:
                l2[s1] = _dot(x3[...], du[...], 1, 0).astype(BF)
                for r in rows[1:]:
                    inward(r)

        @pl.when(i == FEEDS)
        def _():
            if tick == 0:
                for one in later:
                    fetch(*one).wait()
                norm_back()
                fetch(9, at_hbm, x3).start()
            elif tick == 1:
                for r in rows:
                    x1[r] = _dot(x2[r], wo[...], 1, 1).astype(BF)
            elif tick == 2:
                l0[FEEDS % 2] = _dot(o[:, : F], x2[...], 0, 0).astype(BF)
                l0[1 - FEEDS % 2] = _dot(o[:, F:], x2[...], 0, 0).astype(BF)
            else:
                fetch(9, at_hbm, x3).wait()

        @pl.when(attending)
        def _():
            head((i - FEEDS - 1) * TICKS + tick, tick)
            if tick == TICKS - 1:
                l1[s1] = _dot(x3[...], dg[...], 1, 0).astype(BF)
                l2[s1] = _dot(x3[...], du[...], 1, 0).astype(BF)

        if tick == TICKS - 1:

            @pl.when(i == FEEDS + 2)
            def _():
                l1[1 - s1] = _dot(x3[...], dvs[:, : F], 1, 0).astype(BF)
                l2[1 - s1] = _dot(x3[...], dvs[:, F:], 1, 0).astype(BF)


def backward(dy, w, q, k, v, o, lse, at, h, b, bt):
    tokens, d = dy.shape
    c, s = _turns(tokens)
    hbm = pl.BlockSpec(memory_space=pl.ANY)
    last = FEEDS - 1
    feed = pl.BlockSpec(UP, lambda i: (0, jnp.minimum(i, last)))
    square = pltpu.VMEM((tokens, d), BF)
    return pl.pallas_call(
        _backward,
        grid=(ROUNDS + 1 + AT[-1] // TICKS,),
        in_specs=[hbm] * 10 + [_once(lse.shape), _once(c.shape), _once(s.shape), feed, feed, pl.BlockSpec(DOWN, lambda i: (jnp.minimum(i, last), 0))],
        out_specs=[hbm] * 2,
        out_shape=[jax.ShapeDtypeStruct((DOWN[0] * (LAST[0] + 1), DOWN[1]), BF), jax.ShapeDtypeStruct((UP[0], 2 * ROUNDS * UP[1]), BF)],
        scratch_shapes=[one for shape in SHAPES for one in _sum_scratch(*shape)]
        + [square] * 10
        + [pltpu.VMEM((tokens, F), BF)] * 3
        + [pltpu.VMEM((tokens, d), F32)]
        + [pltpu.VMEM((2, *shape), BF) for shape in SHAPES]
        + [pltpu.SemaphoreType.DMA((3, 12)), pltpu.SemaphoreType.DMA((3, 6, 2)), pltpu.SemaphoreType.DMA((3, 6, ROUNDS)), pltpu.SemaphoreType.DMA((10,))],
        compiler_params=pltpu.CompilerParams(dimension_semantics=("arbitrary",), vmem_limit_bytes=VMEM, collective_id=0, has_side_effects=True),
        cost_estimate=pl.CostEstimate(flops=10**11, transcendentals=0, bytes_accessed=2**28),
        name="backward_and_sum",
    )(b, bt, dy, h, at, q, k, v, o, w["wo"], lse, jnp.asarray(c), jnp.asarray(s), w["w_gate"], w["w_up"], w["w_down"])


def solution(mesh):
    def step(x, dy, *arrays):
        weights, m, v = (dict(zip(NAMES, arrays[i : i + 7], strict=True)) for i in (0, 7, 14))
        w = {n: w[0] for n, w in weights.items()}
        rows, cols = backward(dy[0], w, *attention(x[0], w["wq"], w["wk"], w["wv"], w["wo"]))
        block = lambda at, n: cols[:, at * UP[1] : (at + n) * UP[1]]
        cut, at = FEEDS * DOWN[0], FEEDS + 1
        summed = {
            "w_down": rows[:cut], "wo": rows[cut:], "w_gate": block(0, FEEDS), "w_up": block(ROUNDS, FEEDS), "wq": block(at, 2),
            "wk": block(ROUNDS + at, 2), "wv": jnp.concatenate([block(at + 2, 1), block(ROUNDS + at + 2, 1)], 1),
        }
        new = {name: adamw(weights[name].astype(F32), m[name], v[name], summed[name][None].astype(F32)) for name in NAMES}
        return tuple(new[name][which] for which in range(3) for name in NAMES)

    states, all_of = P(("rep", "dp"), None, None), P(None, None, None)
    return jax.shard_map(
        step,
        mesh=mesh,
        in_specs=(states, states) + (all_of,) * 21,
        out_specs=(P("rep", None, None),) * 21,
        check_vma=False,
    )
```

```python
import functools

import jax
import jax.numpy as jnp
import numpy as np
from jax import lax
from jax.experimental import pallas as pl
from jax.experimental.pallas import tpu as pltpu
from jax.sharding import PartitionSpec as P

HEAD = 128
THETA = 10000
NAMES = ("wq", "wk", "wv", "wo", "w_gate", "w_up", "w_down")
LOG2E = 1.4426950408889634
T = 256
F = 512
VMEM = 67043328
BF, F32 = jnp.bfloat16, jnp.float32


def _dots(ca, cb):
    return lambda a, b: lax.dot_general(a, b, (((ca,), (cb,)), ((), ())), preferred_element_type=F32)


_nn, _nt, _tn = _dots(1, 0), _dots(1, 1), _dots(0, 0)


def _turns(tokens):
    half = HEAD // 2
    angle = np.arange(tokens, dtype=np.float32)[:, None] * np.float32(THETA) ** (-np.arange(half, dtype=np.float32) / np.float32(half))
    return np.concatenate([np.cos(angle), np.sin(angle)], 1).astype(np.float32)


def _both(t):
    low, other = lax.broadcasted_iota(jnp.int32, t.shape, 1) < HEAD // 2, pltpu.roll(t, HEAD // 2, 1)
    return jnp.where(low, t, other), jnp.where(low, -other, t)


def _normed(wide):
    return wide * lax.rsqrt(jnp.mean(wide * wide, -1, keepdims=True) + 1e-6)


def _turn(t, c, s):
    t = t.astype(BF).astype(F32)
    parts = [t[:, at : at + HEAD] for at in range(0, t.shape[1], HEAD)]
    return jnp.concatenate([x * c + pltpu.roll(x, HEAD // 2, 1) * s for x in parts], 1).astype(BF)


def _hidden(s):
    n = s.shape[0]
    low = s[n - T :]
    ok = lax.broadcasted_iota(jnp.int32, (T, T), 0) <= lax.broadcasted_iota(jnp.int32, (T, T), 1)
    low = jnp.where(ok, low, -1e30)
    return low if n == T else jnp.concatenate([s[: n - T], low], 0)


def _adamw(w, m, v, g):
    m = 0.9 * m + 0.1 * g
    v = 0.95 * v + 0.05 * g * g
    step = m * lax.rsqrt(v + 1e-8) + 0.1 * w
    return (w - 0.02 * step).astype(BF), m, v


TILE = (256, 1024)
DEEP = 4
CHUNK = 16


def _optimizer(*refs, where):
    n = len(where)
    w, m, v = refs[:n], refs[n : 2 * n], refs[2 * n : 3 * n]
    g, refs = refs[3 * n : 3 * n + 2], refs[3 * n + 2 :]
    out, (wi, mi, vi, gi, wn, mn, vn, came, left) = (refs[:n], refs[n : 2 * n], refs[2 * n : 3 * n]), refs[3 * n :]
    rows, cols = TILE
    tiles = [(one.shape[0] // rows) * (one.shape[1] // cols) for one in w]
    first = [sum(tiles[:j]) for j in range(n + 1)]

    def part(j, t):
        across = w[j].shape[1] // cols
        return lax.div(t, across) * rows, lax.rem(t, across) * cols

    def tile(ref, row, col):
        return ref.at[pl.ds(pl.multiple_of(row, rows), rows), pl.ds(pl.multiple_of(col, 512), cols)]

    def loads(j, t, slot):
        row, col = part(j, t)
        at, r0, c0 = where[j]
        pairs = ((tile(w[j], row, col), wi), (tile(m[j], row, col), mi), (tile(v[j], row, col), vi), (tile(g[at], r0 + row, c0 + col), gi))
        return [pltpu.make_async_copy(src, dst.at[slot], came.at[k, slot]) for k, (src, dst) in enumerate(pairs)]

    def stores(j, t, slot):
        row, col = part(j, t)
        pairs = zip((wn, mn, vn), (tile(o[j], row, col) for o in out), strict=True)
        return [pltpu.make_async_copy(src.at[slot], dst, left.at[k, slot]) for k, (src, dst) in enumerate(pairs)]

    for k in range(DEEP - 1):
        for copy in loads(0, k, k):
            copy.start()
    for j in range(n):

        def body(t, _, j=j):
            k = first[j] + t
            slot = lax.rem(k, DEEP)
            ahead = t + DEEP - 1
            for other in (j, j + 1):
                if other < n:
                    index = ahead if other == j else ahead - tiles[j]

                    @pl.when((index >= 0) & (index < tiles[other]) & (ahead < tiles[j] if other == j else ahead >= tiles[j]))
                    def _():
                        for copy in loads(other, index, lax.rem(k + DEEP - 1, DEEP)):
                            copy.start()
            for copy in loads(j, t, slot):
                copy.wait()

            @pl.when(k >= DEEP)
            def _():
                for copy in stores(0, 0, slot):
                    copy.wait()

            def chunk(c, _):
                r = pl.ds(pl.multiple_of(c * CHUNK, CHUNK), CHUNK)
                wn[slot, r], mn[slot, r], vn[slot, r] = _adamw(wi[slot, r].astype(F32), mi[slot, r], vi[slot, r], gi[slot, r].astype(F32))

            lax.fori_loop(0, rows // CHUNK, chunk, None)
            for copy in stores(j, t, slot):
                copy.start()

        lax.fori_loop(0, tiles[j], body, None)
    for k in range(DEEP):
        for copy in stores(0, 0, k):
            copy.wait()


def optimizer(w, m, v, sums, where):
    like = [jax.ShapeDtypeStruct(one.shape, one.dtype) for one in (*w, *m, *v)]
    hbm, n = pl.BlockSpec(memory_space=pl.ANY), len(w)
    new = pl.pallas_call(
        functools.partial(_optimizer, where=where),
        in_specs=[hbm] * (3 * n + 2),
        out_specs=[hbm] * (3 * n),
        out_shape=like,
        scratch_shapes=[pltpu.VMEM((DEEP, *TILE), kind) for kind in (BF, F32, F32, BF, BF, F32, F32)]
        + [pltpu.SemaphoreType.DMA((4, DEEP)), pltpu.SemaphoreType.DMA((3, DEEP))],
        compiler_params=pltpu.CompilerParams(vmem_limit_bytes=VMEM),
        cost_estimate=pl.CostEstimate(flops=16 * 2**24, transcendentals=2**24, bytes_accessed=22 * 2**24),
        name="optimizer",
    )(*w, *m, *v, *sums)
    return new[:n], new[n : 2 * n], new[2 * n :]


RING = 4
SHIFT = {"x": 5, "y": 3, "z": 1}
COLOURS = (("x", "y", "z"), ("y", "z", "x"), ("z", "x", "y"), ("x", "y", "z"))
TICKS = 4
AT = (0, 2, 3, 5, 7, 8, 11, 12, 15, 17, 20, 24, 28)


class Place:
    def __init__(self):
        me = lax.axis_index("dp")
        self.core = me & 1
        self.partner = me ^ 1
        self.at = {axis: (me >> shift) & 3 for axis, shift in SHIFT.items()}
        self.peers = {axis: {by: me + ((((self.at[axis] + by) & 3) - self.at[axis]) << shift) for by in (1, 2, 3)} for axis, shift in SHIFT.items()}

    def here(self):
        self.everyone = [self.partner] + [peer for axis in SHIFT for peer in self.peers[axis].values()]
        for peer in self.everyone:
            pl.semaphore_signal(pltpu.get_barrier_semaphore(), 1, device_id={"dp": peer})

    def meet(self):
        pl.semaphore_wait(pltpu.get_barrier_semaphore(), 1 + len(SHIFT) * (RING - 1))


class Sum:
    def __init__(self, colour, blk, place, local, out, refs, sems, slot, slot3):
        self.c, (self.R, self.C), self.slot, self.slot3, self.place = colour, blk, slot, slot3, place
        self.local, self.out = local, out
        self.rc, self.sa1, self.ra1, self.sa2, self.ra2, self.ra, self.sb1, self.rb1, self.sb2, self.rb2, self.rb, self.sc, self.rcc, self.all = refs
        self.send, self.recv, self.gather = sems
        self.core = place.core
        self.a, self.b, self.k = (place.at[axis] for axis in COLOURS[colour])
        self.first = (self.core * (self.R // 2), self.core * (self.R // 2) + self.a * (self.R // 8))
        self.first += (self.first[1] + self.b * (self.R // 32),)

    def peer(self, n, by):
        return self.place.peers[COLOURS[self.c][n]][by]

    def copy(self, src, dst, kind, device, slot=None, r=None):
        recv = self.recv.at[self.c, kind, slot] if r is None else self.gather.at[self.c, kind - 6, r]
        return pltpu.make_async_remote_copy(src, dst, self.send.at[self.c, kind], recv, device_id={"dp": device})

    def wait(self, ref, kind, slot=None, r=None, send=None):
        recv = self.recv.at[self.c, kind, slot] if r is None else self.gather.at[self.c, kind - 6, r]
        pltpu.make_async_copy(ref, ref, recv).wait()
        ref = ref if send is None else send
        pltpu.make_async_copy(ref, ref, self.send.at[self.c, kind]).wait()

    def quarter(self, r, by, half=None):
        n8 = self.R // 8
        q = (self.a + by) & 3
        cols = slice(None) if half is None else pl.ds(half * (self.C // 2), self.C // 2)
        mine = self.local[self.slot(r), pl.ds(pl.multiple_of(self.first[0] + q * n8, 16), n8), cols]
        return mine.astype(F32) + self.rc[self.slot3(r), pl.ds(pl.multiple_of(q * n8, 16), n8), cols].astype(F32)

    def cols(self, q):
        return pl.ds(pl.multiple_of(q * (self.C // 4), 128), self.C // 4)

    def stage(self, n, r):
        R, C = self.R, self.C
        slot = self.slot(r)
        n8, n32, half = R // 8, R // 32, C // 2
        left, right = pl.ds(0, half), pl.ds(half, half)
        f32 = lambda v: v.astype(F32)
        low = lambda v: v.astype(BF)
        if n == 0:
            other = pl.ds(pl.multiple_of((1 - self.core) * (R // 2), 16), R // 2)
            self.copy(self.local.at[slot, other], self.rc.at[self.slot3(r)], 0, self.place.partner, slot).start()
        elif n == 1:
            self.wait(self.rc.at[self.slot3(r)], 0, slot)
            self.sa1[:] = low(self.quarter(r, 2))
            self.both(self.sa1, self.ra1, 1, 0, slot, left, right)
        elif n == 2:
            self.wait(self.ra1.at[slot], 1, slot)
            self.sa2[0, :, :half] = low(self.quarter(r, 1, 0) + f32(self.ra1[slot, :, :half]))
            self.sa2[0, :, half:] = low(self.quarter(r, 1, 1))
            self.sa2[1, :, :half] = low(self.quarter(r, 3, 0))
            self.sa2[1, :, half:] = low(self.quarter(r, 3, 1) + f32(self.ra1[slot, :, half:]))
            self.pair(self.sa2, self.ra2, 2, 0, slot)
        elif n == 3:
            self.wait(self.ra2.at[slot], 2, slot)
            self.ra[:] = self.quarter(r, 0) + f32(self.ra2[slot, 0]) + f32(self.ra2[slot, 1])
            self.sb1[:] = low(self.ra[self.sixteenth(2)])
            self.both(self.sb1, self.rb1, 3, 1, slot, left, right)
        elif n == 4:
            self.wait(self.rb1.at[slot], 3, slot)
            up, down = self.sixteenth(1), self.sixteenth(3)
            self.sb2[0, :, :half] = low(self.ra[up, :half] + f32(self.rb1[slot, :, :half]))
            self.sb2[0, :, half:] = low(self.ra[up, half:])
            self.sb2[1, :, :half] = low(self.ra[down, :half])
            self.sb2[1, :, half:] = low(self.ra[down, half:] + f32(self.rb1[slot, :, half:]))
            self.pair(self.sb2, self.rb2, 4, 1, slot)
        elif n == 5:
            self.wait(self.rb2.at[slot], 4, slot)
            total = self.ra[self.sixteenth(0)] + f32(self.rb2[slot, 0]) + f32(self.rb2[slot, 1])
            self.rb[:] = total
            self.sc[:] = low(total)
            for by in (1, 2, 3):
                to = (self.k + by) & 3
                self.copy(self.sc.at[:, self.cols(to)], self.rcc.at[slot, by - 1], 5, self.peer(2, by), slot).start()
        elif n == 6:
            self.wait(self.rcc.at[slot], 5, slot)
            total = self.rb[:, self.cols(self.k)]
            for by in range(3):
                total = total + f32(self.rcc[slot, by])
            self.all[r & 3, self.sixteenth(0), self.cols(self.k)] = low(total)
            mine = self.all.at[r & 3, self.sixteenth(0), self.cols(self.k)]
            for by in (1, 2, 3):
                self.copy(mine, mine, 6, self.peer(2, by), r=r).start()
        elif n == 7:
            self.wait(self.rcc.at[slot], 6, r=r)
            mine = self.all.at[r & 3, self.sixteenth(0)]
            for by in (1, 3):
                self.copy(mine, mine, 7, self.peer(1, by), r=r).start()
        elif n == 8:
            self.wait(self.all.at[r & 3, pl.ds(0, 2 * n32)], 7, r=r)
            self.onward(lambda by: self.all.at[r & 3, self.sixteenth(by)], r, 8, 1, left, right)
        elif n == 9:
            self.wait(self.all.at[r & 3, pl.ds(0, n32)], 8, r=r)
            whole, mine = self.all.at[r & 3], self.out(r, self.first[1], n8)
            pltpu.make_async_copy(whole, mine, self.gather.at[self.c, 3, r]).start()
            for by in (1, 3):
                self.copy(whole, mine, 9, self.peer(0, by), r=r).start()
        elif n == 10:
            self.wait(self.out(r, 0, 3 * n8), 9, r=r, send=self.out(r, 0, 2 * n8))
            self.onward(lambda by: self.out(r, self.first[0] + ((self.a + by) & 3) * n8, n8), r, 10, 0, left, right)
        elif n == 11:
            self.wait(self.out(r, 0, n8), 10, r=r)
            mine = self.out(r, self.first[0], R // 2)
            self.copy(mine, mine, 11, self.place.partner, r=r).start()
        else:
            self.wait(self.out(r, 0, R // 2), 11, r=r)

    def sixteenth(self, by):
        return pl.ds(pl.multiple_of(((self.b + by) & 3) * (self.R // 32), 16), self.R // 32)

    def both(self, src, dst, kind, axis, slot, left, right):
        self.copy(src.at[:, left], dst.at[slot, :, left], kind, self.peer(axis, 1), slot).start()
        self.copy(src.at[:, right], dst.at[slot, :, right], kind, self.peer(axis, 3), slot).start()

    def pair(self, src, dst, kind, axis, slot):
        self.copy(src.at[0], dst.at[slot, 0], kind, self.peer(axis, 1), slot).start()
        self.copy(src.at[1], dst.at[slot, 1], kind, self.peer(axis, 3), slot).start()

    def onward(self, part, r, kind, axis, left, right):
        before, after = part(3).at[:, left], part(1).at[:, right]
        self.copy(before, before, kind, self.peer(axis, 1), r=r).start()
        self.copy(after, after, kind, self.peer(axis, 3), r=r).start()


def _sum_scratch(R, C, deep):
    n2, n8, n32 = R // 2, R // 8, R // 32
    return [pltpu.VMEM(shape, kind) for shape, kind in (
        ((deep, n2, C), BF), ((n8, C), BF), ((2, n8, C), BF), ((2, n8, C), BF), ((2, 2, n8, C), BF), ((n8, C), F32),
        ((n32, C), BF), ((2, n32, C), BF), ((2, n32, C), BF), ((2, 2, n32, C), BF), ((n32, C), F32), ((n32, C), BF), ((2, 3, n32, C // 4), BF),
        ((4, n8, C), BF))]


SUM_REFS = 14


def _stages(step, sums, tick, on):
    for n in reversed(range(len(AT))):
        if AT[n] % TICKS == tick:
            r = step - 1 - AT[n] // TICKS
            for c, one in enumerate(sums):

                @pl.when(on(c, r))
                def _():
                    one.stage(n, r)


DOWN, UP = (512, 1024), (1024, 512)
SHAPES = (DOWN, UP, UP, UP)
PAIRS = 4
FEEDS = 8
ROUNDS = FEEDS + 3


def _has(c, r):
    if c == 0:
        return (r >= 0) & (r <= FEEDS + 1)
    if c == 3:
        return (r > FEEDS) & (r < ROUNDS)
    return (r >= 0) & (r < ROUNDS) & (r != FEEDS)


def _slots(c, n):
    if c in (0, 3):
        return lambda r: lax.rem(r, n)
    if n == 2:
        return lambda r: (r + jnp.where(r > FEEDS, 1, 0)) & 1
    return lambda r: lax.rem(r - jnp.where(r > FEEDS, 1, 0), n)


def _layer(x_hbm, dy_hbm, wo_hbm, t_ref, wq_ref, wk_ref, wv_ref, wg_ref, wu_ref, wd_ref, rows_out, cols_out, *scratch):
    n, colours = SUM_REFS, len(SHAPES)
    parts, rest = [scratch[c * n : (c + 1) * n] for c in range(colours)], scratch[colours * n :]
    locals_, (send, recv, gather, load), rest = rest[:colours], rest[colours : colours + 4], rest[colours + 4 :]
    x1, x2, x3, x4, q, k, v, o, wo, at, act, dg, du, acc, lses = rest
    l0, l1, l2, l3 = locals_
    i = pl.program_id(0) - PAIRS
    tokens = x1.shape[0]
    rows = [slice(r, r + T) for r in range(0, tokens, T)]
    scale = HEAD**-0.5
    e = scale * LOG2E

    def in_rows(r, first, size):
        return rows_out.at[pl.ds(pl.multiple_of(r * DOWN[0] + first, 16), size)]

    def in_cols(c):
        block = lambda r: (c - 1) * ROUNDS + r - (FEEDS + 1 if c == 3 else 0)
        return lambda r, first, size: cols_out.at[pl.ds(pl.multiple_of(first, 16), size), pl.ds(pl.multiple_of(block(r) * UP[1], 128), UP[1])]

    place = Place()
    sums = [Sum(c, SHAPES[c], place, locals_[c], in_cols(c) if c else in_rows, parts[c], (send, recv, gather), _slots(c, 2), _slots(c, 3 if c < 3 else 2))
            for c in range(colours)]
    s0, s1 = _slots(0, 2)(i), _slots(1, 2)(i)

    loads = [pltpu.make_async_copy(src, dst, load.at[n]) for n, (src, dst) in enumerate(((x_hbm, x4), (wo_hbm, wo), (dy_hbm, x2)))]

    @pl.when(i == -PAIRS)
    def _():
        for one in loads:
            one.start()
        place.here()
        loads[0].wait()
        for r in rows:
            a = _normed(x4[r].astype(F32)).astype(BF)
            x1[r] = a
            at[:, r] = a.T
        acc[:] = jnp.zeros_like(acc)

    @pl.when(i == 0)
    def _():
        place.meet()

    def forward():
        pair = i + PAIRS
        both = pl.ds(pl.multiple_of(pair * 2 * HEAD, 2 * HEAD), 2 * HEAD)
        heads = [(n, pl.ds(pl.multiple_of((pair * 2 + n) * HEAD, HEAD), HEAD)) for n in range(2)]
        for r in rows:
            a, turns = x1[r], _both(t_ref[r])
            q[r, both] = _turn(_nn(a, wq_ref[:]), *turns)
            k[r, both] = _turn(_nn(a, wk_ref[:]), *turns)
            v[r, both] = _nn(a, wv_ref[:]).astype(BF)
        for r in rows:
            keys = slice(0, r.stop)
            scores = [_hidden(_nt(k[keys, cols], q[r, cols])) for _, cols in heads]
            tops = [s.max(axis=0, keepdims=True) for s in scores]
            weights = [jnp.exp2((s - top) * e).astype(BF) for s, top in zip(scores, tops)]
            for (n, cols), p, top in zip(heads, weights, tops):
                mix = _nn(jnp.concatenate([v[keys, cols].T, jnp.ones((8, r.stop), BF)], 0), p)
                total = mix[HEAD : HEAD + 1]
                o[r, cols] = (mix[:HEAD] * (1 / total)).T.astype(BF)
                lses[pair, n : n + 1, r] = top * e + jnp.log(total) * LOG2E

    def onto_residual():
        loads[1].wait()
        for r in rows:
            h = x4[r] + _nn(o[r], wo[:]).astype(BF)
            x4[r] = h
            b = _normed(h.astype(F32)).astype(BF)
            x1[r] = b
            x3[:, r] = b.T
        loads[2].wait()

    def units(r):
        b = x1[r]
        gate, up = _nn(b, wg_ref[:]), _nn(b, wu_ref[:])
        da = _nt(x2[r], wd_ref[:]).astype(BF).astype(F32)
        sig = 1 / (1 + jnp.exp2(gate * -LOG2E))
        silu = gate * sig
        act[r] = (silu * up).astype(BF)
        du[r] = (da * silu).astype(BF)
        dg[r] = (da * up * (sig + silu * (1 - sig))).astype(BF)

    def inward(r):
        acc[r] += _nt(dg[r], wg_ref[:]) + _nt(du[r], wu_ref[:])

    def norm_back():
        for r in rows:
            wide, ct = x4[r].astype(F32), acc[r].astype(BF).astype(F32)
            scale = lax.rsqrt(jnp.mean(wide * wide, -1, keepdims=True) + 1e-6)
            back = ct * scale - wide * (scale * scale * scale * jnp.mean(ct * wide, -1, keepdims=True))
            dh = x2[r] + back.astype(BF)
            x2[r] = dh
            x1[r] = _nt(dh, wo[:]).astype(BF)

    def head(n, to):
        cols = pl.ds(pl.multiple_of(n * HEAD, HEAD), HEAD)
        to = pl.ds(pl.multiple_of(to * HEAD, HEAD), HEAD)
        dk, dv = slice(0, HEAD), slice(HEAD, 2 * HEAD)
        for r in reversed(rows):
            keys = slice(0, r.stop)
            dor, qr = x1[r, cols], q[r, cols]
            delta = (dor.astype(F32) * o[r, cols].astype(F32)).T.sum(axis=0, keepdims=True)
            lse = lses[lax.div(n, 2), pl.ds(n & 1, 1), r]
            s = _hidden(_nt(k[keys, cols], qr) * e - lse)
            p = jnp.exp2(s)
            ds = (p * (_nt(v[keys, cols], dor) - delta)).astype(BF)
            if r.stop == tokens:
                acc[keys, dv] = _nn(p.astype(BF), dor)
                acc[keys, dk] = _nn(ds, qr)
            else:
                acc[keys, dv] += _nn(p.astype(BF), dor)
                acc[keys, dk] += _nn(ds, qr)
            t = (_tn(k[keys, cols], ds) * scale).T.astype(BF).astype(F32)
            cos, sin = _both(t_ref[r])
            dg[r, to] = (t * cos - pltpu.roll(t, HEAD // 2, 1) * sin).astype(BF)
        for r in rows:
            act[r, to] = acc[r, dv].astype(BF)
            t = (acc[r, dk] * scale).astype(BF).astype(F32)
            cos, sin = _both(t_ref[r])
            du[r, to] = (t * cos - pltpu.roll(t, HEAD // 2, 1) * sin).astype(BF)

    feeding = (i >= 0) & (i < FEEDS)
    attending = (i == FEEDS + 1) | (i == FEEDS + 2)

    def ticking(tick, _):
        for one in range(TICKS):

            @pl.when(tick == one)
            def _():
                _stages(i, sums, one, _has)

        @pl.when((i < 0) & (tick == 0))
        def _():
            forward()

        @pl.when((i == -1) & (tick == 1))
        def _():
            onto_residual()

        @pl.when(feeding & (tick < 2))
        def _():
            for r in (0, T):
                units(pl.ds(pl.multiple_of(tick * 2 * T + r, T), T))

        @pl.when(feeding & (tick == 2))
        def _():
            l0[s0] = _tn(act[:], x2[:]).astype(BF)
            l1[s1] = _nn(x3[:], dg[:]).astype(BF)
            inward(rows[0])

        @pl.when(feeding & (tick == 3))
        def _():
            l2[s1] = _nn(x3[:], du[:]).astype(BF)
            for r in rows[1:]:
                inward(r)

        @pl.when((i == FEEDS) & (tick == 0))
        def _():
            norm_back()

        @pl.when(((i == FEEDS) | (i == FEEDS + 1)) & (tick == 2))
        def _():
            l0[s0] = _tn(o[:, pl.ds(pl.multiple_of((i - FEEDS) * F, F), F)], x2[:]).astype(BF)

        @pl.when(attending)
        def _():
            head((i - FEEDS - 1) * TICKS + tick, tick)

        @pl.when(attending & (tick == TICKS - 1))
        def _():
            l1[s1] = _nn(at[:], dg[:]).astype(BF)
            l2[s1] = _nn(at[:], du[:]).astype(BF)
            l3[s0] = _nn(at[:], act[:]).astype(BF)

    lax.fori_loop(0, TICKS, ticking, None)


def layer(x, dy, w):
    tokens, d = x.shape
    turns = _turns(tokens)
    hbm = pl.BlockSpec(memory_space=pl.ANY)
    upto = lambda i, n: jnp.clip(i, 0, n - 1)
    heads = pl.BlockSpec((d, 2 * HEAD), lambda i: (0, upto(i, PAIRS)))
    feed = pl.BlockSpec(UP, lambda i: (0, upto(i - PAIRS, FEEDS)))
    down = pl.BlockSpec(DOWN, lambda i: (upto(i - PAIRS, FEEDS), 0))
    dma, vmem = pltpu.SemaphoreType.DMA, pltpu.VMEM
    return pl.pallas_call(
        _layer,
        grid=(PAIRS + ROUNDS + 1 + AT[-1] // TICKS,),
        in_specs=[hbm] * 3 + [pl.BlockSpec(turns.shape, lambda i: (0, 0), pipeline_mode=pl.Buffered(1))] + [heads] * 3 + [feed, feed, down],
        out_specs=[hbm] * 2,
        out_shape=[jax.ShapeDtypeStruct((DOWN[0] * (FEEDS + 2), DOWN[1]), BF), jax.ShapeDtypeStruct((UP[0], (2 * ROUNDS + 2) * UP[1]), BF)],
        scratch_shapes=[one for c, shape in enumerate(SHAPES) for one in _sum_scratch(*shape, 3 if c < 3 else 2)]
        + [vmem((2, *shape), BF) for shape in SHAPES]
        + [dma((len(SHAPES), 12)), dma((len(SHAPES), 6, 2)), dma((len(SHAPES), 6, ROUNDS)), dma((3,))]
        + [vmem((tokens, d), BF)] * 10
        + [vmem((tokens, F), BF)] * 3
        + [vmem((tokens, d), F32), vmem((PAIRS, 8, tokens), F32)],
        compiler_params=pltpu.CompilerParams(dimension_semantics=("arbitrary",), vmem_limit_bytes=VMEM, collective_id=0, has_side_effects=True),
        cost_estimate=pl.CostEstimate(flops=10**11, transcendentals=0, bytes_accessed=2**28),
        name="layer_and_sum",
    )(x, dy, w["wo"], jnp.asarray(turns), *(w[n] for n in ("wq", "wk", "wv", "w_gate", "w_up", "w_down")))


def solution(mesh):
    def step(x, dy, *arrays):
        weights, m, v = (dict(zip(NAMES, arrays[i : i + 7], strict=True)) for i in (0, 7, 14))
        w = {n: w[0] for n, w in weights.items()}
        sums = layer(x[0], dy[0], w)
        wide = UP[1]
        places = {"w_down": (0, 0, 0), "wo": (0, FEEDS * DOWN[0], 0), "w_gate": (1, 0, 0), "wq": (1, 0, (FEEDS + 1) * wide),
                  "w_up": (1, 0, ROUNDS * wide), "wk": (1, 0, (ROUNDS + FEEDS + 1) * wide), "wv": (1, 0, 2 * ROUNDS * wide)}
        order = ("w_down", "w_gate", "w_up", "wo", "wq", "wk", "wv")
        each = ([a[n][0] for n in order] for a in (weights, m, v))
        new = [dict(zip(order, one, strict=True)) for one in optimizer(*each, sums, tuple(places[n] for n in order))]
        return tuple(one[name][None] for one in new for name in NAMES)

    states, all_of = P(("rep", "dp"), None, None), P(None, None, None)
    return jax.shard_map(
        step,
        mesh=mesh,
        in_specs=(states, states) + (all_of,) * 21,
        out_specs=(P("rep", None, None),) * 21,
        check_vma=False,
    )
```

```python
import functools

import jax
import jax.numpy as jnp
import numpy as np
from jax import lax
from jax.experimental import pallas as pl
from jax.experimental.pallas import tpu as pltpu
from jax.sharding import PartitionSpec as P

HEAD = 128
THETA = 10000
NAMES = ("wq", "wk", "wv", "wo", "w_gate", "w_up", "w_down")
LOG2E = 1.4426950408889634
T = 256
F = 512
VMEM = 67043328
BF, F32 = jnp.bfloat16, jnp.float32


def _dots(ca, cb):
    return lambda a, b: lax.dot_general(a, b, (((ca,), (cb,)), ((), ())), preferred_element_type=F32)


_nn, _nt, _tn = _dots(1, 0), _dots(1, 1), _dots(0, 0)


def _turns(tokens):
    half = HEAD // 2
    angle = np.arange(tokens, dtype=np.float32)[:, None] * np.float32(THETA) ** (-np.arange(half, dtype=np.float32) / np.float32(half))
    return np.concatenate([np.cos(angle), np.sin(angle)], 1).astype(np.float32)


def _both(t):
    low, other = lax.broadcasted_iota(jnp.int32, t.shape, 1) < HEAD // 2, pltpu.roll(t, HEAD // 2, 1)
    return jnp.where(low, t, other), jnp.where(low, -other, t)


def _normed(wide):
    return wide * lax.rsqrt(jnp.mean(wide * wide, -1, keepdims=True) + 1e-6)


def _turn(t, c, s):
    t = t.astype(BF).astype(F32)
    parts = [t[:, at : at + HEAD] for at in range(0, t.shape[1], HEAD)]
    return jnp.concatenate([x * c + pltpu.roll(x, HEAD // 2, 1) * s for x in parts], 1).astype(BF)


def _hidden(s):
    n = s.shape[0]
    low = s[n - T :]
    ok = lax.broadcasted_iota(jnp.int32, (T, T), 0) <= lax.broadcasted_iota(jnp.int32, (T, T), 1)
    low = jnp.where(ok, low, -1e30)
    return low if n == T else jnp.concatenate([s[: n - T], low], 0)


def _adamw(w, m, v, g):
    m = 0.9 * m + 0.1 * g
    v = 0.95 * v + 0.05 * g * g
    step = m * lax.rsqrt(v + 1e-8) + 0.1 * w
    return (w - 0.02 * step).astype(BF), m, v


TILE = (512, 1024)
DEEP = 4
CHUNK = 16


def _optimizer(*refs, where):
    n = len(where)
    w, m, v = refs[:n], refs[n : 2 * n], refs[2 * n : 3 * n]
    g, refs = refs[3 * n : 3 * n + 2], refs[3 * n + 2 :]
    out, (wi, mi, vi, gi, wn, mn, vn, came, left) = (refs[:n], refs[n : 2 * n], refs[2 * n : 3 * n]), refs[3 * n :]
    rows, cols = TILE
    tiles = [(one.shape[0] // rows) * (one.shape[1] // cols) for one in w]
    first = [sum(tiles[:j]) for j in range(n + 1)]

    def part(j, t):
        across = w[j].shape[1] // cols
        return lax.div(t, across) * rows, lax.rem(t, across) * cols

    def tile(ref, row, col):
        return ref.at[pl.ds(pl.multiple_of(row, rows), rows), pl.ds(pl.multiple_of(col, 512), cols)]

    def loads(j, t, slot):
        row, col = part(j, t)
        at, r0, c0 = where[j]
        pairs = ((tile(w[j], row, col), wi), (tile(m[j], row, col), mi), (tile(v[j], row, col), vi), (tile(g[at], r0 + row, c0 + col), gi))
        return [pltpu.make_async_copy(src, dst.at[slot], came.at[k, slot]) for k, (src, dst) in enumerate(pairs)]

    def stores(j, t, slot):
        row, col = part(j, t)
        pairs = zip((wn, mn, vn), (tile(o[j], row, col) for o in out), strict=True)
        return [pltpu.make_async_copy(src.at[slot], dst, left.at[k, slot]) for k, (src, dst) in enumerate(pairs)]

    for k in range(DEEP - 1):
        for copy in loads(0, k, k):
            copy.start()
    for j in range(n):

        def body(t, _, j=j):
            k = first[j] + t
            slot = lax.rem(k, DEEP)
            ahead = k + DEEP - 1
            for other in range(j, n):
                if first[other] < first[j + 1] + DEEP - 1:

                    @pl.when((ahead >= first[other]) & (ahead < first[other + 1]))
                    def _():
                        for copy in loads(other, ahead - first[other], lax.rem(ahead, DEEP)):
                            copy.start()
            for copy in loads(j, t, slot):
                copy.wait()

            @pl.when(k >= DEEP)
            def _():
                for copy in stores(0, 0, slot):
                    copy.wait()

            def chunk(c, _):
                r = pl.ds(pl.multiple_of(c * CHUNK, CHUNK), CHUNK)
                wn[slot, r], mn[slot, r], vn[slot, r] = _adamw(wi[slot, r].astype(F32), mi[slot, r], vi[slot, r], gi[slot, r].astype(F32))

            lax.fori_loop(0, rows // CHUNK, chunk, None)
            for copy in stores(j, t, slot):
                copy.start()

        lax.fori_loop(0, tiles[j], body, None)
    for k in range(DEEP):
        for copy in stores(0, 0, k):
            copy.wait()


def optimizer(w, m, v, sums, where):
    like = [jax.ShapeDtypeStruct(one.shape, one.dtype) for one in (*w, *m, *v)]
    hbm, n = pl.BlockSpec(memory_space=pl.ANY), len(w)
    new = pl.pallas_call(
        functools.partial(_optimizer, where=where),
        in_specs=[hbm] * (3 * n + 2),
        out_specs=[hbm] * (3 * n),
        out_shape=like,
        scratch_shapes=[pltpu.VMEM((DEEP, *TILE), kind) for kind in (BF, F32, F32, BF, BF, F32, F32)]
        + [pltpu.SemaphoreType.DMA((4, DEEP)), pltpu.SemaphoreType.DMA((3, DEEP))],
        compiler_params=pltpu.CompilerParams(vmem_limit_bytes=VMEM),
        cost_estimate=pl.CostEstimate(flops=16 * 2**24, transcendentals=2**24, bytes_accessed=22 * 2**24),
        name="optimizer",
    )(*w, *m, *v, *sums)
    return new[:n], new[n : 2 * n], new[2 * n :]


RING = 4
SHIFT = {"x": 5, "y": 3, "z": 1}
COLOURS = (("x", "y", "z"), ("y", "z", "x"), ("z", "x", "y"), ("x", "y", "z"))
TICKS = 4
AT = (0, 2, 3, 5, 7, 8, 11, 12, 15, 17, 20, 24, 28)


class Place:
    def __init__(self):
        me = lax.axis_index("dp")
        self.core = me & 1
        self.partner = me ^ 1
        self.at = {axis: (me >> shift) & 3 for axis, shift in SHIFT.items()}
        self.peers = {axis: {by: me + ((((self.at[axis] + by) & 3) - self.at[axis]) << shift) for by in (1, 2, 3)} for axis, shift in SHIFT.items()}

    def here(self):
        self.everyone = [self.partner] + [peer for axis in SHIFT for peer in self.peers[axis].values()]
        for peer in self.everyone:
            pl.semaphore_signal(pltpu.get_barrier_semaphore(), 1, device_id={"dp": peer})

    def meet(self):
        pl.semaphore_wait(pltpu.get_barrier_semaphore(), 1 + len(SHIFT) * (RING - 1))


class Sum:
    def __init__(self, colour, blk, place, local, out, refs, sems, slot, slot3):
        self.c, (self.R, self.C), self.slot, self.slot3, self.place = colour, blk, slot, slot3, place
        self.local, self.out = local, out
        self.rc, self.sa1, self.ra1, self.sa2, self.ra2, self.ra, self.sb1, self.rb1, self.sb2, self.rb2, self.rb, self.sc, self.rcc, self.all = refs
        self.send, self.recv, self.gather = sems
        self.core = place.core
        self.a, self.b, self.k = (place.at[axis] for axis in COLOURS[colour])
        self.first = (self.core * (self.R // 2), self.core * (self.R // 2) + self.a * (self.R // 8))
        self.first += (self.first[1] + self.b * (self.R // 32),)

    def peer(self, n, by):
        return self.place.peers[COLOURS[self.c][n]][by]

    def copy(self, src, dst, kind, device, slot=None, r=None):
        recv = self.recv.at[self.c, kind, slot] if r is None else self.gather.at[self.c, kind - 6, r]
        return pltpu.make_async_remote_copy(src, dst, self.send.at[self.c, kind], recv, device_id={"dp": device})

    def wait(self, ref, kind, slot=None, r=None, send=None):
        recv = self.recv.at[self.c, kind, slot] if r is None else self.gather.at[self.c, kind - 6, r]
        pltpu.make_async_copy(ref, ref, recv).wait()
        ref = ref if send is None else send
        pltpu.make_async_copy(ref, ref, self.send.at[self.c, kind]).wait()

    def quarter(self, r, by, half=None):
        n8 = self.R // 8
        q = (self.a + by) & 3
        cols = slice(None) if half is None else pl.ds(half * (self.C // 2), self.C // 2)
        mine = self.local[self.slot(r), pl.ds(pl.multiple_of(self.first[0] + q * n8, 16), n8), cols]
        return mine.astype(F32) + self.rc[self.slot3(r), pl.ds(pl.multiple_of(q * n8, 16), n8), cols].astype(F32)

    def cols(self, q):
        return pl.ds(pl.multiple_of(q * (self.C // 4), 128), self.C // 4)

    def stage(self, n, r):
        R, C = self.R, self.C
        slot = self.slot(r)
        n8, n32, half = R // 8, R // 32, C // 2
        left, right = pl.ds(0, half), pl.ds(half, half)
        f32 = lambda v: v.astype(F32)
        low = lambda v: v.astype(BF)
        if n == 0:
            other = pl.ds(pl.multiple_of((1 - self.core) * (R // 2), 16), R // 2)
            self.copy(self.local.at[slot, other], self.rc.at[self.slot3(r)], 0, self.place.partner, slot).start()
        elif n == 1:
            self.wait(self.rc.at[self.slot3(r)], 0, slot)
            self.sa1[:] = low(self.quarter(r, 2))
            self.both(self.sa1, self.ra1, 1, 0, slot, left, right)
        elif n == 2:
            self.wait(self.ra1.at[slot], 1, slot)
            self.sa2[0, :, :half] = low(self.quarter(r, 1, 0) + f32(self.ra1[slot, :, :half]))
            self.sa2[0, :, half:] = low(self.quarter(r, 1, 1))
            self.sa2[1, :, :half] = low(self.quarter(r, 3, 0))
            self.sa2[1, :, half:] = low(self.quarter(r, 3, 1) + f32(self.ra1[slot, :, half:]))
            self.pair(self.sa2, self.ra2, 2, 0, slot)
        elif n == 3:
            self.wait(self.ra2.at[slot], 2, slot)
            self.ra[:] = self.quarter(r, 0) + f32(self.ra2[slot, 0]) + f32(self.ra2[slot, 1])
            self.sb1[:] = low(self.ra[self.sixteenth(2)])
            self.both(self.sb1, self.rb1, 3, 1, slot, left, right)
        elif n == 4:
            self.wait(self.rb1.at[slot], 3, slot)
            up, down = self.sixteenth(1), self.sixteenth(3)
            self.sb2[0, :, :half] = low(self.ra[up, :half] + f32(self.rb1[slot, :, :half]))
            self.sb2[0, :, half:] = low(self.ra[up, half:])
            self.sb2[1, :, :half] = low(self.ra[down, :half])
            self.sb2[1, :, half:] = low(self.ra[down, half:] + f32(self.rb1[slot, :, half:]))
            self.pair(self.sb2, self.rb2, 4, 1, slot)
        elif n == 5:
            self.wait(self.rb2.at[slot], 4, slot)
            total = self.ra[self.sixteenth(0)] + f32(self.rb2[slot, 0]) + f32(self.rb2[slot, 1])
            self.rb[:] = total
            self.sc[:] = low(total)
            for by in (1, 2, 3):
                to = (self.k + by) & 3
                self.copy(self.sc.at[:, self.cols(to)], self.rcc.at[slot, by - 1], 5, self.peer(2, by), slot).start()
        elif n == 6:
            self.wait(self.rcc.at[slot], 5, slot)
            total = self.rb[:, self.cols(self.k)]
            for by in range(3):
                total = total + f32(self.rcc[slot, by])
            self.all[r & 3, self.sixteenth(0), self.cols(self.k)] = low(total)
            mine = self.all.at[r & 3, self.sixteenth(0), self.cols(self.k)]
            for by in (1, 2, 3):
                self.copy(mine, mine, 6, self.peer(2, by), r=r).start()
        elif n == 7:
            self.wait(self.rcc.at[slot], 6, r=r)
            mine = self.all.at[r & 3, self.sixteenth(0)]
            for by in (1, 3):
                self.copy(mine, mine, 7, self.peer(1, by), r=r).start()
        elif n == 8:
            self.wait(self.all.at[r & 3, pl.ds(0, 2 * n32)], 7, r=r)
            self.onward(lambda by: self.all.at[r & 3, self.sixteenth(by)], r, 8, 1, left, right)
        elif n == 9:
            self.wait(self.all.at[r & 3, pl.ds(0, n32)], 8, r=r)
            whole, mine = self.all.at[r & 3], self.out(r, self.first[1], n8)
            pltpu.make_async_copy(whole, mine, self.gather.at[self.c, 3, r]).start()
            for by in (1, 3):
                self.copy(whole, mine, 9, self.peer(0, by), r=r).start()
        elif n == 10:
            self.wait(self.out(r, 0, 3 * n8), 9, r=r, send=self.out(r, 0, 2 * n8))
            self.onward(lambda by: self.out(r, self.first[0] + ((self.a + by) & 3) * n8, n8), r, 10, 0, left, right)
        elif n == 11:
            self.wait(self.out(r, 0, n8), 10, r=r)
            mine = self.out(r, self.first[0], R // 2)
            self.copy(mine, mine, 11, self.place.partner, r=r).start()
        else:
            self.wait(self.out(r, 0, R // 2), 11, r=r)

    def sixteenth(self, by):
        return pl.ds(pl.multiple_of(((self.b + by) & 3) * (self.R // 32), 16), self.R // 32)

    def both(self, src, dst, kind, axis, slot, left, right):
        self.copy(src.at[:, left], dst.at[slot, :, left], kind, self.peer(axis, 1), slot).start()
        self.copy(src.at[:, right], dst.at[slot, :, right], kind, self.peer(axis, 3), slot).start()

    def pair(self, src, dst, kind, axis, slot):
        self.copy(src.at[0], dst.at[slot, 0], kind, self.peer(axis, 1), slot).start()
        self.copy(src.at[1], dst.at[slot, 1], kind, self.peer(axis, 3), slot).start()

    def onward(self, part, r, kind, axis, left, right):
        before, after = part(3).at[:, left], part(1).at[:, right]
        self.copy(before, before, kind, self.peer(axis, 1), r=r).start()
        self.copy(after, after, kind, self.peer(axis, 3), r=r).start()


def _sum_scratch(R, C, deep):
    n2, n8, n32 = R // 2, R // 8, R // 32
    return [pltpu.VMEM(shape, kind) for shape, kind in (
        ((deep, n2, C), BF), ((n8, C), BF), ((2, n8, C), BF), ((2, n8, C), BF), ((2, 2, n8, C), BF), ((n8, C), F32),
        ((n32, C), BF), ((2, n32, C), BF), ((2, n32, C), BF), ((2, 2, n32, C), BF), ((n32, C), F32), ((n32, C), BF), ((2, 3, n32, C // 4), BF),
        ((4, n8, C), BF))]


SUM_REFS = 14


def _stages(step, sums, tick, on):
    for n in reversed(range(len(AT))):
        if AT[n] % TICKS == tick:
            r = step - 1 - AT[n] // TICKS
            for c, one in enumerate(sums):

                @pl.when(on(c, r))
                def _():
                    one.stage(n, r)


DOWN, UP = (512, 1024), (1024, 512)
SHAPES = (DOWN, UP, UP, UP)
PAIRS = 4
FEEDS = 8
ROUNDS = FEEDS + 3


def _has(c, r):
    if c == 0:
        return (r >= 0) & (r <= FEEDS + 1)
    if c == 3:
        return (r > FEEDS) & (r < ROUNDS)
    return (r >= 0) & (r < ROUNDS) & (r != FEEDS)


def _slots(c, n):
    if c in (0, 3):
        return lambda r: lax.rem(r, n)
    if n == 2:
        return lambda r: (r + jnp.where(r > FEEDS, 1, 0)) & 1
    return lambda r: lax.rem(r - jnp.where(r > FEEDS, 1, 0), n)


def _layer(x_hbm, dy_hbm, wo_hbm, t_ref, wq_ref, wk_ref, wv_ref, wg_ref, wu_ref, wd_ref, rows_out, cols_out, *scratch):
    n, colours = SUM_REFS, len(SHAPES)
    parts, rest = [scratch[c * n : (c + 1) * n] for c in range(colours)], scratch[colours * n :]
    locals_, (send, recv, gather, load), rest = rest[:colours], rest[colours : colours + 4], rest[colours + 4 :]
    x1, x2, x3, x4, q, k, v, o, wo, at, act, dg, du, acc, lses = rest
    l0, l1, l2, l3 = locals_
    i = pl.program_id(0) - PAIRS
    tokens = x1.shape[0]
    rows, halves = ([slice(r, r + n) for r in range(0, tokens, n)] for n in (T, F))
    scale = HEAD**-0.5
    e = scale * LOG2E

    def in_rows(r, first, size):
        return rows_out.at[pl.ds(pl.multiple_of(r * DOWN[0] + first, 16), size)]

    def in_cols(c):
        block = lambda r: (c - 1) * ROUNDS + r - (FEEDS + 1 if c == 3 else 0)
        return lambda r, first, size: cols_out.at[pl.ds(pl.multiple_of(first, 16), size), pl.ds(pl.multiple_of(block(r) * UP[1], 128), UP[1])]

    place = Place()
    sums = [Sum(c, SHAPES[c], place, locals_[c], in_cols(c) if c else in_rows, parts[c], (send, recv, gather), _slots(c, 2), _slots(c, 3 if c < 3 else 2))
            for c in range(colours)]
    s0, s1 = _slots(0, 2)(i), _slots(1, 2)(i)

    loads = [pltpu.make_async_copy(src, dst, load.at[n]) for n, (src, dst) in enumerate(((x_hbm, x4), (wo_hbm, wo), (dy_hbm, x2)))]

    @pl.when(i == -PAIRS)
    def _():
        for one in loads:
            one.start()
        place.here()
        loads[0].wait()
        for r in rows:
            a = _normed(x4[r].astype(F32)).astype(BF)
            x1[r] = a
            at[:, r] = a.T
        acc[:] = jnp.zeros_like(acc)

    @pl.when(i == 0)
    def _():
        place.meet()

    def forward():
        pair = i + PAIRS
        both = pl.ds(pl.multiple_of(pair * 2 * HEAD, 2 * HEAD), 2 * HEAD)
        heads = [(n, pl.ds(pl.multiple_of((pair * 2 + n) * HEAD, HEAD), HEAD)) for n in range(2)]
        for r in halves:
            a, turns = x1[r], _both(t_ref[r])
            q[r, both] = _turn(_nn(a, wq_ref[:]), *turns)
            k[r, both] = _turn(_nn(a, wk_ref[:]), *turns)
            v[r, both] = _nn(a, wv_ref[:]).astype(BF)
        for r in rows:
            keys = slice(0, r.stop)
            scores = [_hidden(_nt(k[keys, cols], q[r, cols])) for _, cols in heads]
            tops = [s.max(axis=0, keepdims=True) for s in scores]
            weights = [jnp.exp2((s - top) * e).astype(BF) for s, top in zip(scores, tops)]
            for (n, cols), p, top in zip(heads, weights, tops):
                mix = _nn(jnp.concatenate([v[keys, cols].T, jnp.ones((8, r.stop), BF)], 0), p)
                total = mix[HEAD : HEAD + 1]
                o[r, cols] = (mix[:HEAD] * (1 / total)).T.astype(BF)
                lses[pair, n : n + 1, r] = top * e + jnp.log(total) * LOG2E

    def onto_residual():
        loads[1].wait()
        for r in halves:
            h = x4[r] + _nn(o[r], wo[:]).astype(BF)
            x4[r] = h
            b = _normed(h.astype(F32)).astype(BF)
            x1[r] = b
            x3[:, r] = b.T
        loads[2].wait()

    def units(r):
        b = x1[r]
        gate, up = _nn(b, wg_ref[:]), _nn(b, wu_ref[:])
        da = _nt(x2[r], wd_ref[:]).astype(BF).astype(F32)
        sig = 1 / (1 + jnp.exp2(gate * -LOG2E))
        silu = gate * sig
        act[r] = (silu * up).astype(BF)
        du[r] = (da * silu).astype(BF)
        dg[r] = (da * up * (sig + silu * (1 - sig))).astype(BF)

    def inward(part):
        acc[:, part] += _nt(dg[:], wg_ref[part]) + _nt(du[:], wu_ref[part])

    def norm_back():
        for r in halves:
            wide, ct = x4[r].astype(F32), acc[r].astype(BF).astype(F32)
            scale = lax.rsqrt(jnp.mean(wide * wide, -1, keepdims=True) + 1e-6)
            back = ct * scale - wide * (scale * scale * scale * jnp.mean(ct * wide, -1, keepdims=True))
            dh = x2[r] + back.astype(BF)
            x2[r] = dh
            x1[r] = _nt(dh, wo[:]).astype(BF)

    def head(n, to):
        cols = pl.ds(pl.multiple_of(n * HEAD, HEAD), HEAD)
        to = pl.ds(pl.multiple_of(to * HEAD, HEAD), HEAD)
        dk, dv = slice(0, HEAD), slice(HEAD, 2 * HEAD)
        for r in reversed(rows):
            keys = slice(0, r.stop)
            dor, qr = x1[r, cols], q[r, cols]
            delta = (dor.astype(F32) * o[r, cols].astype(F32)).T.sum(axis=0, keepdims=True)
            lse = lses[lax.div(n, 2), pl.ds(n & 1, 1), r]
            s = _hidden(_nt(k[keys, cols], qr) * e - lse)
            p = jnp.exp2(s)
            ds = (p * (_nt(v[keys, cols], dor) - delta)).astype(BF)
            if r.stop == tokens:
                acc[keys, dv] = _nn(p.astype(BF), dor)
                acc[keys, dk] = _nn(ds, qr)
            else:
                acc[keys, dv] += _nn(p.astype(BF), dor)
                acc[keys, dk] += _nn(ds, qr)
            t = (_tn(k[keys, cols], ds) * scale).T.astype(BF).astype(F32)
            cos, sin = _both(t_ref[r])
            dg[r, to] = (t * cos - pltpu.roll(t, HEAD // 2, 1) * sin).astype(BF)
        for r in rows:
            act[r, to] = acc[r, dv].astype(BF)
            t = (acc[r, dk] * scale).astype(BF).astype(F32)
            cos, sin = _both(t_ref[r])
            du[r, to] = (t * cos - pltpu.roll(t, HEAD // 2, 1) * sin).astype(BF)

    feeding = (i >= 0) & (i < FEEDS)
    attending = (i == FEEDS + 1) | (i == FEEDS + 2)

    def ticking(tick, _):
        for one in range(TICKS):

            @pl.when(tick == one)
            def _():
                _stages(i, sums, one, _has)

        @pl.when((i < 0) & (tick == 0))
        def _():
            forward()

        @pl.when((i == -1) & (tick == 1))
        def _():
            onto_residual()

        @pl.when(feeding & (tick < 2))
        def _():
            units(pl.ds(pl.multiple_of(tick * F, F), F))

        @pl.when(feeding & (tick == 2))
        def _():
            l0[s0] = _tn(act[:], x2[:]).astype(BF)
            l1[s1] = _nn(x3[:], dg[:]).astype(BF)
            inward(halves[0])

        @pl.when(feeding & (tick == 3))
        def _():
            l2[s1] = _nn(x3[:], du[:]).astype(BF)
            inward(halves[1])

        @pl.when((i == FEEDS) & (tick == 0))
        def _():
            norm_back()

        @pl.when(((i == FEEDS) | (i == FEEDS + 1)) & (tick == 2))
        def _():
            l0[s0] = _tn(o[:, pl.ds(pl.multiple_of((i - FEEDS) * F, F), F)], x2[:]).astype(BF)

        @pl.when(attending)
        def _():
            head((i - FEEDS - 1) * TICKS + tick, tick)

        @pl.when(attending & (tick == TICKS - 1))
        def _():
            l1[s1] = _nn(at[:], dg[:]).astype(BF)
            l2[s1] = _nn(at[:], du[:]).astype(BF)
            l3[s0] = _nn(at[:], act[:]).astype(BF)

    lax.fori_loop(0, TICKS, ticking, None)


def layer(x, dy, w):
    tokens, d = x.shape
    turns = _turns(tokens)
    hbm = pl.BlockSpec(memory_space=pl.ANY)
    upto = lambda i, n: jnp.clip(i, 0, n - 1)
    heads = pl.BlockSpec((d, 2 * HEAD), lambda i: (0, upto(i, PAIRS)))
    feed = pl.BlockSpec(UP, lambda i: (0, upto(i - PAIRS, FEEDS)))
    down = pl.BlockSpec(DOWN, lambda i: (upto(i - PAIRS, FEEDS), 0))
    dma, vmem = pltpu.SemaphoreType.DMA, pltpu.VMEM
    return pl.pallas_call(
        _layer,
        grid=(PAIRS + ROUNDS + 1 + AT[-1] // TICKS,),
        in_specs=[hbm] * 3 + [pl.BlockSpec(turns.shape, lambda i: (0, 0), pipeline_mode=pl.Buffered(1))] + [heads] * 3 + [feed, feed, down],
        out_specs=[hbm] * 2,
        out_shape=[jax.ShapeDtypeStruct((DOWN[0] * (FEEDS + 2), DOWN[1]), BF), jax.ShapeDtypeStruct((UP[0], (2 * ROUNDS + 2) * UP[1]), BF)],
        scratch_shapes=[one for c, shape in enumerate(SHAPES) for one in _sum_scratch(*shape, 3 if c < 3 else 2)]
        + [vmem((2, *shape), BF) for shape in SHAPES]
        + [dma((len(SHAPES), 12)), dma((len(SHAPES), 6, 2)), dma((len(SHAPES), 6, ROUNDS)), dma((3,))]
        + [vmem((tokens, d), BF)] * 10
        + [vmem((tokens, F), BF)] * 3
        + [vmem((tokens, d), F32), vmem((PAIRS, 8, tokens), F32)],
        compiler_params=pltpu.CompilerParams(dimension_semantics=("arbitrary",), vmem_limit_bytes=VMEM, collective_id=0, has_side_effects=True),
        cost_estimate=pl.CostEstimate(flops=10**11, transcendentals=0, bytes_accessed=2**28),
        name="layer_and_sum",
    )(x, dy, w["wo"], jnp.asarray(turns), *(w[n] for n in ("wq", "wk", "wv", "w_gate", "w_up", "w_down")))


def solution(mesh):
    def step(x, dy, *arrays):
        weights, m, v = (dict(zip(NAMES, arrays[i : i + 7], strict=True)) for i in (0, 7, 14))
        w = {n: w[0] for n, w in weights.items()}
        sums = layer(x[0], dy[0], w)
        wide = UP[1]
        places = {"w_down": (0, 0, 0), "wo": (0, FEEDS * DOWN[0], 0), "w_gate": (1, 0, 0), "wq": (1, 0, (FEEDS + 1) * wide),
                  "w_up": (1, 0, ROUNDS * wide), "wk": (1, 0, (ROUNDS + FEEDS + 1) * wide), "wv": (1, 0, 2 * ROUNDS * wide)}
        order = ("w_down", "w_gate", "w_up", "wo", "wq", "wk", "wv")
        each = ([a[n][0] for n in order] for a in (weights, m, v))
        new = [dict(zip(order, one, strict=True)) for one in optimizer(*each, sums, tuple(places[n] for n in order))]
        return tuple(one[name][None] for one in new for name in NAMES)

    states, all_of = P(("rep", "dp"), None, None), P(None, None, None)
    return jax.shard_map(
        step,
        mesh=mesh,
        in_specs=(states, states) + (all_of,) * 21,
        out_specs=(P("rep", None, None),) * 21,
        check_vma=False,
    )
```

```python
import functools

import jax
import jax.numpy as jnp
import numpy as np
from jax import lax
from jax.experimental import pallas as pl
from jax.experimental.pallas import tpu as pltpu
from jax.sharding import PartitionSpec as P

HEAD = 128
THETA = 10000
NAMES = ("wq", "wk", "wv", "wo", "w_gate", "w_up", "w_down")
LOG2E = 1.4426950408889634
T = 256
F = 512
VMEM = 67043328
BF, F32 = jnp.bfloat16, jnp.float32


def _dots(ca, cb):
    return lambda a, b: lax.dot_general(a, b, (((ca,), (cb,)), ((), ())), preferred_element_type=F32)


_nn, _nt, _tn = _dots(1, 0), _dots(1, 1), _dots(0, 0)


def _turns(tokens):
    half = HEAD // 2
    angle = np.arange(tokens, dtype=np.float32)[:, None] * np.float32(THETA) ** (-np.arange(half, dtype=np.float32) / np.float32(half))
    return np.concatenate([np.cos(angle), np.sin(angle)], 1).astype(np.float32)


def _both(t):
    low, other = lax.broadcasted_iota(jnp.int32, t.shape, 1) < HEAD // 2, pltpu.roll(t, HEAD // 2, 1)
    return jnp.where(low, t, other), jnp.where(low, -other, t)


def _normed(wide):
    return wide * lax.rsqrt(jnp.mean(wide * wide, -1, keepdims=True) + 1e-6)


def _turn(t, c, s):
    t = t.astype(BF).astype(F32)
    parts = [t[:, at : at + HEAD] for at in range(0, t.shape[1], HEAD)]
    return jnp.concatenate([x * c + pltpu.roll(x, HEAD // 2, 1) * s for x in parts], 1).astype(BF)


def _hidden(s):
    n = s.shape[0]
    low = s[n - T :]
    ok = lax.broadcasted_iota(jnp.int32, (T, T), 0) <= lax.broadcasted_iota(jnp.int32, (T, T), 1)
    low = jnp.where(ok, low, -1e30)
    return low if n == T else jnp.concatenate([s[: n - T], low], 0)


def _adamw(w, m, v, g):
    m = 0.9 * m + 0.1 * g
    v = 0.95 * v + 0.05 * g * g
    step = m * lax.rsqrt(v + 1e-8) + 0.1 * w
    return (w - 0.02 * step).astype(BF), m, v


TILE = (128, 1024)
DEEP = 8
CHUNK = 16


def _optimizer(*refs, where):
    n = len(where)
    w, m, v = refs[:n], refs[n : 2 * n], refs[2 * n : 3 * n]
    g, refs = refs[3 * n : 3 * n + 2], refs[3 * n + 2 :]
    out, (wi, mi, vi, gi, wn, mn, vn, came, left) = (refs[:n], refs[n : 2 * n], refs[2 * n : 3 * n]), refs[3 * n :]
    rows, cols = TILE
    tiles = [(one.shape[0] // rows) * (one.shape[1] // cols) for one in w]
    first = [sum(tiles[:j]) for j in range(n + 1)]

    def part(j, t):
        across = w[j].shape[1] // cols
        return lax.div(t, across) * rows, lax.rem(t, across) * cols

    def tile(ref, row, col):
        return ref.at[pl.ds(pl.multiple_of(row, rows), rows), pl.ds(pl.multiple_of(col, 512), cols)]

    def loads(j, t, slot):
        row, col = part(j, t)
        at, r0, c0 = where[j]
        pairs = ((tile(w[j], row, col), wi), (tile(m[j], row, col), mi), (tile(v[j], row, col), vi), (tile(g[at], r0 + row, c0 + col), gi))
        return [pltpu.make_async_copy(src, dst.at[slot], came.at[k, slot]) for k, (src, dst) in enumerate(pairs)]

    def stores(j, t, slot):
        row, col = part(j, t)
        pairs = zip((wn, mn, vn), (tile(o[j], row, col) for o in out), strict=True)
        return [pltpu.make_async_copy(src.at[slot], dst, left.at[k, slot]) for k, (src, dst) in enumerate(pairs)]

    for k in range(DEEP - 1):
        for copy in loads(0, k, k):
            copy.start()
    for j in range(n):

        def body(t, _, j=j):
            k = first[j] + t
            slot = lax.rem(k, DEEP)
            ahead = k + DEEP - 1
            for other in range(j, n):
                if first[other] < first[j + 1] + DEEP - 1:

                    @pl.when((ahead >= first[other]) & (ahead < first[other + 1]))
                    def _():
                        for copy in loads(other, ahead - first[other], lax.rem(ahead, DEEP)):
                            copy.start()
            for copy in loads(j, t, slot):
                copy.wait()

            @pl.when(k >= DEEP)
            def _():
                for copy in stores(0, 0, slot):
                    copy.wait()

            def chunk(c, _):
                r = pl.ds(pl.multiple_of(c * CHUNK, CHUNK), CHUNK)
                wn[slot, r], mn[slot, r], vn[slot, r] = _adamw(wi[slot, r].astype(F32), mi[slot, r], vi[slot, r], gi[slot, r].astype(F32))

            lax.fori_loop(0, rows // CHUNK, chunk, None)
            for copy in stores(j, t, slot):
                copy.start()

        lax.fori_loop(0, tiles[j], body, None)
    for k in range(DEEP):
        for copy in stores(0, 0, k):
            copy.wait()


def optimizer(w, m, v, sums, where):
    like = [jax.ShapeDtypeStruct(one.shape, one.dtype) for one in (*w, *m, *v)]
    hbm, n = pl.BlockSpec(memory_space=pl.ANY), len(w)
    new = pl.pallas_call(
        functools.partial(_optimizer, where=where),
        in_specs=[hbm] * (3 * n + 2),
        out_specs=[hbm] * (3 * n),
        out_shape=like,
        scratch_shapes=[pltpu.VMEM((DEEP, *TILE), kind) for kind in (BF, F32, F32, BF, BF, F32, F32)]
        + [pltpu.SemaphoreType.DMA((4, DEEP)), pltpu.SemaphoreType.DMA((3, DEEP))],
        compiler_params=pltpu.CompilerParams(vmem_limit_bytes=VMEM),
        name="optimizer",
    )(*w, *m, *v, *sums)
    return new[:n], new[n : 2 * n], new[2 * n :]


RING = 4
OTHERS, NEXT = (1, 2, 3), (1, 3)
SHIFT = {"x": 5, "y": 3, "z": 1}
COLOURS = (("x", "y", "z"), ("y", "z", "x"), ("z", "x", "y"), ("x", "y", "z"))
TICKS = 4
AT = (0, 2, 3, 5, 7, 8, 11, 12, 15, 17, 20, 24, 28)


class Place:
    def __init__(self):
        me = lax.axis_index("dp")
        self.core = me & 1
        self.partner = me ^ 1
        self.at = {axis: (me >> shift) & 3 for axis, shift in SHIFT.items()}
        self.peers = {axis: {by: me + ((((self.at[axis] + by) & 3) - self.at[axis]) << shift) for by in OTHERS} for axis, shift in SHIFT.items()}

    def here(self):
        self.everyone = [self.partner] + [peer for axis in SHIFT for peer in self.peers[axis].values()]
        for peer in self.everyone:
            pl.semaphore_signal(pltpu.get_barrier_semaphore(), 1, device_id={"dp": peer})

    def meet(self):
        pl.semaphore_wait(pltpu.get_barrier_semaphore(), 1 + len(SHIFT) * (RING - 1))


class Sum:
    def __init__(self, colour, blk, place, local, out, refs, sems, slot, slot3):
        self.c, (self.R, self.C), self.slot, self.slot3, self.place = colour, blk, slot, slot3, place
        self.local, self.out = local, out
        self.rc, self.sa1, self.ra1, self.sa2, self.ra2, self.ra, self.sb1, self.rb1, self.sb2, self.rb2, self.rb, self.sc, self.rcc, self.all = refs
        self.send, self.recv, self.gather = sems
        self.core = place.core
        self.a, self.b, self.k = (place.at[axis] for axis in COLOURS[colour])
        self.first = (self.core * (self.R // 2), self.core * (self.R // 2) + self.a * (self.R // 8))
        self.first += (self.first[1] + self.b * (self.R // 32),)

    def peer(self, n, by):
        return self.place.peers[COLOURS[self.c][n]][by]

    def copy(self, src, dst, kind, device, slot=None, r=None):
        recv = self.recv.at[self.c, kind, slot] if r is None else self.gather.at[self.c, kind - 6, r]
        return pltpu.make_async_remote_copy(src, dst, self.send.at[self.c, kind], recv, device_id={"dp": device})

    def wait(self, ref, kind, slot=None, r=None, send=None):
        recv = self.recv.at[self.c, kind, slot] if r is None else self.gather.at[self.c, kind - 6, r]
        pltpu.make_async_copy(ref, ref, recv).wait()
        ref = ref if send is None else send
        pltpu.make_async_copy(ref, ref, self.send.at[self.c, kind]).wait()

    def quarter(self, r, by, half=None):
        n8 = self.R // 8
        q = (self.a + by) & 3
        cols = slice(None) if half is None else pl.ds(half * (self.C // 2), self.C // 2)
        mine = self.local[self.slot(r), pl.ds(pl.multiple_of(self.first[0] + q * n8, 16), n8), cols]
        return mine.astype(F32) + self.rc[self.slot3(r), pl.ds(pl.multiple_of(q * n8, 16), n8), cols].astype(F32)

    def cols(self, q):
        return pl.ds(pl.multiple_of(q * (self.C // 4), 128), self.C // 4)

    def stage(self, n, r):
        R, C = self.R, self.C
        slot = self.slot(r)
        n8, n32, half = R // 8, R // 32, C // 2
        left, right = pl.ds(0, half), pl.ds(half, half)
        f32 = lambda v: v.astype(F32)
        low = lambda v: v.astype(BF)
        if n == 0:
            other = pl.ds(pl.multiple_of((1 - self.core) * (R // 2), 16), R // 2)
            self.copy(self.local.at[slot, other], self.rc.at[self.slot3(r)], 0, self.place.partner, slot).start()
        elif n == 1:
            self.wait(self.rc.at[self.slot3(r)], 0, slot)
            self.sa1[:] = low(self.quarter(r, 2))
            self.both(self.sa1, self.ra1, 1, 0, slot, left, right)
        elif n == 2:
            self.wait(self.ra1.at[slot], 1, slot)
            self.sa2[0, :, :half] = low(self.quarter(r, 1, 0) + f32(self.ra1[slot, :, :half]))
            self.sa2[0, :, half:] = low(self.quarter(r, 1, 1))
            self.sa2[1, :, :half] = low(self.quarter(r, 3, 0))
            self.sa2[1, :, half:] = low(self.quarter(r, 3, 1) + f32(self.ra1[slot, :, half:]))
            self.pair(self.sa2, self.ra2, 2, 0, slot)
        elif n == 3:
            self.wait(self.ra2.at[slot], 2, slot)
            self.ra[:] = self.quarter(r, 0) + f32(self.ra2[slot, 0]) + f32(self.ra2[slot, 1])
            self.sb1[:] = low(self.ra[self.sixteenth(2)])
            self.both(self.sb1, self.rb1, 3, 1, slot, left, right)
        elif n == 4:
            self.wait(self.rb1.at[slot], 3, slot)
            up, down = self.sixteenth(1), self.sixteenth(3)
            self.sb2[0, :, :half] = low(self.ra[up, :half] + f32(self.rb1[slot, :, :half]))
            self.sb2[0, :, half:] = low(self.ra[up, half:])
            self.sb2[1, :, :half] = low(self.ra[down, :half])
            self.sb2[1, :, half:] = low(self.ra[down, half:] + f32(self.rb1[slot, :, half:]))
            self.pair(self.sb2, self.rb2, 4, 1, slot)
        elif n == 5:
            self.wait(self.rb2.at[slot], 4, slot)
            total = self.ra[self.sixteenth(0)] + f32(self.rb2[slot, 0]) + f32(self.rb2[slot, 1])
            self.rb[:] = total
            self.sc[:] = low(total)
            for by in OTHERS:
                to = (self.k + by) & 3
                self.copy(self.sc.at[:, self.cols(to)], self.rcc.at[slot, by - 1], 5, self.peer(2, by), slot).start()
        elif n == 6:
            self.wait(self.rcc.at[slot], 5, slot)
            total = self.rb[:, self.cols(self.k)]
            for by in range(3):
                total = total + f32(self.rcc[slot, by])
            self.all[r & 3, self.sixteenth(0), self.cols(self.k)] = low(total)
            mine = self.all.at[r & 3, self.sixteenth(0), self.cols(self.k)]
            for by in OTHERS:
                self.copy(mine, mine, 6, self.peer(2, by), r=r).start()
        elif n == 7:
            self.wait(self.rcc.at[slot], 6, r=r)
            mine = self.all.at[r & 3, self.sixteenth(0)]
            for by in NEXT:
                self.copy(mine, mine, 7, self.peer(1, by), r=r).start()
        elif n == 8:
            self.wait(self.all.at[r & 3, pl.ds(0, 2 * n32)], 7, r=r)
            self.onward(lambda by: self.all.at[r & 3, self.sixteenth(by)], r, 8, 1, left, right)
        elif n == 9:
            self.wait(self.all.at[r & 3, pl.ds(0, n32)], 8, r=r)
            whole, mine = self.all.at[r & 3], self.out(r, self.first[1], n8)
            pltpu.make_async_copy(whole, mine, self.gather.at[self.c, 3, r]).start()
            for by in NEXT:
                self.copy(whole, mine, 9, self.peer(0, by), r=r).start()
        elif n == 10:
            self.wait(self.out(r, 0, 3 * n8), 9, r=r, send=self.out(r, 0, 2 * n8))
            self.onward(lambda by: self.out(r, self.first[0] + ((self.a + by) & 3) * n8, n8), r, 10, 0, left, right)
        elif n == 11:
            self.wait(self.out(r, 0, n8), 10, r=r)
            mine = self.out(r, self.first[0], R // 2)
            self.copy(mine, mine, 11, self.place.partner, r=r).start()
        else:
            self.wait(self.out(r, 0, R // 2), 11, r=r)

    def sixteenth(self, by):
        return pl.ds(pl.multiple_of(((self.b + by) & 3) * (self.R // 32), 16), self.R // 32)

    def both(self, src, dst, kind, axis, slot, left, right):
        self.copy(src.at[:, left], dst.at[slot, :, left], kind, self.peer(axis, 1), slot).start()
        self.copy(src.at[:, right], dst.at[slot, :, right], kind, self.peer(axis, 3), slot).start()

    def pair(self, src, dst, kind, axis, slot):
        self.copy(src.at[0], dst.at[slot, 0], kind, self.peer(axis, 1), slot).start()
        self.copy(src.at[1], dst.at[slot, 1], kind, self.peer(axis, 3), slot).start()

    def onward(self, part, r, kind, axis, left, right):
        before, after = part(3).at[:, left], part(1).at[:, right]
        self.copy(before, before, kind, self.peer(axis, 1), r=r).start()
        self.copy(after, after, kind, self.peer(axis, 3), r=r).start()


def _sum_scratch(R, C, deep):
    n2, n8, n32 = R // 2, R // 8, R // 32
    return [pltpu.VMEM(shape, kind) for shape, kind in (
        ((deep, n2, C), BF), ((n8, C), BF), ((2, n8, C), BF), ((2, n8, C), BF), ((2, 2, n8, C), BF), ((n8, C), F32),
        ((n32, C), BF), ((2, n32, C), BF), ((2, n32, C), BF), ((2, 2, n32, C), BF), ((n32, C), F32), ((n32, C), BF), ((2, 3, n32, C // 4), BF),
        ((4, n8, C), BF))]


SUM_REFS = 14


def _stages(step, sums, tick, on):
    for n in reversed(range(len(AT))):
        if AT[n] % TICKS == tick:
            r = step - 1 - AT[n] // TICKS
            for c, one in enumerate(sums):

                @pl.when(on(c, r))
                def _():
                    one.stage(n, r)


DOWN, UP = (512, 1024), (1024, 512)
SHAPES = (DOWN, UP, UP, UP)
PAIRS = 4
FEEDS = 8
ROUNDS = FEEDS + 3


def _has(c, r):
    if c == 0:
        return (r >= 0) & (r <= FEEDS + 1)
    if c == 3:
        return (r > FEEDS) & (r < ROUNDS)
    return (r >= 0) & (r < ROUNDS) & (r != FEEDS)


def _slots(c, n):
    if c in (0, 3):
        return lambda r: lax.rem(r, n)
    if n == 2:
        return lambda r: (r + jnp.where(r > FEEDS, 1, 0)) & 1
    return lambda r: lax.rem(r - jnp.where(r > FEEDS, 1, 0), n)


def _layer(x_hbm, dy_hbm, wo_hbm, t_ref, wq_ref, wk_ref, wv_ref, wg_ref, wu_ref, wd_ref, rows_out, cols_out, weights_out, *scratch):
    n, colours = SUM_REFS, len(SHAPES)
    parts, rest = [scratch[c * n : (c + 1) * n] for c in range(colours)], scratch[colours * n :]
    locals_, (send, recv, gather, load), rest = rest[:colours], rest[colours : colours + 4], rest[colours + 4 :]
    x1, x2, xs, q, k, v, o, wo, at, act, dg, du, acc, shares = rest
    x3, x4 = xs.at[0], xs.at[1]
    l0, l1, l2, l3 = locals_
    i = pl.program_id(0) - PAIRS
    tokens = x1.shape[0]
    rows, halves = ([slice(r, r + n) for r in range(0, tokens, n)] for n in (T, F))
    scale = HEAD**-0.5
    e = scale * LOG2E

    def in_rows(r, first, size):
        return rows_out.at[pl.ds(pl.multiple_of(r * DOWN[0] + first, 16), size)]

    def in_cols(c):
        block = lambda r: (c - 1) * ROUNDS + r - (FEEDS + 1 if c == 3 else 0)
        return lambda r, first, size: cols_out.at[pl.ds(pl.multiple_of(first, 16), size), pl.ds(pl.multiple_of(block(r) * UP[1], 128), UP[1])]

    place = Place()
    sums = [Sum(c, SHAPES[c], place, locals_[c], in_cols(c) if c else in_rows, parts[c], (send, recv, gather), _slots(c, 2), _slots(c, 3 if c < 3 else 2))
            for c in range(colours)]
    s0, s1 = _slots(0, 2)(i), _slots(1, 2)(i)

    loads = [pltpu.make_async_copy(src, dst, load.at[n]) for n, (src, dst) in enumerate(((x_hbm, x4), (wo_hbm, wo), (dy_hbm, x2)))]
    pair = i + PAIRS
    saves = [pltpu.make_async_copy(src, weights_out.at[jnp.clip(pair, 0, PAIRS - 1) * 2 + n], load.at[3 + n]) for n, src in enumerate((x2, x3))]

    @pl.when(pair == 0)
    def _():
        loads[0].start()
        place.here()
        loads[0].wait()
        loads[1].start()
        for r in rows:
            a = _normed(x4[r].astype(F32)).astype(BF)
            x1[r] = a
            at[:, r] = a.T

    @pl.when((pair > 0) & (i < 0))
    def _():
        for one in saves:
            one.wait()

    @pl.when(i == 0)
    def _():
        place.meet()
        acc[:] = jnp.zeros_like(acc)

    def forward():
        both = pl.ds(pl.multiple_of(pair * 2 * HEAD, 2 * HEAD), 2 * HEAD)
        heads = [(n, pl.ds(pl.multiple_of((pair * 2 + n) * HEAD, HEAD), HEAD)) for n in range(2)]
        for r in halves:
            a, turns = x1[r], _both(t_ref[r])
            q[r, both] = _turn(_nn(a, wq_ref[:]), *turns)
            k[r, both] = _turn(_nn(a, wk_ref[:]), *turns)
            v[r, both] = _nn(a, wv_ref[:]).astype(BF)

        def spot(j, n):
            return slice((j % 2 * 2 + n) * T, (j % 2 * 2 + n + 1) * T)

        def score(j):
            for n, cols in heads:
                acc[: rows[j].stop, spot(j, n)] = _hidden(_nt(k[: rows[j].stop, cols], q[rows[j], cols]))

        score(0)
        for j, r in enumerate(rows):
            if r.stop < tokens:
                score(j + 1)
            keys = slice(0, r.stop)
            for (n, cols), kept in zip(heads, (x2, x3)):
                s = acc[keys, spot(j, n)]
                p = jnp.exp2((s - s.max(axis=0, keepdims=True)) * e).astype(BF)
                kept[keys, r] = p
                mix = _nn(jnp.concatenate([v[keys, cols].T, jnp.ones((8, r.stop), BF)], 0), p)
                share = 1 / mix[HEAD : HEAD + 1]
                o[r, cols] = (mix[:HEAD] * share).T.astype(BF)
                shares[pair, n : n + 1, r] = share
        for one in saves:
            one.start()

    def onto_residual():
        for one in saves:
            one.wait()
        loads[2].start()
        loads[1].wait()
        for r in halves:
            h = x4[r] + _nn(o[r], wo[:]).astype(BF)
            x4[r] = h
            b = _normed(h.astype(F32)).astype(BF)
            x1[r] = b
            x3[:, r] = b.T
        loads[2].wait()

    def units(r):
        b = x1[r]
        gate, up = _nn(b, wg_ref[:]), _nn(b, wu_ref[:])
        da = _nt(x2[r], wd_ref[:]).astype(BF).astype(F32)
        sig = 1 / (1 + jnp.exp2(gate * -LOG2E))
        silu = gate * sig
        act[r] = (silu * up).astype(BF)
        du[r] = (da * silu).astype(BF)
        dg[r] = (da * up * (sig + silu * (1 - sig))).astype(BF)

    def inward(part):
        acc[:, part] += _nt(dg[:], wg_ref[part]) + _nt(du[:], wu_ref[part])

    def norm_back():
        for r in halves:
            wide, ct = x4[r].astype(F32), acc[r].astype(BF).astype(F32)
            scale = lax.rsqrt(jnp.mean(wide * wide, -1, keepdims=True) + 1e-6)
            back = ct * scale - wide * (scale * scale * scale * jnp.mean(ct * wide, -1, keepdims=True))
            dh = x2[r] + back.astype(BF)
            x2[r] = dh
            x1[r] = _nt(dh, wo[:]).astype(BF)

    def head(n, to):
        cols = pl.ds(pl.multiple_of(n * HEAD, HEAD), HEAD)
        to = pl.ds(pl.multiple_of(to * HEAD, HEAD), HEAD)
        dk, dv = slice(0, HEAD), slice(HEAD, 2 * HEAD)
        for r in reversed(rows):
            keys = slice(0, r.stop)
            dor, qr = x1[r, cols], q[r, cols]
            delta = (dor.astype(F32) * o[r, cols].astype(F32)).T.sum(axis=0, keepdims=True)
            p = xs[n & 1, keys, r].astype(F32) * shares[lax.div(n, 2), pl.ds(n & 1, 1), r]
            ds = (p * (_nt(v[keys, cols], dor) - delta)).astype(BF)
            if r.stop == tokens:
                acc[keys, dv] = _nn(p.astype(BF), dor)
                acc[keys, dk] = _nn(ds, qr)
            else:
                acc[keys, dv] += _nn(p.astype(BF), dor)
                acc[keys, dk] += _nn(ds, qr)
            t = (_tn(k[keys, cols], ds) * scale).T.astype(BF).astype(F32)
            cos, sin = _both(t_ref[r])
            dg[r, to] = (t * cos - pltpu.roll(t, HEAD // 2, 1) * sin).astype(BF)
        for r in rows:
            act[r, to] = acc[r, dv].astype(BF)
            t = (acc[r, dk] * scale).astype(BF).astype(F32)
            cos, sin = _both(t_ref[r])
            du[r, to] = (t * cos - pltpu.roll(t, HEAD // 2, 1) * sin).astype(BF)

    def recall(n):
        return pltpu.make_async_copy(weights_out.at[n], xs.at[n & 1], load.at[3 + (n & 1)])

    feeding = (i >= 0) & (i < FEEDS)
    attending = (i == FEEDS + 1) | (i == FEEDS + 2)

    def ticking(tick, _):
        for one in range(TICKS):

            @pl.when(tick == one)
            def _():
                _stages(i, sums, one, _has)

        @pl.when((i < 0) & (tick == 0))
        def _():
            forward()

        @pl.when((i == -1) & (tick == 1))
        def _():
            onto_residual()

        @pl.when(feeding & (tick < 2))
        def _():
            units(pl.ds(pl.multiple_of(tick * F, F), F))

        @pl.when(feeding & (tick == 2))
        def _():
            l0[s0] = _tn(act[:], x2[:]).astype(BF)
            l1[s1] = _nn(x3[:], dg[:]).astype(BF)
            inward(halves[0])

        @pl.when(feeding & (tick == 3))
        def _():
            l2[s1] = _nn(x3[:], du[:]).astype(BF)
            inward(halves[1])

        @pl.when((i == FEEDS) & (tick == 0))
        def _():
            recall(0).start()
            norm_back()
            recall(1).start()

        @pl.when(((i == FEEDS) | (i == FEEDS + 1)) & (tick == 2))
        def _():
            l0[s0] = _tn(o[:, pl.ds(pl.multiple_of((i - FEEDS) * F, F), F)], x2[:]).astype(BF)

        @pl.when(attending)
        def _():
            n = (i - FEEDS - 1) * TICKS + tick
            recall(n).wait()
            head(n, tick)

            @pl.when(n + 2 < 2 * PAIRS)
            def _():
                recall(n + 2).start()


        @pl.when(attending & (tick == TICKS - 1))
        def _():
            l1[s1] = _nn(at[:], dg[:]).astype(BF)
            l2[s1] = _nn(at[:], du[:]).astype(BF)
            l3[s0] = _nn(at[:], act[:]).astype(BF)

    lax.fori_loop(0, TICKS, ticking, None)


def layer(x, dy, w):
    tokens, d = x.shape
    turns = _turns(tokens)
    hbm = pl.BlockSpec(memory_space=pl.ANY)
    upto = lambda i, n: jnp.clip(i, 0, n - 1)
    heads = pl.BlockSpec((d, 2 * HEAD), lambda i: (0, upto(i, PAIRS)))
    feed = pl.BlockSpec(UP, lambda i: (0, upto(i - PAIRS, FEEDS)))
    down = pl.BlockSpec(DOWN, lambda i: (upto(i - PAIRS, FEEDS), 0))
    dma, vmem = pltpu.SemaphoreType.DMA, pltpu.VMEM
    return pl.pallas_call(
        _layer,
        grid=(PAIRS + ROUNDS + 1 + AT[-1] // TICKS,),
        in_specs=[hbm] * 3 + [pl.BlockSpec(turns.shape, lambda i: (0, 0), pipeline_mode=pl.Buffered(1))] + [heads] * 3 + [feed, feed, down],
        out_specs=[hbm] * 3,
        out_shape=[jax.ShapeDtypeStruct(shape, BF) for shape in (
            (DOWN[0] * (FEEDS + 2), DOWN[1]), (UP[0], (2 * ROUNDS + 2) * UP[1]), (2 * PAIRS, tokens, tokens))],
        scratch_shapes=[one for c, shape in enumerate(SHAPES) for one in _sum_scratch(*shape, 3 if c < 3 else 2)]
        + [vmem((2, *shape), BF) for shape in SHAPES]
        + [dma((len(SHAPES), 12)), dma((len(SHAPES), 6, 2)), dma((len(SHAPES), 6, ROUNDS)), dma((5,))]
        + [vmem((tokens, d), BF)] * 2
        + [vmem((2, tokens, d), BF)]
        + [vmem((tokens, d), BF)] * 6
        + [vmem((tokens, F), BF)] * 3
        + [vmem((tokens, d), F32), vmem((PAIRS, 8, tokens), F32)],
        compiler_params=pltpu.CompilerParams(dimension_semantics=("arbitrary",), vmem_limit_bytes=VMEM, collective_id=0, has_side_effects=True),
        name="layer_and_sum",
    )(x, dy, w["wo"], jnp.asarray(turns), *(w[n] for n in ("wq", "wk", "wv", "w_gate", "w_up", "w_down")))[:2]


def solution(mesh):
    def step(x, dy, *arrays):
        weights, m, v = (dict(zip(NAMES, arrays[i : i + 7], strict=True)) for i in (0, 7, 14))
        w = {n: w[0] for n, w in weights.items()}
        sums = layer(x[0], dy[0], w)
        wide = UP[1]
        places = {"w_down": (0, 0, 0), "wo": (0, FEEDS * DOWN[0], 0), "w_gate": (1, 0, 0), "wq": (1, 0, (FEEDS + 1) * wide),
                  "w_up": (1, 0, ROUNDS * wide), "wk": (1, 0, (ROUNDS + FEEDS + 1) * wide), "wv": (1, 0, 2 * ROUNDS * wide)}
        order = ("w_down", "w_gate", "w_up", "wo", "wq", "wk", "wv")
        each = ([a[n][0] for n in order] for a in (weights, m, v))
        new = [dict(zip(order, one, strict=True)) for one in optimizer(*each, sums, tuple(places[n] for n in order))]
        return tuple(one[name][None] for one in new for name in NAMES)

    states, all_of = P(("rep", "dp"), None, None), P(None, None, None)
    return jax.shard_map(
        step,
        mesh=mesh,
        in_specs=(states, states) + (all_of,) * 21,
        out_specs=(P("rep", None, None),) * 21,
        check_vma=False,
    )
```

```python
import functools

import jax
import jax.numpy as jnp
import numpy as np
from jax import lax
from jax.experimental import pallas as pl
from jax.experimental.pallas import tpu as pltpu
from jax.sharding import PartitionSpec as P

HEAD = 128
THETA = 10000
NAMES = ("wq", "wk", "wv", "wo", "w_gate", "w_up", "w_down")
LOG2E = 1.4426950408889634
T = 256
F = 512
VMEM = 67043328
BF, F32 = jnp.bfloat16, jnp.float32


def _dots(ca, cb):
    return lambda a, b: lax.dot_general(a, b, (((ca,), (cb,)), ((), ())), preferred_element_type=F32)


_nn, _nt, _tn = _dots(1, 0), _dots(1, 1), _dots(0, 0)


def _turns(tokens):
    half = HEAD // 2
    angle = np.arange(tokens, dtype=np.float32)[:, None] * np.float32(THETA) ** (-np.arange(half, dtype=np.float32) / np.float32(half))
    return np.concatenate([np.cos(angle), np.sin(angle)], 1).astype(np.float32)


def _both(t):
    low, other = lax.broadcasted_iota(jnp.int32, t.shape, 1) < HEAD // 2, pltpu.roll(t, HEAD // 2, 1)
    return jnp.where(low, t, other), jnp.where(low, -other, t)


def _normed(wide):
    return wide * lax.rsqrt(jnp.mean(wide * wide, -1, keepdims=True) + 1e-6)


def _turn(t, c, s):
    t = t.astype(BF).astype(F32)
    parts = [t[:, at : at + HEAD] for at in range(0, t.shape[1], HEAD)]
    return jnp.concatenate([x * c + pltpu.roll(x, HEAD // 2, 1) * s for x in parts], 1).astype(BF)


def _hidden(s):
    n = s.shape[0]
    low = s[n - T :]
    ok = lax.broadcasted_iota(jnp.int32, (T, T), 0) <= lax.broadcasted_iota(jnp.int32, (T, T), 1)
    low = jnp.where(ok, low, -1e30)
    return low if n == T else jnp.concatenate([s[: n - T], low], 0)


def _adamw(w, m, v, g):
    m = 0.9 * m + 0.1 * g
    v = 0.95 * v + 0.05 * g * g
    step = m * lax.rsqrt(v + 1e-8) + 0.1 * w
    return (w - 0.02 * step).astype(BF), m, v


TILE = (128, 1024)
DEEP = 8
CHUNK = 16


def _optimizer(*refs, where):
    n = len(where)
    w, m, v = refs[:n], refs[n : 2 * n], refs[2 * n : 3 * n]
    g, refs = refs[3 * n : 3 * n + 2], refs[3 * n + 2 :]
    out, (wi, mi, vi, gi, wn, mn, vn, came, left) = (refs[:n], refs[n : 2 * n], refs[2 * n : 3 * n]), refs[3 * n :]
    rows, cols = TILE
    tiles = [(one.shape[0] // rows) * (one.shape[1] // cols) for one in w]
    first = [sum(tiles[:j]) for j in range(n + 1)]

    def part(j, t):
        across = w[j].shape[1] // cols
        return lax.div(t, across) * rows, lax.rem(t, across) * cols

    def tile(ref, row, col):
        return ref.at[pl.ds(pl.multiple_of(row, rows), rows), pl.ds(pl.multiple_of(col, 512), cols)]

    def loads(j, t, slot):
        row, col = part(j, t)
        at, r0, c0 = where[j]
        pairs = ((tile(w[j], row, col), wi), (tile(m[j], row, col), mi), (tile(v[j], row, col), vi), (tile(g[at], r0 + row, c0 + col), gi))
        return [pltpu.make_async_copy(src, dst.at[slot], came.at[k, slot]) for k, (src, dst) in enumerate(pairs)]

    def stores(j, t, slot):
        row, col = part(j, t)
        pairs = zip((wn, mn, vn), (tile(o[j], row, col) for o in out), strict=True)
        return [pltpu.make_async_copy(src.at[slot], dst, left.at[k, slot]) for k, (src, dst) in enumerate(pairs)]

    for k in range(DEEP - 1):
        for copy in loads(0, k, k):
            copy.start()
    for j in range(n):

        def body(t, _, j=j):
            k = first[j] + t
            slot = lax.rem(k, DEEP)
            ahead = k + DEEP - 1
            for other in range(j, n):
                if first[other] < first[j + 1] + DEEP - 1:

                    @pl.when((ahead >= first[other]) & (ahead < first[other + 1]))
                    def _():
                        for copy in loads(other, ahead - first[other], lax.rem(ahead, DEEP)):
                            copy.start()
            for copy in loads(j, t, slot):
                copy.wait()

            @pl.when(k >= DEEP)
            def _():
                for copy in stores(0, 0, slot):
                    copy.wait()

            def chunk(c, _):
                r = pl.ds(pl.multiple_of(c * CHUNK, CHUNK), CHUNK)
                wn[slot, r], mn[slot, r], vn[slot, r] = _adamw(wi[slot, r].astype(F32), mi[slot, r], vi[slot, r], gi[slot, r].astype(F32))

            lax.fori_loop(0, rows // CHUNK, chunk, None)
            for copy in stores(j, t, slot):
                copy.start()

        lax.fori_loop(0, tiles[j], body, None)
    for k in range(DEEP):
        for copy in stores(0, 0, k):
            copy.wait()


def optimizer(w, m, v, sums, where):
    like = [jax.ShapeDtypeStruct(one.shape, one.dtype) for one in (*w, *m, *v)]
    hbm, n = pl.BlockSpec(memory_space=pl.ANY), len(w)
    new = pl.pallas_call(
        functools.partial(_optimizer, where=where),
        in_specs=[hbm] * (3 * n + 2),
        out_specs=[hbm] * (3 * n),
        out_shape=like,
        scratch_shapes=[pltpu.VMEM((DEEP, *TILE), kind) for kind in (BF, F32, F32, BF, BF, F32, F32)]
        + [pltpu.SemaphoreType.DMA((4, DEEP)), pltpu.SemaphoreType.DMA((3, DEEP))],
        compiler_params=pltpu.CompilerParams(vmem_limit_bytes=VMEM),
        name="optimizer",
    )(*w, *m, *v, *sums)
    return new[:n], new[n : 2 * n], new[2 * n :]


RING = 4
OTHERS, NEXT = (1, 2, 3), (1, 3)
SHIFT = {"x": 5, "y": 3, "z": 1}
COLOURS = (("x", "y", "z"), ("y", "z", "x"), ("z", "x", "y"), ("x", "y", "z"))
TICKS = 3
AT = (0, 1, 2, 4, 5, 7, 8, 10, 11, 12, 14, 17, 20)


class Place:
    def __init__(self):
        me = lax.axis_index("dp")
        self.core = me & 1
        self.partner = me ^ 1
        self.at = {axis: (me >> shift) & 3 for axis, shift in SHIFT.items()}
        self.peers = {axis: {by: me + ((((self.at[axis] + by) & 3) - self.at[axis]) << shift) for by in OTHERS} for axis, shift in SHIFT.items()}

    def here(self):
        self.everyone = [self.partner] + [peer for axis in SHIFT for peer in self.peers[axis].values()]
        for peer in self.everyone:
            pl.semaphore_signal(pltpu.get_barrier_semaphore(), 1, device_id={"dp": peer})

    def meet(self):
        pl.semaphore_wait(pltpu.get_barrier_semaphore(), 1 + len(SHIFT) * (RING - 1))


class Sum:
    def __init__(self, colour, blk, place, local, out, refs, sems, slot, slot3):
        self.c, (self.R, self.C), self.slot, self.slot3, self.place = colour, blk, slot, slot3, place
        self.local, self.out = local, out
        self.rc, self.sa1, self.ra1, self.sa2, self.ra2, self.ra, self.sb1, self.rb1, self.sb2, self.rb2, self.rb, self.sc, self.rcc, self.all = refs
        self.send, self.recv, self.gather = sems
        self.core = place.core
        self.a, self.b, self.k = (place.at[axis] for axis in COLOURS[colour])
        self.first = (self.core * (self.R // 2), self.core * (self.R // 2) + self.a * (self.R // 8))
        self.first += (self.first[1] + self.b * (self.R // 32),)

    def peer(self, n, by):
        return self.place.peers[COLOURS[self.c][n]][by]

    def copy(self, src, dst, kind, device, slot=None, r=None):
        recv = self.recv.at[self.c, kind, slot] if r is None else self.gather.at[self.c, kind - 6, r]
        return pltpu.make_async_remote_copy(src, dst, self.send.at[self.c, kind], recv, device_id={"dp": device})

    def wait(self, ref, kind, slot=None, r=None, send=None):
        recv = self.recv.at[self.c, kind, slot] if r is None else self.gather.at[self.c, kind - 6, r]
        pltpu.make_async_copy(ref, ref, recv).wait()
        ref = ref if send is None else send
        pltpu.make_async_copy(ref, ref, self.send.at[self.c, kind]).wait()

    def quarter(self, r, by, half=None):
        n8 = self.R // 8
        q = (self.a + by) & 3
        cols = slice(None) if half is None else pl.ds(half * (self.C // 2), self.C // 2)
        mine = self.local[self.slot(r), pl.ds(pl.multiple_of(self.first[0] + q * n8, 16), n8), cols]
        return mine.astype(F32) + self.rc[self.slot3(r), pl.ds(pl.multiple_of(q * n8, 16), n8), cols].astype(F32)

    def cols(self, q):
        return pl.ds(pl.multiple_of(q * (self.C // 4), 128), self.C // 4)

    def stage(self, n, r):
        R, C = self.R, self.C
        slot = self.slot(r)
        n8, n32, half = R // 8, R // 32, C // 2
        left, right = pl.ds(0, half), pl.ds(half, half)
        f32 = lambda v: v.astype(F32)
        low = lambda v: v.astype(BF)
        if n == 0:
            other = pl.ds(pl.multiple_of((1 - self.core) * (R // 2), 16), R // 2)
            self.copy(self.local.at[slot, other], self.rc.at[self.slot3(r)], 0, self.place.partner, slot).start()
        elif n == 1:
            self.wait(self.rc.at[self.slot3(r)], 0, slot)
            self.sa1[:] = low(self.quarter(r, 2))
            self.both(self.sa1, self.ra1, 1, 0, slot, left, right)
        elif n == 2:
            self.wait(self.ra1.at[slot], 1, slot)
            self.sa2[0, :, :half] = low(self.quarter(r, 1, 0) + f32(self.ra1[slot, :, :half]))
            self.sa2[0, :, half:] = low(self.quarter(r, 1, 1))
            self.sa2[1, :, :half] = low(self.quarter(r, 3, 0))
            self.sa2[1, :, half:] = low(self.quarter(r, 3, 1) + f32(self.ra1[slot, :, half:]))
            self.pair(self.sa2, self.ra2, 2, 0, slot)
        elif n == 3:
            self.wait(self.ra2.at[slot], 2, slot)
            self.ra[:] = self.quarter(r, 0) + f32(self.ra2[slot, 0]) + f32(self.ra2[slot, 1])
            self.sb1[:] = low(self.ra[self.sixteenth(2)])
            self.both(self.sb1, self.rb1, 3, 1, slot, left, right)
        elif n == 4:
            self.wait(self.rb1.at[slot], 3, slot)
            up, down = self.sixteenth(1), self.sixteenth(3)
            self.sb2[0, :, :half] = low(self.ra[up, :half] + f32(self.rb1[slot, :, :half]))
            self.sb2[0, :, half:] = low(self.ra[up, half:])
            self.sb2[1, :, :half] = low(self.ra[down, :half])
            self.sb2[1, :, half:] = low(self.ra[down, half:] + f32(self.rb1[slot, :, half:]))
            self.pair(self.sb2, self.rb2, 4, 1, slot)
        elif n == 5:
            self.wait(self.rb2.at[slot], 4, slot)
            total = self.ra[self.sixteenth(0)] + f32(self.rb2[slot, 0]) + f32(self.rb2[slot, 1])
            self.rb[:] = total
            self.sc[:] = low(total)
            for by in OTHERS:
                to = (self.k + by) & 3
                self.copy(self.sc.at[:, self.cols(to)], self.rcc.at[slot, by - 1], 5, self.peer(2, by), slot).start()
        elif n == 6:
            self.wait(self.rcc.at[slot], 5, slot)
            total = self.rb[:, self.cols(self.k)]
            for by in range(3):
                total = total + f32(self.rcc[slot, by])
            self.all[r & 3, self.sixteenth(0), self.cols(self.k)] = low(total)
            mine = self.all.at[r & 3, self.sixteenth(0), self.cols(self.k)]
            for by in OTHERS:
                self.copy(mine, mine, 6, self.peer(2, by), r=r).start()
        elif n == 7:
            self.wait(self.rcc.at[slot], 6, r=r)
            mine = self.all.at[r & 3, self.sixteenth(0)]
            for by in NEXT:
                self.copy(mine, mine, 7, self.peer(1, by), r=r).start()
        elif n == 8:
            self.wait(self.all.at[r & 3, pl.ds(0, 2 * n32)], 7, r=r)
            self.onward(lambda by: self.all.at[r & 3, self.sixteenth(by)], r, 8, 1, left, right)
        elif n == 9:
            self.wait(self.all.at[r & 3, pl.ds(0, n32)], 8, r=r)
            whole, mine = self.all.at[r & 3], self.out(r, self.first[1], n8)
            pltpu.make_async_copy(whole, mine, self.gather.at[self.c, 3, r]).start()
            for by in NEXT:
                self.copy(whole, mine, 9, self.peer(0, by), r=r).start()
        elif n == 10:
            self.wait(self.out(r, 0, 3 * n8), 9, r=r, send=self.out(r, 0, 2 * n8))
            self.onward(lambda by: self.out(r, self.first[0] + ((self.a + by) & 3) * n8, n8), r, 10, 0, left, right)
        elif n == 11:
            self.wait(self.out(r, 0, n8), 10, r=r)
            mine = self.out(r, self.first[0], R // 2)
            self.copy(mine, mine, 11, self.place.partner, r=r).start()
        else:
            self.wait(self.out(r, 0, R // 2), 11, r=r)

    def sixteenth(self, by):
        return pl.ds(pl.multiple_of(((self.b + by) & 3) * (self.R // 32), 16), self.R // 32)

    def both(self, src, dst, kind, axis, slot, left, right):
        self.copy(src.at[:, left], dst.at[slot, :, left], kind, self.peer(axis, 1), slot).start()
        self.copy(src.at[:, right], dst.at[slot, :, right], kind, self.peer(axis, 3), slot).start()

    def pair(self, src, dst, kind, axis, slot):
        self.copy(src.at[0], dst.at[slot, 0], kind, self.peer(axis, 1), slot).start()
        self.copy(src.at[1], dst.at[slot, 1], kind, self.peer(axis, 3), slot).start()

    def onward(self, part, r, kind, axis, left, right):
        before, after = part(3).at[:, left], part(1).at[:, right]
        self.copy(before, before, kind, self.peer(axis, 1), r=r).start()
        self.copy(after, after, kind, self.peer(axis, 3), r=r).start()


def _sum_scratch(R, C, deep):
    n2, n8, n32 = R // 2, R // 8, R // 32
    return [pltpu.VMEM(shape, kind) for shape, kind in (
        ((deep, n2, C), BF), ((n8, C), BF), ((2, n8, C), BF), ((2, n8, C), BF), ((2, 2, n8, C), BF), ((n8, C), F32),
        ((n32, C), BF), ((2, n32, C), BF), ((2, n32, C), BF), ((2, 2, n32, C), BF), ((n32, C), F32), ((n32, C), BF), ((2, 3, n32, C // 4), BF),
        ((4, n8, C), BF))]


SUM_REFS = 14


def _stages(step, sums, tick, on):
    for n in reversed(range(len(AT))):
        if AT[n] % TICKS == tick:
            r = step - 1 - AT[n] // TICKS
            for c, one in enumerate(sums):

                @pl.when(on(c, r))
                def _():
                    one.stage(n, r)


DOWN, UP = (512, 1024), (1024, 512)
SHAPES = (DOWN, UP, UP, UP)
PAIRS = 4
FEEDS = 8
ROUNDS = FEEDS + 3


def _has(c, r):
    if c == 0:
        return (r >= 0) & (r <= FEEDS + 1)
    if c == 3:
        return (r > FEEDS) & (r < ROUNDS)
    return (r >= 0) & (r < ROUNDS) & (r != FEEDS)


def _slots(c, n):
    if c in (0, 3):
        return lambda r: lax.rem(r, n)
    if n == 2:
        return lambda r: (r + jnp.where(r > FEEDS, 1, 0)) & 1
    return lambda r: lax.rem(r - jnp.where(r > FEEDS, 1, 0), n)


def _layer(x_hbm, dy_hbm, wo_hbm, t_ref, wq_ref, wk_ref, wv_ref, wg_ref, wu_ref, wd_ref, rows_out, cols_out, weights_out, *scratch):
    n, colours = SUM_REFS, len(SHAPES)
    parts, rest = [scratch[c * n : (c + 1) * n] for c in range(colours)], scratch[colours * n :]
    locals_, (send, recv, gather, load), rest = rest[:colours], rest[colours : colours + 4], rest[colours + 4 :]
    x1, x2, xs, q, k, v, o, wo, at, act, dg, du, acc, shares = rest
    x3, x4 = xs.at[0], xs.at[1]
    l0, l1, l2, l3 = locals_
    i = pl.program_id(0) - PAIRS
    tokens = x1.shape[0]
    rows, halves = ([slice(r, r + n) for r in range(0, tokens, n)] for n in (T, F))
    scale = HEAD**-0.5
    e = scale * LOG2E

    def in_rows(r, first, size):
        return rows_out.at[pl.ds(pl.multiple_of(r * DOWN[0] + first, 16), size)]

    def in_cols(c):
        block = lambda r: (c - 1) * ROUNDS + r - (FEEDS + 1 if c == 3 else 0)
        return lambda r, first, size: cols_out.at[pl.ds(pl.multiple_of(first, 16), size), pl.ds(pl.multiple_of(block(r) * UP[1], 128), UP[1])]

    place = Place()
    sums = [Sum(c, SHAPES[c], place, locals_[c], in_cols(c) if c else in_rows, parts[c], (send, recv, gather), _slots(c, 2), _slots(c, 3 if c < 3 else 2))
            for c in range(colours)]
    s0, s1 = _slots(0, 2)(i), _slots(1, 2)(i)

    loads = [pltpu.make_async_copy(src, dst, load.at[n]) for n, (src, dst) in enumerate(((x_hbm, x4), (wo_hbm, wo), (dy_hbm, x2)))]
    pair = i + PAIRS
    saves = [pltpu.make_async_copy(src, weights_out.at[jnp.clip(pair, 0, PAIRS - 1) * 2 + n], load.at[3 + n]) for n, src in enumerate((x2, x3))]

    @pl.when(pair == 0)
    def _():
        loads[0].start()
        place.here()
        loads[0].wait()
        loads[1].start()
        for r in rows:
            a = _normed(x4[r].astype(F32)).astype(BF)
            x1[r] = a
            at[:, r] = a.T

    @pl.when((pair > 0) & (i < 0))
    def _():
        for one in saves:
            one.wait()

    @pl.when(i == 0)
    def _():
        place.meet()
        acc[:] = jnp.zeros_like(acc)

    def forward():
        both = pl.ds(pl.multiple_of(pair * 2 * HEAD, 2 * HEAD), 2 * HEAD)
        heads = [(n, pl.ds(pl.multiple_of((pair * 2 + n) * HEAD, HEAD), HEAD)) for n in range(2)]
        for r in halves:
            a, turns = x1[r], _both(t_ref[r])
            q[r, both] = _turn(_nn(a, wq_ref[:]), *turns)
            k[r, both] = _turn(_nn(a, wk_ref[:]), *turns)
            v[r, both] = _nn(a, wv_ref[:]).astype(BF)

        def spot(j, n):
            return slice((j % 2 * 2 + n) * T, (j % 2 * 2 + n + 1) * T)

        def score(j):
            for n, cols in heads:
                acc[: rows[j].stop, spot(j, n)] = _hidden(_nt(k[: rows[j].stop, cols], q[rows[j], cols]))

        score(0)
        for j, r in enumerate(rows):
            if r.stop < tokens:
                score(j + 1)
            keys = slice(0, r.stop)
            for (n, cols), kept in zip(heads, (x2, x3)):
                s = acc[keys, spot(j, n)]
                p = jnp.exp2((s - s.max(axis=0, keepdims=True)) * e).astype(BF)
                kept[keys, r] = p
                mix = _nn(jnp.concatenate([v[keys, cols].T, jnp.ones((8, r.stop), BF)], 0), p)
                share = 1 / mix[HEAD : HEAD + 1]
                o[r, cols] = (mix[:HEAD] * share).T.astype(BF)
                shares[pair, n : n + 1, r] = share
        for one in saves:
            one.start()

    def onto_residual():
        for one in saves:
            one.wait()
        loads[2].start()
        loads[1].wait()
        for r in halves:
            h = x4[r] + _nn(o[r], wo[:]).astype(BF)
            x4[r] = h
            b = _normed(h.astype(F32)).astype(BF)
            x1[r] = b
            x3[:, r] = b.T
        loads[2].wait()

    def units(r):
        b = x1[r]
        gate, up = _nn(b, wg_ref[:]), _nn(b, wu_ref[:])
        da = _nt(x2[r], wd_ref[:]).astype(BF).astype(F32)
        sig = 1 / (1 + jnp.exp2(gate * -LOG2E))
        silu = gate * sig
        act[r] = (silu * up).astype(BF)
        du[r] = (da * silu).astype(BF)
        dg[r] = (da * up * (sig + silu * (1 - sig))).astype(BF)

    def inward(part):
        acc[:, part] += _nt(dg[:], wg_ref[part]) + _nt(du[:], wu_ref[part])

    def norm_back():
        for r in halves:
            wide, ct = x4[r].astype(F32), acc[r].astype(BF).astype(F32)
            scale = lax.rsqrt(jnp.mean(wide * wide, -1, keepdims=True) + 1e-6)
            back = ct * scale - wide * (scale * scale * scale * jnp.mean(ct * wide, -1, keepdims=True))
            dh = x2[r] + back.astype(BF)
            x2[r] = dh
            x1[r] = _nt(dh, wo[:]).astype(BF)

    def head(n, to):
        cols = pl.ds(pl.multiple_of(n * HEAD, HEAD), HEAD)
        to = pl.ds(pl.multiple_of(to * HEAD, HEAD), HEAD)
        dk, dv = slice(0, HEAD), slice(HEAD, 2 * HEAD)
        for r in reversed(rows):
            keys = slice(0, r.stop)
            dor, qr = x1[r, cols], q[r, cols]
            delta = (dor.astype(F32) * o[r, cols].astype(F32)).T.sum(axis=0, keepdims=True)
            p = xs[n & 1, keys, r].astype(F32) * shares[lax.div(n, 2), pl.ds(n & 1, 1), r]
            ds = (p * (_nt(v[keys, cols], dor) - delta)).astype(BF)
            if r.stop == tokens:
                acc[keys, dv] = _nn(p.astype(BF), dor)
                acc[keys, dk] = _nn(ds, qr)
            else:
                acc[keys, dv] += _nn(p.astype(BF), dor)
                acc[keys, dk] += _nn(ds, qr)
            t = (_tn(k[keys, cols], ds) * scale).T.astype(BF).astype(F32)
            cos, sin = _both(t_ref[r])
            dg[r, to] = (t * cos - pltpu.roll(t, HEAD // 2, 1) * sin).astype(BF)
        for r in rows:
            act[r, to] = acc[r, dv].astype(BF)
            t = (acc[r, dk] * scale).astype(BF).astype(F32)
            cos, sin = _both(t_ref[r])
            du[r, to] = (t * cos - pltpu.roll(t, HEAD // 2, 1) * sin).astype(BF)

    def recall(n):
        return pltpu.make_async_copy(weights_out.at[n], xs.at[n & 1], load.at[3 + (n & 1)])

    feeding = (i >= 0) & (i < FEEDS)
    attending = (i == FEEDS + 1) | (i == FEEDS + 2)

    def ticking(tick, _):
        for one in range(TICKS):

            @pl.when(tick == one)
            def _():
                _stages(i, sums, one, _has)

        @pl.when((i < 0) & (tick == 0))
        def _():
            forward()

        @pl.when((i == -1) & (tick == 1))
        def _():
            onto_residual()

        @pl.when(feeding & (tick == 0))
        def _():
            for r in halves:
                units(r)

        @pl.when(feeding & (tick == 1))
        def _():
            l0[s0] = _tn(act[:], x2[:]).astype(BF)
            l1[s1] = _nn(x3[:], dg[:]).astype(BF)
            inward(halves[0])

        @pl.when(feeding & (tick == 2))
        def _():
            l2[s1] = _nn(x3[:], du[:]).astype(BF)
            inward(halves[1])

        @pl.when((i == FEEDS) & (tick == 0))
        def _():
            recall(0).start()
            norm_back()
            recall(1).start()

        @pl.when(((i == FEEDS) | (i == FEEDS + 1)) & (tick == 2))
        def _():
            l0[s0] = _tn(o[:, pl.ds(pl.multiple_of((i - FEEDS) * F, F), F)], x2[:]).astype(BF)

        @pl.when(attending)
        def _():
            def one(j, _):
                n = (i - FEEDS - 1) * PAIRS + j
                recall(n).wait()
                head(n, j)

                @pl.when(n + 2 < 2 * PAIRS)
                def _():
                    recall(n + 2).start()

            begin = lambda t: t + (t >> 1)
            lax.fori_loop(begin(tick), begin(tick + 1), one, None)

        @pl.when(attending & (tick == TICKS - 1))
        def _():
            l1[s1] = _nn(at[:], dg[:]).astype(BF)
            l2[s1] = _nn(at[:], du[:]).astype(BF)
            l3[s0] = _nn(at[:], act[:]).astype(BF)

    lax.fori_loop(0, TICKS, ticking, None)


def layer(x, dy, w):
    tokens, d = x.shape
    turns = _turns(tokens)
    hbm = pl.BlockSpec(memory_space=pl.ANY)
    upto = lambda i, n: jnp.clip(i, 0, n - 1)
    heads = pl.BlockSpec((d, 2 * HEAD), lambda i: (0, upto(i, PAIRS)))
    feed = pl.BlockSpec(UP, lambda i: (0, upto(i - PAIRS, FEEDS)))
    down = pl.BlockSpec(DOWN, lambda i: (upto(i - PAIRS, FEEDS), 0))
    dma, vmem = pltpu.SemaphoreType.DMA, pltpu.VMEM
    return pl.pallas_call(
        _layer,
        grid=(PAIRS + ROUNDS + 1 + AT[-1] // TICKS,),
        in_specs=[hbm] * 3 + [pl.BlockSpec(turns.shape, lambda i: (0, 0), pipeline_mode=pl.Buffered(1))] + [heads] * 3 + [feed, feed, down],
        out_specs=[hbm] * 3,
        out_shape=[jax.ShapeDtypeStruct(shape, BF) for shape in (
            (DOWN[0] * (FEEDS + 2), DOWN[1]), (UP[0], (2 * ROUNDS + 2) * UP[1]), (2 * PAIRS, tokens, tokens))],
        scratch_shapes=[one for c, shape in enumerate(SHAPES) for one in _sum_scratch(*shape, 3 if c < 3 else 2)]
        + [vmem((2, *shape), BF) for shape in SHAPES]
        + [dma((len(SHAPES), 12)), dma((len(SHAPES), 6, 2)), dma((len(SHAPES), 6, ROUNDS)), dma((5,))]
        + [vmem((tokens, d), BF)] * 2
        + [vmem((2, tokens, d), BF)]
        + [vmem((tokens, d), BF)] * 6
        + [vmem((tokens, F), BF)] * 3
        + [vmem((tokens, d), F32), vmem((PAIRS, 8, tokens), F32)],
        compiler_params=pltpu.CompilerParams(dimension_semantics=("arbitrary",), vmem_limit_bytes=VMEM, collective_id=0, has_side_effects=True),
        name="layer_and_sum",
    )(x, dy, w["wo"], jnp.asarray(turns), *(w[n] for n in ("wq", "wk", "wv", "w_gate", "w_up", "w_down")))[:2]


def solution(mesh):
    def step(x, dy, *arrays):
        weights, m, v = (dict(zip(NAMES, arrays[i : i + 7], strict=True)) for i in (0, 7, 14))
        w = {n: w[0] for n, w in weights.items()}
        sums = layer(x[0], dy[0], w)
        wide = UP[1]
        places = {"w_down": (0, 0, 0), "wo": (0, FEEDS * DOWN[0], 0), "w_gate": (1, 0, 0), "wq": (1, 0, (FEEDS + 1) * wide),
                  "w_up": (1, 0, ROUNDS * wide), "wk": (1, 0, (ROUNDS + FEEDS + 1) * wide), "wv": (1, 0, 2 * ROUNDS * wide)}
        order = ("w_down", "w_gate", "w_up", "wo", "wq", "wk", "wv")
        each = ([a[n][0] for n in order] for a in (weights, m, v))
        new = [dict(zip(order, one, strict=True)) for one in optimizer(*each, sums, tuple(places[n] for n in order))]
        return tuple(one[name][None] for one in new for name in NAMES)

    states, all_of = P(("rep", "dp"), None, None), P(None, None, None)
    return jax.shard_map(
        step,
        mesh=mesh,
        in_specs=(states, states) + (all_of,) * 21,
        out_specs=(P("rep", None, None),) * 21,
        check_vma=False,
    )
```

```python
import functools

import jax
import jax.numpy as jnp
import numpy as np
from jax import lax
from jax.experimental import pallas as pl
from jax.experimental.pallas import tpu as pltpu
from jax.sharding import PartitionSpec as P

HEAD = 128
THETA = 10000
NAMES = ("wq", "wk", "wv", "wo", "w_gate", "w_up", "w_down")
LOG2E = 1.4426950408889634
T = 256
F = 512
VMEM = 67043328
BF, F32 = jnp.bfloat16, jnp.float32


def _dots(ca, cb):
    return lambda a, b: lax.dot_general(a, b, (((ca,), (cb,)), ((), ())), preferred_element_type=F32)


_nn, _nt, _tn = _dots(1, 0), _dots(1, 1), _dots(0, 0)


def _turns(tokens):
    half = HEAD // 2
    angle = np.arange(tokens, dtype=np.float32)[:, None] * np.float32(THETA) ** (-np.arange(half, dtype=np.float32) / np.float32(half))
    return np.concatenate([np.cos(angle), np.sin(angle)], 1).astype(np.float32)


def _both(t):
    low, other = lax.broadcasted_iota(jnp.int32, t.shape, 1) < HEAD // 2, pltpu.roll(t, HEAD // 2, 1)
    return jnp.where(low, t, other), jnp.where(low, -other, t)


def _normed(wide):
    return wide * lax.rsqrt(jnp.mean(wide * wide, -1, keepdims=True) + 1e-6)


def _turn(t, c, s):
    t = t.astype(BF).astype(F32)
    parts = [t[:, at : at + HEAD] for at in range(0, t.shape[1], HEAD)]
    return jnp.concatenate([x * c + pltpu.roll(x, HEAD // 2, 1) * s for x in parts], 1).astype(BF)


def _hidden(s):
    n = s.shape[0]
    low = s[n - T :]
    ok = lax.broadcasted_iota(jnp.int32, (T, T), 0) <= lax.broadcasted_iota(jnp.int32, (T, T), 1)
    low = jnp.where(ok, low, -1e30)
    return low if n == T else jnp.concatenate([s[: n - T], low], 0)


def _adamw(w, m, v, g):
    m = 0.9 * m + 0.1 * g
    v = 0.95 * v + 0.05 * g * g
    step = m * lax.rsqrt(v + 1e-8) + 0.1 * w
    return (w - 0.02 * step).astype(BF), m, v


TILE = (128, 1024)
DEEP = 8
CHUNK = 16


def _optimizer(*refs, where):
    n = len(where)
    w, m, v = refs[:n], refs[n : 2 * n], refs[2 * n : 3 * n]
    g, refs = refs[3 * n : 3 * n + 2], refs[3 * n + 2 :]
    out, (wi, mi, vi, gi, wn, mn, vn, came, left) = (refs[:n], refs[n : 2 * n], refs[2 * n : 3 * n]), refs[3 * n :]
    rows, cols = TILE
    tiles = [(one.shape[0] // rows) * (one.shape[1] // cols) for one in w]
    first = [sum(tiles[:j]) for j in range(n + 1)]

    def part(j, t):
        across = w[j].shape[1] // cols
        return lax.div(t, across) * rows, lax.rem(t, across) * cols

    def tile(ref, row, col):
        return ref.at[pl.ds(pl.multiple_of(row, rows), rows), pl.ds(pl.multiple_of(col, 512), cols)]

    def loads(j, t, slot):
        row, col = part(j, t)
        at, r0, c0 = where[j]
        pairs = ((tile(w[j], row, col), wi), (tile(m[j], row, col), mi), (tile(v[j], row, col), vi), (tile(g[at], r0 + row, c0 + col), gi))
        return [pltpu.make_async_copy(src, dst.at[slot], came.at[k, slot]) for k, (src, dst) in enumerate(pairs)]

    def stores(j, t, slot):
        row, col = part(j, t)
        pairs = zip((wn, mn, vn), (tile(o[j], row, col) for o in out), strict=True)
        return [pltpu.make_async_copy(src.at[slot], dst, left.at[k, slot]) for k, (src, dst) in enumerate(pairs)]

    for k in range(DEEP - 1):
        for copy in loads(0, k, k):
            copy.start()
    for j in range(n):

        def body(t, _, j=j):
            k = first[j] + t
            slot = lax.rem(k, DEEP)
            ahead = k + DEEP - 1
            for other in range(j, n):
                if first[other] < first[j + 1] + DEEP - 1:

                    @pl.when((ahead >= first[other]) & (ahead < first[other + 1]))
                    def _():
                        for copy in loads(other, ahead - first[other], lax.rem(ahead, DEEP)):
                            copy.start()
            for copy in loads(j, t, slot):
                copy.wait()

            @pl.when(k >= DEEP)
            def _():
                for copy in stores(0, 0, slot):
                    copy.wait()

            def chunk(c, _):
                r = pl.ds(pl.multiple_of(c * CHUNK, CHUNK), CHUNK)
                wn[slot, r], mn[slot, r], vn[slot, r] = _adamw(wi[slot, r].astype(F32), mi[slot, r], vi[slot, r], gi[slot, r].astype(F32))

            lax.fori_loop(0, rows // CHUNK, chunk, None)
            for copy in stores(j, t, slot):
                copy.start()

        lax.fori_loop(0, tiles[j], body, None)
    for k in range(DEEP):
        for copy in stores(0, 0, k):
            copy.wait()


def optimizer(w, m, v, sums, where):
    like = [jax.ShapeDtypeStruct(one.shape, one.dtype) for one in (*w, *m, *v)]
    hbm, n = pl.BlockSpec(memory_space=pl.ANY), len(w)
    new = pl.pallas_call(
        functools.partial(_optimizer, where=where),
        in_specs=[hbm] * (3 * n + 2),
        out_specs=[hbm] * (3 * n),
        out_shape=like,
        scratch_shapes=[pltpu.VMEM((DEEP, *TILE), kind) for kind in (BF, F32, F32, BF, BF, F32, F32)]
        + [pltpu.SemaphoreType.DMA((4, DEEP)), pltpu.SemaphoreType.DMA((3, DEEP))],
        compiler_params=pltpu.CompilerParams(vmem_limit_bytes=VMEM),
        name="optimizer",
    )(*w, *m, *v, *sums)
    return new[:n], new[n : 2 * n], new[2 * n :]


RING = 4
OTHERS, NEXT = (1, 2, 3), (1, 3)
SHIFT = {"x": 5, "y": 3, "z": 1}
COLOURS = (("x", "y", "z"), ("y", "z", "x"), ("z", "x", "y"), ("x", "y", "z"))
TICKS = 3
AT = (0, 1, 2, 4, 5, 7, 8, 10, 11, 12, 14, 16, 19)


class Place:
    def __init__(self):
        me = lax.axis_index("dp")
        self.core = me & 1
        self.partner = me ^ 1
        self.at = {axis: (me >> shift) & 3 for axis, shift in SHIFT.items()}
        self.peers = {axis: {by: me + ((((self.at[axis] + by) & 3) - self.at[axis]) << shift) for by in OTHERS} for axis, shift in SHIFT.items()}

    def here(self):
        self.everyone = [self.partner] + [peer for axis in SHIFT for peer in self.peers[axis].values()]
        for peer in self.everyone:
            pl.semaphore_signal(pltpu.get_barrier_semaphore(), 1, device_id={"dp": peer})

    def meet(self):
        pl.semaphore_wait(pltpu.get_barrier_semaphore(), 1 + len(SHIFT) * (RING - 1))


class Sum:
    def __init__(self, colour, blk, place, local, out, refs, sems, slot, slot3):
        self.c, (self.R, self.C), self.slot, self.slot3, self.place = colour, blk, slot, slot3, place
        self.local, self.out = local, out
        self.rc, self.sa1, self.ra1, self.sa2, self.ra2, self.ra, self.sb1, self.rb1, self.sb2, self.rb2, self.rb, self.sc, self.rcc, self.all = refs
        self.send, self.recv, self.gather = sems
        self.core = place.core
        self.a, self.b, self.k = (place.at[axis] for axis in COLOURS[colour])
        self.first = (self.core * (self.R // 2), self.core * (self.R // 2) + self.a * (self.R // 8))
        self.first += (self.first[1] + self.b * (self.R // 32),)

    def peer(self, n, by):
        return self.place.peers[COLOURS[self.c][n]][by]

    def copy(self, src, dst, kind, device, slot=None, r=None):
        recv = self.recv.at[self.c, kind, slot] if r is None else self.gather.at[self.c, kind - 6, r]
        return pltpu.make_async_remote_copy(src, dst, self.send.at[self.c, kind], recv, device_id={"dp": device})

    def wait(self, ref, kind, slot=None, r=None, send=None):
        recv = self.recv.at[self.c, kind, slot] if r is None else self.gather.at[self.c, kind - 6, r]
        pltpu.make_async_copy(ref, ref, recv).wait()
        ref = ref if send is None else send
        pltpu.make_async_copy(ref, ref, self.send.at[self.c, kind]).wait()

    def quarter(self, r, by, half=None):
        n8 = self.R // 8
        q = (self.a + by) & 3
        cols = slice(None) if half is None else pl.ds(half * (self.C // 2), self.C // 2)
        mine = self.local[self.slot(r), pl.ds(pl.multiple_of(self.first[0] + q * n8, 16), n8), cols]
        return mine.astype(F32) + self.rc[self.slot3(r), pl.ds(pl.multiple_of(q * n8, 16), n8), cols].astype(F32)

    def cols(self, q):
        return pl.ds(pl.multiple_of(q * (self.C // 4), 128), self.C // 4)

    def stage(self, n, r):
        R, C = self.R, self.C
        slot = self.slot(r)
        n8, n32, half = R // 8, R // 32, C // 2
        left, right = pl.ds(0, half), pl.ds(half, half)
        f32 = lambda v: v.astype(F32)
        low = lambda v: v.astype(BF)
        if n == 0:
            other = pl.ds(pl.multiple_of((1 - self.core) * (R // 2), 16), R // 2)
            self.copy(self.local.at[slot, other], self.rc.at[self.slot3(r)], 0, self.place.partner, slot).start()
        elif n == 1:
            self.wait(self.rc.at[self.slot3(r)], 0, slot)
            self.sa1[:] = low(self.quarter(r, 2))
            self.both(self.sa1, self.ra1, 1, 0, slot, left, right)
        elif n == 2:
            self.wait(self.ra1.at[slot], 1, slot)
            self.sa2[0, :, :half] = low(self.quarter(r, 1, 0) + f32(self.ra1[slot, :, :half]))
            self.sa2[0, :, half:] = low(self.quarter(r, 1, 1))
            self.sa2[1, :, :half] = low(self.quarter(r, 3, 0))
            self.sa2[1, :, half:] = low(self.quarter(r, 3, 1) + f32(self.ra1[slot, :, half:]))
            self.pair(self.sa2, self.ra2, 2, 0, slot)
        elif n == 3:
            self.wait(self.ra2.at[slot], 2, slot)
            self.ra[:] = self.quarter(r, 0) + f32(self.ra2[slot, 0]) + f32(self.ra2[slot, 1])
            self.sb1[:] = low(self.ra[self.sixteenth(2)])
            self.both(self.sb1, self.rb1, 3, 1, slot, left, right)
        elif n == 4:
            self.wait(self.rb1.at[slot], 3, slot)
            up, down = self.sixteenth(1), self.sixteenth(3)
            self.sb2[0, :, :half] = low(self.ra[up, :half] + f32(self.rb1[slot, :, :half]))
            self.sb2[0, :, half:] = low(self.ra[up, half:])
            self.sb2[1, :, :half] = low(self.ra[down, :half])
            self.sb2[1, :, half:] = low(self.ra[down, half:] + f32(self.rb1[slot, :, half:]))
            self.pair(self.sb2, self.rb2, 4, 1, slot)
        elif n == 5:
            self.wait(self.rb2.at[slot], 4, slot)
            total = self.ra[self.sixteenth(0)] + f32(self.rb2[slot, 0]) + f32(self.rb2[slot, 1])
            self.rb[:] = total
            self.sc[:] = low(total)
            for by in OTHERS:
                to = (self.k + by) & 3
                self.copy(self.sc.at[:, self.cols(to)], self.rcc.at[slot, by - 1], 5, self.peer(2, by), slot).start()
        elif n == 6:
            self.wait(self.rcc.at[slot], 5, slot)
            total = self.rb[:, self.cols(self.k)]
            for by in range(3):
                total = total + f32(self.rcc[slot, by])
            self.all[r & 3, self.sixteenth(0), self.cols(self.k)] = low(total)
            mine = self.all.at[r & 3, self.sixteenth(0), self.cols(self.k)]
            for by in OTHERS:
                self.copy(mine, mine, 6, self.peer(2, by), r=r).start()
        elif n == 7:
            self.wait(self.rcc.at[slot], 6, r=r)
            mine = self.all.at[r & 3, self.sixteenth(0)]
            for by in NEXT:
                self.copy(mine, mine, 7, self.peer(1, by), r=r).start()
        elif n == 8:
            self.wait(self.all.at[r & 3, pl.ds(0, 2 * n32)], 7, r=r)
            self.onward(lambda by: self.all.at[r & 3, self.sixteenth(by)], r, 8, 1, left, right)
        elif n == 9:
            self.wait(self.all.at[r & 3, pl.ds(0, n32)], 8, r=r)
            whole, mine = self.all.at[r & 3], self.out(r, self.first[1], n8)
            pltpu.make_async_copy(whole, mine, self.gather.at[self.c, 3, r]).start()
            for by in NEXT:
                self.copy(whole, mine, 9, self.peer(0, by), r=r).start()
        elif n == 10:
            self.wait(self.out(r, 0, 3 * n8), 9, r=r, send=self.out(r, 0, 2 * n8))
            self.onward(lambda by: self.out(r, self.first[0] + ((self.a + by) & 3) * n8, n8), r, 10, 0, left, right)
        elif n == 11:
            self.wait(self.out(r, 0, n8), 10, r=r)
            mine = self.out(r, self.first[0], R // 2)
            self.copy(mine, mine, 11, self.place.partner, r=r).start()
        else:
            self.wait(self.out(r, 0, R // 2), 11, r=r)

    def sixteenth(self, by):
        return pl.ds(pl.multiple_of(((self.b + by) & 3) * (self.R // 32), 16), self.R // 32)

    def both(self, src, dst, kind, axis, slot, left, right):
        self.copy(src.at[:, left], dst.at[slot, :, left], kind, self.peer(axis, 1), slot).start()
        self.copy(src.at[:, right], dst.at[slot, :, right], kind, self.peer(axis, 3), slot).start()

    def pair(self, src, dst, kind, axis, slot):
        self.copy(src.at[0], dst.at[slot, 0], kind, self.peer(axis, 1), slot).start()
        self.copy(src.at[1], dst.at[slot, 1], kind, self.peer(axis, 3), slot).start()

    def onward(self, part, r, kind, axis, left, right):
        before, after = part(3).at[:, left], part(1).at[:, right]
        self.copy(before, before, kind, self.peer(axis, 1), r=r).start()
        self.copy(after, after, kind, self.peer(axis, 3), r=r).start()


def _sum_scratch(R, C, deep):
    n2, n8, n32 = R // 2, R // 8, R // 32
    return [pltpu.VMEM(shape, kind) for shape, kind in (
        ((deep, n2, C), BF), ((n8, C), BF), ((2, n8, C), BF), ((2, n8, C), BF), ((2, 2, n8, C), BF), ((n8, C), F32),
        ((n32, C), BF), ((2, n32, C), BF), ((2, n32, C), BF), ((2, 2, n32, C), BF), ((n32, C), F32), ((n32, C), BF), ((2, 3, n32, C // 4), BF),
        ((4, n8, C), BF))]


SUM_REFS = 14


def _stages(step, sums, tick, on):
    for n in sorted(range(len(AT)), key=lambda n: (n == len(AT) - 2, -n)):
        if AT[n] % TICKS == tick:
            r = step - 1 - AT[n] // TICKS
            for c, one in enumerate(sums):

                @pl.when(on(c, r))
                def _():
                    one.stage(n, r)


DOWN, UP = (512, 1024), (1024, 512)
SHAPES = (DOWN, UP, UP, UP)
PAIRS = 4
FEEDS = 8
ROUNDS = FEEDS + 3


def _has(c, r):
    if c == 0:
        return (r >= 0) & (r <= FEEDS + 1)
    if c == 3:
        return (r > FEEDS) & (r < ROUNDS)
    return (r >= 0) & (r < ROUNDS) & (r != FEEDS)


def _slots(c, n):
    if c in (0, 3):
        return lambda r: lax.rem(r, n)
    if n == 2:
        return lambda r: (r + jnp.where(r > FEEDS, 1, 0)) & 1
    return lambda r: lax.rem(r - jnp.where(r > FEEDS, 1, 0), n)


def _layer(x_hbm, dy_hbm, wo_hbm, t_ref, wq_ref, wk_ref, wv_ref, wg_ref, wu_ref, wd_ref, rows_out, cols_out, weights_out, *scratch):
    n, colours = SUM_REFS, len(SHAPES)
    parts, rest = [scratch[c * n : (c + 1) * n] for c in range(colours)], scratch[colours * n :]
    locals_, (send, recv, gather, load), rest = rest[:colours], rest[colours : colours + 4], rest[colours + 4 :]
    x1, x2, xs, q, k, v, o, wo, at, act, dg, du, acc, shares = rest
    x3, x4 = xs.at[0], xs.at[1]
    l0, l1, l2, l3 = locals_
    i = pl.program_id(0) - PAIRS
    tokens = x1.shape[0]
    rows, halves = ([slice(r, r + n) for r in range(0, tokens, n)] for n in (T, F))
    scale = HEAD**-0.5
    e = scale * LOG2E

    def in_rows(r, first, size):
        return rows_out.at[pl.ds(pl.multiple_of(r * DOWN[0] + first, 16), size)]

    def in_cols(c):
        block = lambda r: (c - 1) * ROUNDS + r - (FEEDS + 1 if c == 3 else 0)
        return lambda r, first, size: cols_out.at[pl.ds(pl.multiple_of(first, 16), size), pl.ds(pl.multiple_of(block(r) * UP[1], 128), UP[1])]

    place = Place()
    sums = [Sum(c, SHAPES[c], place, locals_[c], in_cols(c) if c else in_rows, parts[c], (send, recv, gather), _slots(c, 2), _slots(c, 3 if c < 3 else 2))
            for c in range(colours)]
    s0, s1 = _slots(0, 2)(i), _slots(1, 2)(i)

    loads = [pltpu.make_async_copy(src, dst, load.at[n]) for n, (src, dst) in enumerate(((x_hbm, x4), (wo_hbm, wo), (dy_hbm, x2)))]
    pair = i + PAIRS
    saves = [pltpu.make_async_copy(src, weights_out.at[jnp.clip(pair, 0, PAIRS - 1) * 2 + n], load.at[3 + n]) for n, src in enumerate((x2, x3))]

    @pl.when(pair == 0)
    def _():
        loads[0].start()
        place.here()
        loads[0].wait()
        loads[1].start()
        for r in rows:
            a = _normed(x4[r].astype(F32)).astype(BF)
            x1[r] = a
            at[:, r] = a.T

    @pl.when((pair > 0) & (i < 0))
    def _():
        for one in saves:
            one.wait()

    @pl.when(i == 0)
    def _():
        place.meet()
        acc[:] = jnp.zeros_like(acc)

    def forward():
        both = pl.ds(pl.multiple_of(pair * 2 * HEAD, 2 * HEAD), 2 * HEAD)
        heads = [(n, pl.ds(pl.multiple_of((pair * 2 + n) * HEAD, HEAD), HEAD)) for n in range(2)]
        for r in halves:
            a, turns = x1[r], _both(t_ref[r])
            q[r, both] = _turn(_nn(a, wq_ref[:]), *turns)
            k[r, both] = _turn(_nn(a, wk_ref[:]), *turns)
            v[r, both] = _nn(a, wv_ref[:]).astype(BF)

        def spot(j, n):
            return slice((j % 2 * 2 + n) * T, (j % 2 * 2 + n + 1) * T)

        def score(j):
            for n, cols in heads:
                acc[: rows[j].stop, spot(j, n)] = _hidden(_nt(k[: rows[j].stop, cols], q[rows[j], cols]))

        score(0)
        for j, r in enumerate(rows):
            if r.stop < tokens:
                score(j + 1)
            keys = slice(0, r.stop)
            for (n, cols), kept in zip(heads, (x2, x3)):
                s = acc[keys, spot(j, n)]
                p = jnp.exp2((s - s.max(axis=0, keepdims=True)) * e).astype(BF)
                kept[keys, r] = p
                mix = _nn(jnp.concatenate([v[keys, cols].T, jnp.ones((8, r.stop), BF)], 0), p)
                share = 1 / mix[HEAD : HEAD + 1]
                o[r, cols] = (mix[:HEAD] * share).T.astype(BF)
                shares[pair, n : n + 1, r] = share
        for one in saves:
            one.start()

    def onto_residual():
        for one in saves:
            one.wait()
        loads[2].start()
        loads[1].wait()
        for r in halves:
            h = x4[r] + _nn(o[r], wo[:]).astype(BF)
            x4[r] = h
            b = _normed(h.astype(F32)).astype(BF)
            x1[r] = b
            x3[:, r] = b.T
        loads[2].wait()

    def units(r):
        b = x1[r]
        gate, up = _nn(b, wg_ref[:]), _nn(b, wu_ref[:])
        da = _nt(x2[r], wd_ref[:]).astype(BF).astype(F32)
        sig = 1 / (1 + jnp.exp2(gate * -LOG2E))
        silu = gate * sig
        act[r] = (silu * up).astype(BF)
        du[r] = (da * silu).astype(BF)
        dg[r] = (da * up * (sig + silu * (1 - sig))).astype(BF)

    def inward(part):
        acc[:, part] += _nt(dg[:], wg_ref[part]) + _nt(du[:], wu_ref[part])

    def norm_back():
        for r in halves:
            wide, ct = x4[r].astype(F32), acc[r].astype(BF).astype(F32)
            scale = lax.rsqrt(jnp.mean(wide * wide, -1, keepdims=True) + 1e-6)
            back = ct * scale - wide * (scale * scale * scale * jnp.mean(ct * wide, -1, keepdims=True))
            dh = x2[r] + back.astype(BF)
            x2[r] = dh
            x1[r] = _nt(dh, wo[:]).astype(BF)

    def head(n, to):
        cols = pl.ds(pl.multiple_of(n * HEAD, HEAD), HEAD)
        to = pl.ds(pl.multiple_of(to * HEAD, HEAD), HEAD)
        dk, dv = slice(0, HEAD), slice(HEAD, 2 * HEAD)
        for r in reversed(rows):
            keys = slice(0, r.stop)
            dor, qr = x1[r, cols], q[r, cols]
            delta = (dor.astype(F32) * o[r, cols].astype(F32)).T.sum(axis=0, keepdims=True)
            p = xs[n & 1, keys, r].astype(F32) * shares[lax.div(n, 2), pl.ds(n & 1, 1), r]
            ds = (p * (_nt(v[keys, cols], dor) - delta)).astype(BF)
            if r.stop == tokens:
                acc[keys, dv] = _nn(p.astype(BF), dor)
                acc[keys, dk] = _nn(ds, qr)
            else:
                acc[keys, dv] += _nn(p.astype(BF), dor)
                acc[keys, dk] += _nn(ds, qr)
            t = (_tn(k[keys, cols], ds) * scale).T.astype(BF).astype(F32)
            cos, sin = _both(t_ref[r])
            dg[r, to] = (t * cos - pltpu.roll(t, HEAD // 2, 1) * sin).astype(BF)
        for r in rows:
            act[r, to] = acc[r, dv].astype(BF)
            t = (acc[r, dk] * scale).astype(BF).astype(F32)
            cos, sin = _both(t_ref[r])
            du[r, to] = (t * cos - pltpu.roll(t, HEAD // 2, 1) * sin).astype(BF)

    def recall(n):
        return pltpu.make_async_copy(weights_out.at[n], xs.at[n & 1], load.at[3 + (n & 1)])

    def ticking(t, _):
        i, tick = pl.program_id(0) - PAIRS + lax.div(t, TICKS), lax.rem(t, TICKS)
        feeding = (i >= 0) & (i < FEEDS)
        attending = (i == FEEDS + 1) | (i == FEEDS + 2)
        for one in range(TICKS):

            @pl.when(tick == one)
            def _():
                _stages(i, sums, one, _has)

        @pl.when((i < 0) & (tick == 0))
        def _():
            forward()

        @pl.when((i == -1) & (tick == 1))
        def _():
            onto_residual()

        @pl.when(feeding & (tick == 0))
        def _():
            for r in halves:
                units(r)

        @pl.when(feeding & (tick == 1))
        def _():
            l0[s0] = _tn(act[:], x2[:]).astype(BF)
            l1[s1] = _nn(x3[:], dg[:]).astype(BF)
            inward(halves[0])

        @pl.when(feeding & (tick == 2))
        def _():
            l2[s1] = _nn(x3[:], du[:]).astype(BF)
            inward(halves[1])

        @pl.when((i == FEEDS) & (tick == 0))
        def _():
            recall(0).start()
            norm_back()
            recall(1).start()

        @pl.when(((i == FEEDS) | (i == FEEDS + 1)) & (tick == 2))
        def _():
            l0[s0] = _tn(o[:, pl.ds(pl.multiple_of((i - FEEDS) * F, F), F)], x2[:]).astype(BF)

        @pl.when(attending)
        def _():
            def one(j, _):
                n = (i - FEEDS - 1) * PAIRS + j
                recall(n).wait()
                head(n, j)

                @pl.when(n + 2 < 2 * PAIRS)
                def _():
                    recall(n + 2).start()

            begin = lambda t: t + (t >> 1)
            lax.fori_loop(begin(tick), begin(tick + 1), one, None)

        @pl.when(attending & (tick == TICKS - 1))
        def _():
            l1[s1] = _nn(at[:], dg[:]).astype(BF)
            l2[s1] = _nn(at[:], du[:]).astype(BF)
            l3[s0] = _nn(at[:], act[:]).astype(BF)

    lax.fori_loop(0, jnp.where(i < ROUNDS, TICKS, TICKS + AT[-1]), ticking, None)


def layer(x, dy, w):
    tokens, d = x.shape
    turns = _turns(tokens)
    hbm = pl.BlockSpec(memory_space=pl.ANY)
    upto = lambda i, n: jnp.clip(i, 0, n - 1)
    heads = pl.BlockSpec((d, 2 * HEAD), lambda i: (0, upto(i, PAIRS)))
    feed = pl.BlockSpec(UP, lambda i: (0, upto(i - PAIRS, FEEDS)))
    down = pl.BlockSpec(DOWN, lambda i: (upto(i - PAIRS, FEEDS), 0))
    dma, vmem = pltpu.SemaphoreType.DMA, pltpu.VMEM
    return pl.pallas_call(
        _layer,
        grid=(PAIRS + ROUNDS + 1,),
        in_specs=[hbm] * 3 + [pl.BlockSpec(turns.shape, lambda i: (0, 0), pipeline_mode=pl.Buffered(1))] + [heads] * 3 + [feed, feed, down],
        out_specs=[hbm] * 3,
        out_shape=[jax.ShapeDtypeStruct(shape, BF) for shape in (
            (DOWN[0] * (FEEDS + 2), DOWN[1]), (UP[0], (2 * ROUNDS + 2) * UP[1]), (2 * PAIRS, tokens, tokens))],
        scratch_shapes=[one for c, shape in enumerate(SHAPES) for one in _sum_scratch(*shape, 3 if c < 3 else 2)]
        + [vmem((2, *shape), BF) for shape in SHAPES]
        + [dma((len(SHAPES), 12)), dma((len(SHAPES), 6, 2)), dma((len(SHAPES), 6, ROUNDS)), dma((5,))]
        + [vmem((tokens, d), BF)] * 2
        + [vmem((2, tokens, d), BF)]
        + [vmem((tokens, d), BF)] * 6
        + [vmem((tokens, F), BF)] * 3
        + [vmem((tokens, d), F32), vmem((PAIRS, 8, tokens), F32)],
        compiler_params=pltpu.CompilerParams(dimension_semantics=("arbitrary",), vmem_limit_bytes=VMEM, collective_id=0, has_side_effects=True),
        name="layer_and_sum",
    )(x, dy, w["wo"], jnp.asarray(turns), *(w[n] for n in ("wq", "wk", "wv", "w_gate", "w_up", "w_down")))[:2]


def solution(mesh):
    def step(x, dy, *arrays):
        weights, m, v = (dict(zip(NAMES, arrays[i : i + 7], strict=True)) for i in (0, 7, 14))
        w = {n: w[0] for n, w in weights.items()}
        sums = layer(x[0], dy[0], w)
        wide = UP[1]
        places = {"w_down": (0, 0, 0), "wo": (0, FEEDS * DOWN[0], 0), "w_gate": (1, 0, 0), "wq": (1, 0, (FEEDS + 1) * wide),
                  "w_up": (1, 0, ROUNDS * wide), "wk": (1, 0, (ROUNDS + FEEDS + 1) * wide), "wv": (1, 0, 2 * ROUNDS * wide)}
        order = ("w_down", "w_gate", "w_up", "wo", "wq", "wk", "wv")
        each = ([a[n][0] for n in order] for a in (weights, m, v))
        new = [dict(zip(order, one, strict=True)) for one in optimizer(*each, sums, tuple(places[n] for n in order))]
        return tuple(one[name][None] for one in new for name in NAMES)

    states, all_of = P(("rep", "dp"), None, None), P(None, None, None)
    return jax.shard_map(
        step,
        mesh=mesh,
        in_specs=(states, states) + (all_of,) * 21,
        out_specs=(P("rep", None, None),) * 21,
        check_vma=False,
    )
```

```python
import functools

import jax
import jax.numpy as jnp
import numpy as np
from jax import lax
from jax.experimental import pallas as pl
from jax.experimental.pallas import tpu as pltpu
from jax.sharding import PartitionSpec as P

HEAD = 128
THETA = 10000
NAMES = ("wq", "wk", "wv", "wo", "w_gate", "w_up", "w_down")
LOG2E = 1.4426950408889634
T = 256
F = 512
VMEM = 67043328
BF, F32 = jnp.bfloat16, jnp.float32


def _dots(ca, cb):
    return lambda a, b: lax.dot_general(a, b, (((ca,), (cb,)), ((), ())), preferred_element_type=F32)


_nn, _nt, _tn = _dots(1, 0), _dots(1, 1), _dots(0, 0)


def _turns(tokens):
    half = HEAD // 2
    angle = np.arange(tokens, dtype=np.float32)[:, None] * np.float32(THETA) ** (-np.arange(half, dtype=np.float32) / np.float32(half))
    return np.concatenate([np.cos(angle), np.sin(angle)], 1).astype(np.float32)


def _both(t):
    low, other = lax.broadcasted_iota(jnp.int32, t.shape, 1) < HEAD // 2, pltpu.roll(t, HEAD // 2, 1)
    return jnp.where(low, t, other), jnp.where(low, -other, t)


def _normed(wide):
    return wide * lax.rsqrt(jnp.mean(wide * wide, -1, keepdims=True) + 1e-6)


def _turn(t, c, s):
    t = t.astype(BF).astype(F32)
    parts = [t[:, at : at + HEAD] for at in range(0, t.shape[1], HEAD)]
    return jnp.concatenate([x * c + pltpu.roll(x, HEAD // 2, 1) * s for x in parts], 1).astype(BF)


def _hidden(s):
    n = s.shape[0]
    low = s[n - T :]
    ok = lax.broadcasted_iota(jnp.int32, (T, T), 0) <= lax.broadcasted_iota(jnp.int32, (T, T), 1)
    low = jnp.where(ok, low, -1e30)
    return low if n == T else jnp.concatenate([s[: n - T], low], 0)


def _adamw(w, m, v, g):
    m = 0.9 * m + 0.1 * g
    v = 0.95 * v + 0.05 * g * g
    step = m * lax.rsqrt(v + 1e-8) + 0.1 * w
    return (w - 0.02 * step).astype(BF), m, v


TILE = (64, 1024)
DEEP = 16
CHUNK = 16


def _optimizer(*refs, where):
    n = len(where)
    w, m, v = refs[:n], refs[n : 2 * n], refs[2 * n : 3 * n]
    g, refs = refs[3 * n : 3 * n + 2], refs[3 * n + 2 :]
    out, (wi, mi, vi, gi, wn, mn, vn, came, left) = (refs[:n], refs[n : 2 * n], refs[2 * n : 3 * n]), refs[3 * n :]
    rows, cols = TILE
    tiles = [(one.shape[0] // rows) * (one.shape[1] // cols) for one in w]
    first = [sum(tiles[:j]) for j in range(n + 1)]

    def part(j, t):
        across = w[j].shape[1] // cols
        return lax.div(t, across) * rows, lax.rem(t, across) * cols

    def tile(ref, row, col):
        return ref.at[pl.ds(pl.multiple_of(row, rows), rows), pl.ds(pl.multiple_of(col, 512), cols)]

    def loads(j, t, slot):
        row, col = part(j, t)
        at, r0, c0 = where[j]
        pairs = ((tile(w[j], row, col), wi), (tile(m[j], row, col), mi), (tile(v[j], row, col), vi), (tile(g[at], r0 + row, c0 + col), gi))
        return [pltpu.make_async_copy(src, dst.at[slot], came.at[k, slot]) for k, (src, dst) in enumerate(pairs)]

    def stores(j, t, slot):
        row, col = part(j, t)
        pairs = zip((wn, mn, vn), (tile(o[j], row, col) for o in out), strict=True)
        return [pltpu.make_async_copy(src.at[slot], dst, left.at[k, slot]) for k, (src, dst) in enumerate(pairs)]

    for k in range(DEEP - 1):
        for copy in loads(0, k, k):
            copy.start()
    for j in range(n):

        def body(t, _, j=j):
            k = first[j] + t
            slot = lax.rem(k, DEEP)
            ahead = k + DEEP - 1
            for other in range(j, n):
                if first[other] < first[j + 1] + DEEP - 1:

                    @pl.when((ahead >= first[other]) & (ahead < first[other + 1]))
                    def _():
                        for copy in loads(other, ahead - first[other], lax.rem(ahead, DEEP)):
                            copy.start()
            for copy in loads(j, t, slot):
                copy.wait()

            @pl.when(k >= DEEP)
            def _():
                for copy in stores(0, 0, slot):
                    copy.wait()

            def chunk(c, _):
                r = pl.ds(pl.multiple_of(c * CHUNK, CHUNK), CHUNK)
                wn[slot, r], mn[slot, r], vn[slot, r] = _adamw(wi[slot, r].astype(F32), mi[slot, r], vi[slot, r], gi[slot, r].astype(F32))

            lax.fori_loop(0, rows // CHUNK, chunk, None)
            for copy in stores(j, t, slot):
                copy.start()

        lax.fori_loop(0, tiles[j], body, None)
    for k in range(DEEP):
        for copy in stores(0, 0, k):
            copy.wait()


def optimizer(w, m, v, sums, where):
    like = [jax.ShapeDtypeStruct(one.shape, one.dtype) for one in (*w, *m, *v)]
    hbm, n = pl.BlockSpec(memory_space=pl.ANY), len(w)
    new = pl.pallas_call(
        functools.partial(_optimizer, where=where),
        in_specs=[hbm] * (3 * n + 2),
        out_specs=[hbm] * (3 * n),
        out_shape=like,
        scratch_shapes=[pltpu.VMEM((DEEP, *TILE), kind) for kind in (BF, F32, F32, BF, BF, F32, F32)]
        + [pltpu.SemaphoreType.DMA((4, DEEP)), pltpu.SemaphoreType.DMA((3, DEEP))],
        compiler_params=pltpu.CompilerParams(vmem_limit_bytes=VMEM),
        name="optimizer",
    )(*w, *m, *v, *sums)
    return new[:n], new[n : 2 * n], new[2 * n :]


RING = 4
OTHERS, NEXT = (1, 2, 3), (1, 3)
SHIFT = {"x": 5, "y": 3, "z": 1}
COLOURS = (("x", "y", "z"), ("y", "z", "x"), ("z", "x", "y"), ("x", "y", "z"))
TICKS = 3
AT = (0, 1, 2, 4, 5, 7, 8, 10, 11, 12, 14, 17, 20)


class Place:
    def __init__(self):
        me = lax.axis_index("dp")
        self.core = me & 1
        self.partner = me ^ 1
        self.at = {axis: (me >> shift) & 3 for axis, shift in SHIFT.items()}
        self.peers = {axis: {by: me + ((((self.at[axis] + by) & 3) - self.at[axis]) << shift) for by in OTHERS} for axis, shift in SHIFT.items()}

    def here(self):
        self.everyone = [self.partner] + [peer for axis in SHIFT for peer in self.peers[axis].values()]
        for peer in self.everyone:
            pl.semaphore_signal(pltpu.get_barrier_semaphore(), 1, device_id={"dp": peer})

    def meet(self):
        pl.semaphore_wait(pltpu.get_barrier_semaphore(), 1 + len(SHIFT) * (RING - 1))


class Sum:
    def __init__(self, colour, blk, place, local, out, refs, sems, slot, slot3):
        self.c, (self.R, self.C), self.slot, self.slot3, self.place = colour, blk, slot, slot3, place
        self.local, self.out = local, out
        self.rc, self.sa1, self.ra1, self.sa2, self.ra2, self.ra, self.sb1, self.rb1, self.sb2, self.rb2, self.rb, self.sc, self.rcc, self.all = refs
        self.send, self.recv, self.gather = sems
        self.core = place.core
        self.a, self.b, self.k = (place.at[axis] for axis in COLOURS[colour])
        self.first = (self.core * (self.R // 2), self.core * (self.R // 2) + self.a * (self.R // 8))
        self.first += (self.first[1] + self.b * (self.R // 32),)

    def peer(self, n, by):
        return self.place.peers[COLOURS[self.c][n]][by]

    def copy(self, src, dst, kind, device, slot=None, r=None):
        recv = self.recv.at[self.c, kind, slot] if r is None else self.gather.at[self.c, kind - 6, r]
        return pltpu.make_async_remote_copy(src, dst, self.send.at[self.c, kind], recv, device_id={"dp": device})

    def wait(self, ref, kind, slot=None, r=None, send=None):
        recv = self.recv.at[self.c, kind, slot] if r is None else self.gather.at[self.c, kind - 6, r]
        pltpu.make_async_copy(ref, ref, recv).wait()
        ref = ref if send is None else send
        pltpu.make_async_copy(ref, ref, self.send.at[self.c, kind]).wait()

    def quarter(self, r, by, half=None):
        n8 = self.R // 8
        q = (self.a + by) & 3
        cols = slice(None) if half is None else pl.ds(half * (self.C // 2), self.C // 2)
        mine = self.local[self.slot(r), pl.ds(pl.multiple_of(self.first[0] + q * n8, 16), n8), cols]
        return mine.astype(F32) + self.rc[self.slot3(r), pl.ds(pl.multiple_of(q * n8, 16), n8), cols].astype(F32)

    def cols(self, q):
        return pl.ds(pl.multiple_of(q * (self.C // 4), 128), self.C // 4)

    def stage(self, n, r):
        R, C = self.R, self.C
        slot = self.slot(r)
        n8, n32, half = R // 8, R // 32, C // 2
        left, right = pl.ds(0, half), pl.ds(half, half)
        f32 = lambda v: v.astype(F32)
        low = lambda v: v.astype(BF)
        if n == 0:
            other = pl.ds(pl.multiple_of((1 - self.core) * (R // 2), 16), R // 2)
            self.copy(self.local.at[slot, other], self.rc.at[self.slot3(r)], 0, self.place.partner, slot).start()
        elif n == 1:
            self.wait(self.rc.at[self.slot3(r)], 0, slot)
            self.sa1[:] = low(self.quarter(r, 2))
            self.both(self.sa1, self.ra1, 1, 0, slot, left, right)
        elif n == 2:
            self.wait(self.ra1.at[slot], 1, slot)
            self.sa2[0, :, :half] = low(self.quarter(r, 1, 0) + f32(self.ra1[slot, :, :half]))
            self.sa2[0, :, half:] = low(self.quarter(r, 1, 1))
            self.sa2[1, :, :half] = low(self.quarter(r, 3, 0))
            self.sa2[1, :, half:] = low(self.quarter(r, 3, 1) + f32(self.ra1[slot, :, half:]))
            self.pair(self.sa2, self.ra2, 2, 0, slot)
        elif n == 3:
            self.wait(self.ra2.at[slot], 2, slot)
            self.ra[:] = self.quarter(r, 0) + f32(self.ra2[slot, 0]) + f32(self.ra2[slot, 1])
            self.sb1[:] = low(self.ra[self.sixteenth(2)])
            self.both(self.sb1, self.rb1, 3, 1, slot, left, right)
        elif n == 4:
            self.wait(self.rb1.at[slot], 3, slot)
            up, down = self.sixteenth(1), self.sixteenth(3)
            self.sb2[0, :, :half] = low(self.ra[up, :half] + f32(self.rb1[slot, :, :half]))
            self.sb2[0, :, half:] = low(self.ra[up, half:])
            self.sb2[1, :, :half] = low(self.ra[down, :half])
            self.sb2[1, :, half:] = low(self.ra[down, half:] + f32(self.rb1[slot, :, half:]))
            self.pair(self.sb2, self.rb2, 4, 1, slot)
        elif n == 5:
            self.wait(self.rb2.at[slot], 4, slot)
            total = self.ra[self.sixteenth(0)] + f32(self.rb2[slot, 0]) + f32(self.rb2[slot, 1])
            self.rb[:] = total
            self.sc[:] = low(total)
            for by in OTHERS:
                to = (self.k + by) & 3
                self.copy(self.sc.at[:, self.cols(to)], self.rcc.at[slot, by - 1], 5, self.peer(2, by), slot).start()
        elif n == 6:
            self.wait(self.rcc.at[slot], 5, slot)
            total = self.rb[:, self.cols(self.k)]
            for by in range(3):
                total = total + f32(self.rcc[slot, by])
            self.all[r & 3, self.sixteenth(0), self.cols(self.k)] = low(total)
            mine = self.all.at[r & 3, self.sixteenth(0), self.cols(self.k)]
            for by in OTHERS:
                self.copy(mine, mine, 6, self.peer(2, by), r=r).start()
        elif n == 7:
            self.wait(self.rcc.at[slot], 6, r=r)
            mine = self.all.at[r & 3, self.sixteenth(0)]
            for by in NEXT:
                self.copy(mine, mine, 7, self.peer(1, by), r=r).start()
        elif n == 8:
            self.wait(self.all.at[r & 3, pl.ds(0, 2 * n32)], 7, r=r)
            self.onward(lambda by: self.all.at[r & 3, self.sixteenth(by)], r, 8, 1, left, right)
        elif n == 9:
            self.wait(self.all.at[r & 3, pl.ds(0, n32)], 8, r=r)
            whole, mine = self.all.at[r & 3], self.out(r, self.first[1], n8)
            pltpu.make_async_copy(whole, mine, self.gather.at[self.c, 3, r]).start()
            for by in NEXT:
                self.copy(whole, mine, 9, self.peer(0, by), r=r).start()
        elif n == 10:
            self.wait(self.out(r, 0, 3 * n8), 9, r=r, send=self.out(r, 0, 2 * n8))
            self.onward(lambda by: self.out(r, self.first[0] + ((self.a + by) & 3) * n8, n8), r, 10, 0, left, right)
        elif n == 11:
            self.wait(self.out(r, 0, n8), 10, r=r)
            mine = self.out(r, self.first[0], R // 2)
            self.copy(mine, mine, 11, self.place.partner, r=r).start()
        else:
            self.wait(self.out(r, 0, R // 2), 11, r=r)

    def sixteenth(self, by):
        return pl.ds(pl.multiple_of(((self.b + by) & 3) * (self.R // 32), 16), self.R // 32)

    def both(self, src, dst, kind, axis, slot, left, right):
        self.copy(src.at[:, left], dst.at[slot, :, left], kind, self.peer(axis, 1), slot).start()
        self.copy(src.at[:, right], dst.at[slot, :, right], kind, self.peer(axis, 3), slot).start()

    def pair(self, src, dst, kind, axis, slot):
        self.copy(src.at[0], dst.at[slot, 0], kind, self.peer(axis, 1), slot).start()
        self.copy(src.at[1], dst.at[slot, 1], kind, self.peer(axis, 3), slot).start()

    def onward(self, part, r, kind, axis, left, right):
        before, after = part(3).at[:, left], part(1).at[:, right]
        self.copy(before, before, kind, self.peer(axis, 1), r=r).start()
        self.copy(after, after, kind, self.peer(axis, 3), r=r).start()


def _sum_scratch(R, C, deep):
    n2, n8, n32 = R // 2, R // 8, R // 32
    return [pltpu.VMEM(shape, kind) for shape, kind in (
        ((deep, n2, C), BF), ((n8, C), BF), ((2, n8, C), BF), ((2, n8, C), BF), ((2, 2, n8, C), BF), ((n8, C), F32),
        ((n32, C), BF), ((2, n32, C), BF), ((2, n32, C), BF), ((2, 2, n32, C), BF), ((n32, C), F32), ((n32, C), BF), ((2, 3, n32, C // 4), BF),
        ((4, n8, C), BF))]


SUM_REFS = 14


def _stages(step, sums, tick, on):
    for n in reversed(range(len(AT))):
        if AT[n] % TICKS == tick:
            r = step - 1 - AT[n] // TICKS
            for c, one in enumerate(sums):

                @pl.when(on(c, r))
                def _():
                    one.stage(n, r)


DOWN, UP = (512, 1024), (1024, 512)
SHAPES = (DOWN, UP, UP, UP)
PAIRS = 4
FEEDS = 8
ROUNDS = FEEDS + 3


def _has(c, r):
    if c == 0:
        return (r >= 0) & (r <= FEEDS + 1)
    if c == 3:
        return (r > FEEDS) & (r < ROUNDS)
    return (r >= 0) & (r < ROUNDS) & (r != FEEDS)


def _slots(c, n):
    if c in (0, 3):
        return lambda r: lax.rem(r, n)
    if n == 2:
        return lambda r: (r + jnp.where(r > FEEDS, 1, 0)) & 1
    return lambda r: lax.rem(r - jnp.where(r > FEEDS, 1, 0), n)


def _layer(x_hbm, dy_hbm, wo_hbm, t_ref, wq_ref, wk_ref, wv_ref, wg_ref, wu_ref, wd_ref, rows_out, cols_out, weights_out, *scratch):
    n, colours = SUM_REFS, len(SHAPES)
    parts, rest = [scratch[c * n : (c + 1) * n] for c in range(colours)], scratch[colours * n :]
    locals_, (send, recv, gather, load), rest = rest[:colours], rest[colours : colours + 4], rest[colours + 4 :]
    x1, x2, xs, q, k, v, o, wo, at, act, dg, du, acc, shares = rest
    x3, x4 = xs.at[0], xs.at[1]
    l0, l1, l2, l3 = locals_
    i = pl.program_id(0) - PAIRS
    tokens = x1.shape[0]
    rows, halves = ([slice(r, r + n) for r in range(0, tokens, n)] for n in (T, F))
    scale = HEAD**-0.5
    e = scale * LOG2E

    def in_rows(r, first, size):
        return rows_out.at[pl.ds(pl.multiple_of(r * DOWN[0] + first, 16), size)]

    def in_cols(c):
        block = lambda r: (c - 1) * ROUNDS + r - (FEEDS + 1 if c == 3 else 0)
        return lambda r, first, size: cols_out.at[pl.ds(pl.multiple_of(first, 16), size), pl.ds(pl.multiple_of(block(r) * UP[1], 128), UP[1])]

    place = Place()
    sums = [Sum(c, SHAPES[c], place, locals_[c], in_cols(c) if c else in_rows, parts[c], (send, recv, gather), _slots(c, 2), _slots(c, 3 if c < 3 else 2))
            for c in range(colours)]
    s0, s1 = _slots(0, 2)(i), _slots(1, 2)(i)

    loads = [pltpu.make_async_copy(src, dst, load.at[n]) for n, (src, dst) in enumerate(((x_hbm, x4), (wo_hbm, wo), (dy_hbm, x2)))]
    pair = i + PAIRS
    saves = [pltpu.make_async_copy(src, weights_out.at[jnp.clip(pair, 0, PAIRS - 1) * 2 + n], load.at[3 + n]) for n, src in enumerate((x2, x3))]

    @pl.when(pair == 0)
    def _():
        loads[0].start()
        place.here()
        loads[0].wait()
        loads[1].start()
        for r in rows:
            a = _normed(x4[r].astype(F32)).astype(BF)
            x1[r] = a
            at[:, r] = a.T

    @pl.when((pair > 0) & (i < 0))
    def _():
        for one in saves:
            one.wait()

    @pl.when(i == 0)
    def _():
        place.meet()
        acc[:] = jnp.zeros_like(acc)

    def forward():
        both = pl.ds(pl.multiple_of(pair * 2 * HEAD, 2 * HEAD), 2 * HEAD)
        heads = [(n, pl.ds(pl.multiple_of((pair * 2 + n) * HEAD, HEAD), HEAD)) for n in range(2)]
        for r in halves:
            a, turns = x1[r], _both(t_ref[r])
            q[r, both] = _turn(_nn(a, wq_ref[:]), *turns)
            k[r, both] = _turn(_nn(a, wk_ref[:]), *turns)
            v[r, both] = _nn(a, wv_ref[:]).astype(BF)

        def spot(j, n):
            return slice((j % 2 * 2 + n) * T, (j % 2 * 2 + n + 1) * T)

        def score(j):
            for n, cols in heads:
                acc[: rows[j].stop, spot(j, n)] = _hidden(_nt(k[: rows[j].stop, cols], q[rows[j], cols]))

        score(0)
        for j, r in enumerate(rows):
            if r.stop < tokens:
                score(j + 1)
            keys = slice(0, r.stop)
            for (n, cols), kept in zip(heads, (x2, x3)):
                s = acc[keys, spot(j, n)]
                p = jnp.exp2((s - s.max(axis=0, keepdims=True)) * e).astype(BF)
                kept[keys, r] = p
                mix = _nn(jnp.concatenate([v[keys, cols].T, jnp.ones((8, r.stop), BF)], 0), p)
                share = 1 / mix[HEAD : HEAD + 1]
                o[r, cols] = (mix[:HEAD] * share).T.astype(BF)
                shares[pair, n : n + 1, r] = share
        for one in saves:
            one.start()

    def onto_residual():
        for one in saves:
            one.wait()
        loads[2].start()
        loads[1].wait()
        for r in halves:
            h = x4[r] + _nn(o[r], wo[:]).astype(BF)
            x4[r] = h
            b = _normed(h.astype(F32)).astype(BF)
            x1[r] = b
            x3[:, r] = b.T
        loads[2].wait()

    def units(r):
        b = x1[r]
        gate, up = _nn(b, wg_ref[:]), _nn(b, wu_ref[:])
        da = _nt(x2[r], wd_ref[:]).astype(BF).astype(F32)
        sig = 1 / (1 + jnp.exp2(gate * -LOG2E))
        silu = gate * sig
        act[r] = (silu * up).astype(BF)
        du[r] = (da * silu).astype(BF)
        dg[r] = (da * up * (sig + silu * (1 - sig))).astype(BF)

    def inward(part):
        acc[:, part] += _nt(dg[:], wg_ref[part]) + _nt(du[:], wu_ref[part])

    def norm_back():
        for r in halves:
            wide, ct = x4[r].astype(F32), acc[r].astype(BF).astype(F32)
            scale = lax.rsqrt(jnp.mean(wide * wide, -1, keepdims=True) + 1e-6)
            back = ct * scale - wide * (scale * scale * scale * jnp.mean(ct * wide, -1, keepdims=True))
            dh = x2[r] + back.astype(BF)
            x2[r] = dh
            x1[r] = _nt(dh, wo[:]).astype(BF)

    def head(n, to):
        cols = pl.ds(pl.multiple_of(n * HEAD, HEAD), HEAD)
        to = pl.ds(pl.multiple_of(to * HEAD, HEAD), HEAD)
        dk, dv = slice(0, HEAD), slice(HEAD, 2 * HEAD)
        for r in reversed(rows):
            keys = slice(0, r.stop)
            dor, qr = x1[r, cols], q[r, cols]
            delta = (dor.astype(F32) * o[r, cols].astype(F32)).T.sum(axis=0, keepdims=True)
            p = xs[n & 1, keys, r].astype(F32) * shares[lax.div(n, 2), pl.ds(n & 1, 1), r]
            ds = (p * (_nt(v[keys, cols], dor) - delta)).astype(BF)
            if r.stop == tokens:
                acc[keys, dv] = _nn(p.astype(BF), dor)
                acc[keys, dk] = _nn(ds, qr)
            else:
                acc[keys, dv] += _nn(p.astype(BF), dor)
                acc[keys, dk] += _nn(ds, qr)
            t = (_tn(k[keys, cols], ds) * scale).T.astype(BF).astype(F32)
            cos, sin = _both(t_ref[r])
            dg[r, to] = (t * cos - pltpu.roll(t, HEAD // 2, 1) * sin).astype(BF)
        for r in rows:
            act[r, to] = acc[r, dv].astype(BF)
            t = (acc[r, dk] * scale).astype(BF).astype(F32)
            cos, sin = _both(t_ref[r])
            du[r, to] = (t * cos - pltpu.roll(t, HEAD // 2, 1) * sin).astype(BF)

    def recall(n):
        return pltpu.make_async_copy(weights_out.at[n], xs.at[n & 1], load.at[3 + (n & 1)])

    feeding = (i >= 0) & (i < FEEDS)
    attending = (i == FEEDS + 1) | (i == FEEDS + 2)

    def ticking(tick, _):
        for one in range(TICKS):

            @pl.when(tick == one)
            def _():
                _stages(i, sums, one, _has)

        @pl.when((i < 0) & (tick == 0))
        def _():
            forward()

        @pl.when((i == -1) & (tick == 1))
        def _():
            onto_residual()

        @pl.when(feeding & (tick == 0))
        def _():
            for r in halves:
                units(r)

        @pl.when(feeding & (tick == 1))
        def _():
            l0[s0] = _tn(act[:], x2[:]).astype(BF)
            l1[s1] = _nn(x3[:], dg[:]).astype(BF)
            inward(halves[0])

        @pl.when(feeding & (tick == 2))
        def _():
            l2[s1] = _nn(x3[:], du[:]).astype(BF)
            inward(halves[1])

        @pl.when((i == FEEDS) & (tick == 0))
        def _():
            recall(0).start()
            norm_back()
            recall(1).start()

        @pl.when(((i == FEEDS) | (i == FEEDS + 1)) & (tick == 2))
        def _():
            l0[s0] = _tn(o[:, pl.ds(pl.multiple_of((i - FEEDS) * F, F), F)], x2[:]).astype(BF)

        @pl.when(attending)
        def _():
            def one(j, _):
                n = (i - FEEDS - 1) * PAIRS + j
                recall(n).wait()
                head(n, j)

                @pl.when(n + 2 < 2 * PAIRS)
                def _():
                    recall(n + 2).start()

            begin = lambda t: t + (t >> 1)
            lax.fori_loop(begin(tick), begin(tick + 1), one, None)

        @pl.when(attending & (tick == TICKS - 1))
        def _():
            l1[s1] = _nn(at[:], dg[:]).astype(BF)
            l2[s1] = _nn(at[:], du[:]).astype(BF)
            l3[s0] = _nn(at[:], act[:]).astype(BF)

    lax.fori_loop(0, TICKS, ticking, None)


def layer(x, dy, w):
    tokens, d = x.shape
    turns = _turns(tokens)
    hbm = pl.BlockSpec(memory_space=pl.ANY)
    upto = lambda i, n: jnp.clip(i, 0, n - 1)
    heads = pl.BlockSpec((d, 2 * HEAD), lambda i: (0, upto(i, PAIRS)))
    feed = pl.BlockSpec(UP, lambda i: (0, upto(i - PAIRS, FEEDS)))
    down = pl.BlockSpec(DOWN, lambda i: (upto(i - PAIRS, FEEDS), 0))
    dma, vmem = pltpu.SemaphoreType.DMA, pltpu.VMEM
    return pl.pallas_call(
        _layer,
        grid=(PAIRS + ROUNDS + 1 + AT[-1] // TICKS,),
        in_specs=[hbm] * 3 + [pl.BlockSpec(turns.shape, lambda i: (0, 0), pipeline_mode=pl.Buffered(1))] + [heads] * 3 + [feed, feed, down],
        out_specs=[hbm] * 3,
        out_shape=[jax.ShapeDtypeStruct(shape, BF) for shape in (
            (DOWN[0] * (FEEDS + 2), DOWN[1]), (UP[0], (2 * ROUNDS + 2) * UP[1]), (2 * PAIRS, tokens, tokens))],
        scratch_shapes=[one for c, shape in enumerate(SHAPES) for one in _sum_scratch(*shape, 3 if c < 3 else 2)]
        + [vmem((2, *shape), BF) for shape in SHAPES]
        + [dma((len(SHAPES), 12)), dma((len(SHAPES), 6, 2)), dma((len(SHAPES), 6, ROUNDS)), dma((5,))]
        + [vmem((tokens, d), BF)] * 2
        + [vmem((2, tokens, d), BF)]
        + [vmem((tokens, d), BF)] * 6
        + [vmem((tokens, F), BF)] * 3
        + [vmem((tokens, d), F32), vmem((PAIRS, 8, tokens), F32)],
        compiler_params=pltpu.CompilerParams(dimension_semantics=("arbitrary",), vmem_limit_bytes=VMEM, collective_id=0, has_side_effects=True),
        name="layer_and_sum",
    )(x, dy, w["wo"], jnp.asarray(turns), *(w[n] for n in ("wq", "wk", "wv", "w_gate", "w_up", "w_down")))[:2]


def solution(mesh):
    def step(x, dy, *arrays):
        weights, m, v = (dict(zip(NAMES, arrays[i : i + 7], strict=True)) for i in (0, 7, 14))
        w = {n: w[0] for n, w in weights.items()}
        sums = layer(x[0], dy[0], w)
        wide = UP[1]
        places = {"w_down": (0, 0, 0), "wo": (0, FEEDS * DOWN[0], 0), "w_gate": (1, 0, 0), "wq": (1, 0, (FEEDS + 1) * wide),
                  "w_up": (1, 0, ROUNDS * wide), "wk": (1, 0, (ROUNDS + FEEDS + 1) * wide), "wv": (1, 0, 2 * ROUNDS * wide)}
        order = ("w_down", "w_gate", "w_up", "wo", "wq", "wk", "wv")
        each = ([a[n][0] for n in order] for a in (weights, m, v))
        new = [dict(zip(order, one, strict=True)) for one in optimizer(*each, sums, tuple(places[n] for n in order))]
        return tuple(one[name][None] for one in new for name in NAMES)

    states, all_of = P(("rep", "dp"), None, None), P(None, None, None)
    return jax.shard_map(
        step,
        mesh=mesh,
        in_specs=(states, states) + (all_of,) * 21,
        out_specs=(P("rep", None, None),) * 21,
        check_vma=False,
    )
```
